512 devices in a mesh: gx: 4 (over x), gy: 16 (over z), gz: 8 (over y, core).
Axes of the slice: x: 4, y: 4, z: 16, core: 2. Of those that a mesh axis runs over, the one named last changes fastest.
Arguments:
- old_data: float32 [6144, 5, 16, 256], P(('gx', 'gy', 'gz')), may hold values from -6 to 24, as said below
- pair_old: int32 [16384], P(('gx', 'gy', 'gz')), may hold values from 0 to 11
- pair_slot: int32 [16384], P(('gx', 'gy', 'gz')), may hold values from 0 to 2
- pair_shift: int32 [16384, 3], P(('gx', 'gy', 'gz')), may hold values from -2 to 2
- pair_dest: int32 [16384, 1], P(('gx', 'gy', 'gz')), may hold values from 0 to 31; in each aligned block of 32 rows (0 to 31, 32 to 63, ...) at most 2 rows name the same one
- new_ratio: int32 [1536], replicated, may hold values from 1 to 2, as said below
- neighbor_side: int32 [1536, 6], P(('gx', 'gy', 'gz')), may hold values from 0 to 3
- neighbor_patch: int32 [1536, 6], P(('gx', 'gy', 'gz')), may hold values from 0 to 2
Outputs:
- new_data: float32 [1536, 5, 16, 256], P(('gx', 'gy', 'gz'))
- interface_jump: float32 [1536, 5, 6, 256], P(('gx', 'gy', 'gz'))
- mass_totals: float32 [2, 5], replicated
The draws below stay inside these ranges and needn't reach their ends.
Inputs may be any that keep to these rules, and one draw needn't show every extreme that they name: `old_data`: values of order one whose level differs from patch to patch and field to field. `pair_dest`: on the rows of one device no owner is named more than 2 times, and some device names some owner exactly 2 times. `new_ratio`: 1 marks a new patch on the old level, 2 one coarser by a factor of two in each direction. `neighbor_side`: 0: on the device before in the order d, 1: on the same device, 2: on the device after, 3: no neighbour.
All inputs are finite; a program needn't handle non-finite values.
Results may differ from the reference program's by a relative error of at most 0.0001.
Values sent between devices are 32-bit elements; how exact they have to be, the bound alone decides.
No kernel may reach another device: no remote copies, remote signals or barrier semaphores. Data moves between devices by JAX's collectives and lax.ppermute only.
A program may use at most 64 MiB of HBM per device.

```python
import math
import jax
import jax.numpy as jnp
import numpy as np
from jax import lax

FIELDS = 5
EDGE = 16
CAP = 2
P_OLD = 12
P_NEW = 3
PAIRS_DEV = 32
OLD = 6144
NEW = 1536
PAIRS = 16384
N_GX = 4
N_GY = 16
N_GZ = 8
DEVICES = 512


def draw_old_data(key, part):
    noise_key, base_key = jax.random.split(key, 2)
    block_shape = (OLD, FIELDS, EDGE, EDGE * EDGE)
    rising = jnp.exp(jnp.log(3.0) * jnp.arange(OLD, dtype=jnp.float32) / max(OLD - 1, 1))
    field_base = jax.random.uniform(base_key, (FIELDS,), jnp.float32, 0.5, 2.0)
    noise_draw = jnp.clip(0.6 * jax.random.normal(noise_key, block_shape, jnp.float32), -2.0, 2.0)
    base_level = rising[:, None, None, None] * field_base[None, :, None, None]
    return (base_level * (1.0 + noise_draw)).astype(jnp.float32)


def draw_new_ratio(key, part):
    ratio_key = jax.random.fold_in(key, 17)
    picks = jax.random.randint(ratio_key, (NEW,), 0, 8, dtype=jnp.int32)
    return (1 + (picks == 0).astype(jnp.int32)).astype(jnp.int32)


def touch_ends(drawn, stream_key, smallest, largest):
    shape = drawn.shape
    place = [jax.random.randint(jax.random.fold_in(stream_key, axis), (), 0, shape[axis]) for axis in range(len(shape))]
    drawn = drawn.at[tuple(place)].set(smallest)
    longest = shape.index(max(shape))
    place[longest] = (place[longest] + 1) % shape[longest]
    return drawn.at[tuple(place)].set(largest)


def assign_block(own_key, own, number, rows, number_of, top, bound, slope):
    sequence = jax.random.permutation(own_key, number_of)
    crowded, ordinary = portions_of(number_of, rows * top, bound, slope, True), portions_of(number_of, rows * top, bound, slope, False)
    places = jnp.arange(number_of)

    def named(sizes, offset_by):
        used = int((sizes > 0).sum())
        fixed = max(1, used // 4)
        shifted = fixed + (places - fixed + offset_by * (used - fixed)) % max(1, number_of - fixed)
        return jnp.zeros((number_of,), jnp.int32).at[sequence[jnp.where(places < fixed, places, shifted)]].set(jnp.asarray(sizes, jnp.int32))

    sizes = jnp.where(number % 4 == 0, named(crowded, number // 4), named(ordinary, number - number // 4 - 1))
    mixed = jax.random.permutation(jax.random.fold_in(own, 3), number_of)
    donor, taker = mixed[0:number_of // 2 * 2:2], mixed[1:number_of // 2 * 2:2]
    slack = jnp.minimum(sizes[donor] - 1, bound - sizes[taker]) // 2
    slack = jnp.where((donor == sequence[0]) | (taker == sequence[0]) | (sizes[taker] == 0), 0, jnp.maximum(slack, 0))
    shifted = jax.random.randint(jax.random.fold_in(own, 4), (number_of // 2,), 0, 1 << 20) % (slack + 1)
    sizes = sizes.at[donor].add(-shifted).at[taker].add(shifted)
    labels = jnp.searchsorted(jnp.cumsum(sizes), jnp.arange(rows * top), side="right").astype(jnp.int32)
    grid = labels.reshape(top, rows).T
    grid = grid[jax.random.permutation(jax.random.fold_in(own, 1), rows)]
    offset_by = jax.random.randint(jax.random.fold_in(own, 2), (rows, 1), 0, top)
    return jnp.take_along_axis(grid, (jnp.arange(top)[None, :] + offset_by) % top, axis=1)


def portions_of(number_of, total, reach, skew, full):
    weights = [(1 << 20) // math.isqrt(standing ** skew) + 1 for standing in range(1, number_of + 1)]
    largest = reach if full else min(reach, max(-(-total // number_of), total * weights[0] // sum(weights)))
    least = 1 if total - largest >= number_of - 1 else 0
    holding, rest = [largest] + [least] * (number_of - 1), total - largest - least * (number_of - 1)
    while rest > 0:
        movable = [i for i in range(1, number_of) if holding[i] < largest] or [i for i in range(1, number_of) if holding[i] < reach]
        whole, left = sum([weights[i] for i in movable]), rest
        for i in movable:
            addition = min(reach - holding[i], max(1, left * weights[i] // whole), rest)
            holding[i] = holding[i] + addition
            rest = rest - addition
    return np.array(holding)


def setup_inputs(seed: int = 0) -> dict:
    key_list = jax.random.split(jax.random.key(seed), 9)
    old_data = draw_old_data(jax.random.fold_in(key_list[8], 71), 0)
    pair_old = touch_ends(jax.random.randint(key_list[1], (PAIRS,), 0, P_OLD), jax.random.fold_in(key_list[1], 1), 0, P_OLD - 1).astype(jnp.int32)
    pair_slot = touch_ends(jax.random.randint(key_list[2], (PAIRS,), 0, P_NEW), jax.random.fold_in(key_list[2], 1), 0, P_NEW - 1).astype(jnp.int32)
    pair_shift = touch_ends(jax.random.randint(key_list[3], (PAIRS, 3), -2, 3), jax.random.fold_in(key_list[3], 1), -2, 2).astype(jnp.int32)
    pair_dest_keys = jax.random.split(jax.random.fold_in(key_list[4], 1), PAIRS // PAIRS_DEV)
    pair_dest_turns = jax.random.permutation(jax.random.fold_in(key_list[4], 3), PAIRS // PAIRS_DEV)
    pair_dest = jax.vmap(lambda own, number: assign_block(jax.random.fold_in(key_list[4], 2), own, number, PAIRS_DEV, N_GX * N_GZ, 1, CAP, 2))(pair_dest_keys, pair_dest_turns).reshape((PAIRS, 1))
    new_ratio = draw_new_ratio(jax.random.fold_in(key_list[8], 71), 0)
    neighbor_side = touch_ends(jax.random.randint(key_list[6], (NEW, 6), 0, 4), jax.random.fold_in(key_list[6], 1), 0, 3).astype(jnp.int32)
    neighbor_patch = touch_ends(jax.random.randint(key_list[7], (NEW, 6), 0, P_NEW), jax.random.fold_in(key_list[7], 1), 0, P_NEW - 1).astype(jnp.int32)
    return dict(old_data=old_data, pair_old=pair_old, pair_slot=pair_slot, pair_shift=pair_shift, pair_dest=pair_dest, new_ratio=new_ratio, neighbor_side=neighbor_side, neighbor_patch=neighbor_patch)


precise = lax.Precision.HIGHEST


def intersection_weights(offsets, ratios, edge_cells):
    cell_index = jnp.arange(edge_cells, dtype=jnp.int32)
    distance = cell_index[None, None, :] - offsets[:, None, None]
    within = (distance >= 0) & (jnp.floor_divide(distance, ratios[:, None, None]) == cell_index[None, :, None])
    scaled = 1.0 / ratios[:, None, None].astype(jnp.float32)
    return jnp.where(within, scaled, jnp.zeros_like(scaled)).astype(jnp.float32)


def reference(old_data, pair_old, pair_slot, pair_shift, pair_dest, new_ratio, neighbor_side, neighbor_patch):
    pair_ids = jnp.arange(PAIRS, dtype=jnp.int32)
    sender = pair_ids // PAIRS_DEV
    sender_y = (sender // N_GZ) % N_GY
    target = pair_dest[:, 0]
    owner_device = ((target // N_GZ) * N_GY + sender_y) * N_GZ + target % N_GZ
    new_index = (owner_device * P_NEW + pair_slot).astype(jnp.int32)
    old_index = (sender * P_OLD + pair_old).astype(jnp.int32)
    ratios = new_ratio[new_index]
    block_size = math.gcd(PAIRS, 256)

    def add_block(block_index, totals):
        start = (block_index * block_size).astype(jnp.int32)
        sources = lax.dynamic_slice_in_dim(old_index, start, block_size)
        targets = lax.dynamic_slice_in_dim(new_index, start, block_size)
        shifts = lax.dynamic_slice_in_dim(pair_shift, start, block_size)
        block_ratio = lax.dynamic_slice_in_dim(ratios, start, block_size)
        cube_data = old_data[sources].reshape(block_size, FIELDS, EDGE, EDGE, EDGE)
        weight_x = intersection_weights(shifts[:, 0], block_ratio, EDGE)
        weight_y = intersection_weights(shifts[:, 1], block_ratio, EDGE)
        weight_z = intersection_weights(shifts[:, 2], block_ratio, EDGE)
        section_x = jnp.einsum("pim,pfmnl->pfinl", weight_x, cube_data, precision=precise)
        section_y = jnp.einsum("pjn,pfinl->pfijl", weight_y, section_x, precision=precise)
        section_z = jnp.einsum("pkl,pfijl->pfijk", weight_z, section_y, precision=precise)
        return totals.at[targets].add(section_z.reshape(block_size, FIELDS, EDGE, EDGE * EDGE))

    new_data = lax.fori_loop(0, PAIRS // block_size, add_block, jnp.zeros((NEW, FIELDS, EDGE, EDGE * EDGE), jnp.float32))

    cube_view = new_data.reshape(NEW, FIELDS, EDGE, EDGE, EDGE)
    face_layers = jnp.stack([cube_view[:, :, 0], cube_view[:, :, -1], cube_view[:, :, :, 0], cube_view[:, :, :, -1], cube_view[:, :, :, :, 0], cube_view[:, :, :, :, -1]], axis=2).reshape(NEW, FIELDS, 6, EDGE * EDGE)
    opposite = face_layers.reshape(NEW, FIELDS, 3, 2, EDGE * EDGE)[:, :, :, ::-1].reshape(NEW, FIELDS, 6, EDGE * EDGE)
    device_of = jnp.arange(NEW, dtype=jnp.int32) // P_NEW
    source_device = device_of[:, None] + neighbor_side - 1
    present = (neighbor_side < 3) & (source_device >= 0) & (source_device < DEVICES)
    neighbor_index = (jnp.clip(source_device, 0, DEVICES - 1) * P_NEW + neighbor_patch).astype(jnp.int32)
    by_face = jnp.transpose(opposite, (0, 2, 1, 3))
    ghosts = by_face[neighbor_index, jnp.arange(6, dtype=jnp.int32)[None, :]]
    ghosts = jnp.transpose(ghosts, (0, 2, 1, 3))
    jumps = ghosts - face_layers
    interface_jump = jnp.where(present[:, None, :, None], jumps, jnp.zeros_like(jumps))

    total_cells = OLD * EDGE ** 3
    old_total = jnp.sum(old_data, axis=(0, 2, 3))
    ratio_cubes = new_ratio.astype(jnp.float32) ** 3
    new_total = jnp.sum(ratio_cubes[:, None] * jnp.sum(new_data, axis=(2, 3)), axis=0)
    mass_totals = jnp.stack([old_total, new_total]) / total_cells
    return new_data, interface_jump, mass_totals
```

```python
import functools

import jax
import jax.numpy as jnp
from jax import lax
from jax.experimental import pallas as pl
from jax.experimental.pallas import tpu as pltpu
from jax.sharding import Mesh
from jax.sharding import PartitionSpec as P

ALL_AXES = ("gx", "gy", "gz_0", "gz_1")
PLANE = ("gx", "gz_0")
COLUMN = ("gy", "gz_1")
UNROLL = 4
BF16 = jnp.bfloat16
F32 = jnp.float32
I32 = jnp.int32
VMEM = pltpu.VMEM
SMEM = pltpu.SMEM


def shifted(block, axis, distance):
    devices = range(lax.axis_size(axis))
    route = [(i - distance, i) for i in devices if i - distance in devices]
    return lax.ppermute(block, axis, route)


def halves(block):
    high = block.astype(BF16)
    low = (block - high.astype(F32)).astype(BF16)
    return high, low


def iota(shape, dim):
    return lax.broadcasted_iota(I32, shape, dim)


def partials_kernel(
    place, meta_own, meta_peer, ratio, own, peer,
    out_a, out_b, out_mass,
    table, split, code_k, code_x,
    *, patches, fields, edge, size_x, size_y, chips_y, cores, new_count, pairs,
):
    rows = fields * edge
    lanes = edge * edge
    half = lanes // 2
    index_y = place[0]
    core = place[1]
    size_z = chips_y * cores
    owners = size_x * chips_y * new_count

    def prepare(o, totals):
        block = own[o]
        high, low = halves(block)
        split[o, 0:rows] = high
        split[o, rows:2 * rows] = low
        high, low = halves(peer[o])
        split[patches + o, 0:rows] = high
        split[patches + o, rows:2 * rows] = low
        return totals + (block[:, :half] + block[:, half:])

    old_sums = lax.fori_loop(0, patches, prepare, jnp.zeros((rows, half), F32))

    out_a[...] = jnp.zeros_like(out_a)
    out_b[...] = jnp.zeros_like(out_b)
    cell = iota((lanes, lanes), 0)
    code_k[...] = (cell // edge) * 4096 + cell % edge
    row = iota((rows, 2 * rows), 0)
    col = iota((rows, 2 * rows), 1) % rows
    code_x[...] = (col // edge - row // edge) * 4096 + col % edge

    def enlist(p, found, meta, base):
        dest = meta[5, p]
        mine = dest % cores == core

        @pl.when(mine)
        def _():
            table[0, found] = base + meta[0, p]
            iz = dest % size_z
            ix = dest // size_z
            slot = meta[1, p]
            owner = (ix * size_y + index_y) * size_z + iz
            table[1, found] = ratio[owner * new_count + slot]
            table[2, found] = meta[2, p]
            table[3, found] = meta[3, p] * 4096 + meta[4, p]
            table[4, found] = (ix * chips_y + iz // cores) * new_count + slot
            table[5, found] = ((iz // cores) * size_x + ix) * new_count + slot

        return found + mine.astype(I32)

    found = lax.fori_loop(0, pairs, functools.partial(enlist, meta=meta_own, base=0), jnp.int32(0))
    found = lax.fori_loop(0, pairs, functools.partial(enlist, meta=meta_peer, base=patches), found)

    for extra in range(UNROLL - 1):
        table[0, found + extra] = 0
        table[1, found + extra] = 1
        table[2, found + extra] = 0
        table[3, found + extra] = 0
        table[4, found + extra] = 0
        table[5, found + extra] = 0

    lane_k = iota((1, lanes), 1)
    lane_code = (lane_k // edge) * 4096 + lane_k % edge
    row_x = iota((rows, 1), 0) % edge

    def remap(step, sums):
        results = []
        for u in range(UNROLL):
            p = step * UNROLL + u
            live = (p < found).astype(F32)
            r = table[1, p]
            inverse = jnp.where(r == 2, 0.5, 1.0).astype(F32)
            spread = code_x[...] - (row_x * r + table[2, p])
            weight_x = jnp.where((spread & ~(r - 1)) == 0, inverse, 0.0).astype(BF16)
            section = jnp.dot(weight_x, split[table[0, p]], preferred_element_type=F32)
            spread = code_k[...] - (lane_code * r + table[3, p])
            weight_k = jnp.where((spread & ~((r - 1) * 4097)) == 0, inverse * inverse, 0.0).astype(BF16)
            high, low = halves(section)
            stacked = jnp.concatenate([high, low], axis=0)
            product = jnp.dot(stacked, weight_k, preferred_element_type=F32)
            part = (product[:rows] + product[rows:]) * live
            cube = (r * r * r).astype(F32)
            sums = sums + cube * (part[:, :half] + part[:, half:])
            results.append((p, part))
        for p, part in results:
            to_a = table[4, p]
            to_b = table[5, p]
            out_a[to_a] = out_a[to_a] + part[:, :half]
            out_b[to_b] = out_b[to_b] + part[:, half:]
        return sums

    steps = (found + UNROLL - 1) // UNROLL
    new_sums = lax.fori_loop(0, steps, remap, jnp.zeros((rows, half), F32))

    lane = iota((1, half), 1)
    lines = []
    for f in range(fields):
        old_f = jnp.sum(old_sums[f * edge:(f + 1) * edge], keepdims=True)
        new_f = jnp.sum(new_sums[f * edge:(f + 1) * edge], keepdims=True)
        lines.append(jnp.where(lane == 0, old_f, jnp.where(lane == 1, new_f, 0.0)))
    lines.append(jnp.zeros((8 - fields, half), F32))
    packed = jnp.concatenate(lines, axis=0)
    out_mass[...] = jnp.broadcast_to(packed[None], out_mass.shape)


def gather_kernel(a, b, new_data, faces, *, count, fields, edge):
    rows = fields * edge
    lanes = edge * edge
    half = lanes // 2
    sources = a.shape[0]
    total_a = a[0]
    total_b = b[0]
    for s in range(1, sources):
        total_a = total_a + a[s]
        total_b = total_b + b[s]
    whole = jnp.concatenate([total_a, total_b], axis=1)
    new_data[...] = whole
    high, low = halves(whole)
    stacked = jnp.concatenate([high, low], axis=0)
    source = iota((lanes, lanes), 0)
    target = iota((lanes, lanes), 1) % edge
    here = (iota((edge, lanes), 1) // edge) == iota((edge, lanes), 0)
    picks = (
        source == target,
        source == target + (lanes - edge),
        source == target * edge,
        source == target * edge + (edge - 1),
    )
    for q in range(count):
        for f in range(fields):
            start = q * rows + f * edge
            faces[q, 0, f:f + 1, :] = whole[start:start + 1]
            faces[q, 1, f:f + 1, :] = whole[start + edge - 1:start + edge]
    for e, pick in enumerate(picks):
        weight = jnp.where(pick, 1.0, 0.0).astype(BF16)
        product = jnp.dot(stacked, weight, preferred_element_type=F32)
        layer = product[:count * rows] + product[count * rows:]
        for q in range(count):
            for f in range(fields):
                start = q * rows + f * edge
                line = jnp.sum(jnp.where(here, layer[start:start + edge], 0.0), axis=0, keepdims=True)
                faces[q, 2 + e, f:f + 1, :] = line


def jump_kernel(place, side, patch, own, before, after, jump, *, count, fields, devices):
    linear = place[2]
    for q in range(count):
        for e in range(6):
            u = side[q, e]
            n = patch[q, e]
            at = linear + u - 1
            present = (u < 3) & (at >= 0) & (at < devices)
            other = e ^ 1
            ghost = jnp.where(
                u == 0, before[n, other], jnp.where(u == 1, own[n, other], after[n, other])
            )
            line = jnp.where(present, ghost - own[q, e], 0.0)
            for f in range(fields):
                jump[q, f, e:e + 1, :] = line[f:f + 1]


def body(
    old_data, pair_old, pair_slot, pair_shift, pair_dest, new_ratio, neighbor_side, neighbor_patch
):
    patches, fields, edge, lanes = old_data.shape
    pairs = pair_old.shape[0]
    count = neighbor_side.shape[0]
    rows = fields * edge
    half = lanes // 2
    size_x = lax.axis_size("gx")
    size_y = lax.axis_size("gy")
    chips_y = lax.axis_size("gz_0")
    cores = lax.axis_size("gz_1")
    devices = size_x * size_y * chips_y * cores
    index_y = lax.axis_index("gy")
    core = lax.axis_index("gz_1")
    linear = (lax.axis_index("gx") * size_y + index_y) * chips_y * cores + lax.axis_index("gz_0") * cores + core
    place = jnp.stack([index_y, core, linear]).astype(I32)
    meta = jnp.concatenate(
        [pair_old[None], pair_slot[None], pair_shift.T, pair_dest.T], axis=0
    )
    own = old_data.reshape(patches, rows, lanes)
    swap = [(i, cores - 1 - i) for i in range(cores)]
    peer_meta = lax.ppermute(meta, "gz_1", swap)
    peer = lax.ppermute(own, "gz_1", swap)
    owners = size_x * chips_y * count
    smem = pl.BlockSpec(memory_space=SMEM)
    vmem = pl.BlockSpec(memory_space=VMEM)
    out_a, out_b, mass = pl.pallas_call(
        functools.partial(
            partials_kernel, patches=patches, fields=fields, edge=edge, size_x=size_x,
            size_y=size_y, chips_y=chips_y, cores=cores, new_count=count, pairs=pairs,
        ),
        out_shape=(
            jax.ShapeDtypeStruct((owners, rows, half), F32),
            jax.ShapeDtypeStruct((owners, rows, half), F32),
            jax.ShapeDtypeStruct((size_y * cores, 8, half), F32),
        ),
        in_specs=[smem, smem, smem, smem, vmem, vmem],
        out_specs=(vmem, vmem, vmem),
        scratch_shapes=[
            pltpu.SMEM((6, 2 * pairs + UNROLL), I32),
            pltpu.VMEM((2 * patches, 2 * rows, lanes), BF16),
            pltpu.VMEM((lanes, lanes), I32),
            pltpu.VMEM((rows, 2 * rows), I32),
        ],
        name="partials",
    )(place, meta, peer_meta, new_ratio, own, peer)

    first_a = lax.all_to_all(out_a, "gx", 0, 0, tiled=True)
    first_b = lax.all_to_all(out_b, "gz_0", 0, 0, tiled=True)
    column = lax.all_to_all(mass, COLUMN, 0, 0, tiled=True)
    column_sum = jnp.broadcast_to(jnp.sum(column, axis=0)[None], (size_x * chips_y, 8, half))
    plane = lax.all_to_all(column_sum, PLANE, 0, 0, tiled=True)
    mid_a = jnp.sum(first_a.reshape(size_x, chips_y * count * rows, half), axis=0)
    mid_b = jnp.sum(first_b.reshape(chips_y, size_x * count * rows, half), axis=0)
    last_a = lax.all_to_all(mid_a.reshape(chips_y * count, rows, half), "gz_0", 0, 0, tiled=True)
    last_b = lax.all_to_all(mid_b.reshape(size_x * count, rows, half), "gx", 0, 0, tiled=True)

    new_data, faces = pl.pallas_call(
        functools.partial(gather_kernel, count=count, fields=fields, edge=edge),
        out_shape=(
            jax.ShapeDtypeStruct((count * rows, lanes), F32),
            jax.ShapeDtypeStruct((count, 6, fields, lanes), F32),
        ),
        in_specs=[vmem, vmem],
        out_specs=(vmem, vmem),
        name="gather",
    )(
        last_a.reshape(chips_y, count * rows, half),
        last_b.reshape(size_x, count * rows, half),
    )
    before = shifted(faces, ALL_AXES, 1)
    after = shifted(faces, ALL_AXES, -1)
    interface_jump = pl.pallas_call(
        functools.partial(jump_kernel, count=count, fields=fields, devices=devices),
        out_shape=jax.ShapeDtypeStruct((count, fields, 6, lanes), F32),
        in_specs=[smem, smem, smem, vmem, vmem, vmem],
        out_specs=vmem,
        name="jump",
    )(place, neighbor_side, neighbor_patch, faces, before, after)
    total_cells = patches * devices * edge * lanes
    mass_totals = jnp.sum(plane, axis=0)[:fields, :2].T / total_cells
    return (new_data.reshape(count, fields, edge, lanes), interface_jump, mass_totals)


def solution(mesh):
    torus = Mesh(
        mesh.devices.reshape(mesh.shape["gx"], mesh.shape["gy"], 4, 2), ("gx", "gy", "gz_0", "gz_1")
    )
    return jax.shard_map(
        body,
        mesh=torus,
        in_specs=(
            P(ALL_AXES, None, None, None),
            P(ALL_AXES),
            P(ALL_AXES),
            P(ALL_AXES, None),
            P(ALL_AXES, None),
            P(),
            P(ALL_AXES, None),
            P(ALL_AXES, None),
        ),
        out_specs=(P(ALL_AXES, None, None, None), P(ALL_AXES, None, None, None), P()),
        check_vma=False,
    )
```

```python
import functools

import jax
import jax.numpy as jnp
from jax import lax
from jax.experimental import pallas as pl
from jax.experimental.pallas import tpu as pltpu
from jax.sharding import Mesh
from jax.sharding import PartitionSpec as P


ALL_AXES = ("gx", "gy", "gz_0", "gz_1")
PLANE = ("gx", "gz_0")
UNROLL = 4
BF16 = jnp.bfloat16
F32 = jnp.float32
I32 = jnp.int32
VMEM = pltpu.VMEM
SMEM = pltpu.SMEM


def shifted(block, axis, distance):
    devices = range(lax.axis_size(axis))
    route = [(i - distance, i) for i in devices if i - distance in devices]
    return lax.ppermute(block, axis, route)


def rotated(block, axis, distance):
    size = lax.axis_size(axis)
    return lax.ppermute(block, axis, [(i, (i + distance) % size) for i in range(size)])


def crossed(block, axis, distance):
    return block + lax.ppermute(block, axis, [(i, i ^ distance) for i in range(lax.axis_size(axis))])


def fast(block):
    return pltpu.with_memory_space_constraint(block, VMEM)


def halves(block):
    high = block.astype(BF16)
    low = (block - high.astype(F32)).astype(BF16)
    return high, low


def iota(shape, dim):
    return lax.broadcasted_iota(I32, shape, dim)


def mass_kernel(place, meta, ratio, own, out, counts, *, patches, fields, edge, size_y, size_z, new_count, pairs):
    lanes = edge * edge
    half = lanes // 2
    index_y = place[0]
    counts[...] = jnp.zeros_like(counts)
    at_x = iota((edge, lanes), 0)
    at_y = iota((edge, lanes), 1) // edge
    at_z = iota((edge, lanes), 1) % edge

    def count(p, carry):
        dest = meta[5, p]
        owner = ((dest // size_z) * size_y + index_y) * size_z + dest % size_z
        reach = edge * ratio[owner * new_count + meta[1, p]]
        hit = jnp.full((edge, lanes), True)
        for a, at in enumerate((at_x, at_y, at_z)):
            distance = at - meta[2 + a, p]
            hit = hit & (distance >= 0) & (distance < reach)
        o = meta[0, p]
        counts[o] = counts[o] + jnp.where(hit, 1.0, 0.0)
        return carry

    lax.fori_loop(0, pairs, count, 0)

    def add(o, sums):
        weight = counts[o]
        olds, news = sums
        old_list, new_list = [], []
        for f in range(fields):
            block = own[o, f * edge:(f + 1) * edge]
            scaled = block * weight
            old_list.append(olds[f] + (block[:, :half] + block[:, half:]))
            new_list.append(news[f] + (scaled[:, :half] + scaled[:, half:]))
        return tuple(old_list), tuple(new_list)

    zero = tuple(jnp.zeros((edge, half), F32) for _ in range(fields))
    olds, news = lax.fori_loop(0, patches, add, (zero, zero))
    lane = iota((1, half), 1)
    lines = []
    for f in range(fields):
        old_f = jnp.sum(olds[f], keepdims=True)
        new_f = jnp.sum(news[f], keepdims=True)
        lines.append(jnp.where(lane == 0, old_f, jnp.where(lane == 1, new_f, 0.0)))
    lines.append(jnp.zeros((8 - fields, half), F32))
    packed = jnp.concatenate(lines, axis=0)
    out[...] = jnp.broadcast_to(packed[None], out.shape)


def partials_kernel(
    place, meta_own, meta_peer, ratio, own, peer,
    out_a, out_b0, out_b1, out_b2, out_b3,
    out_b, table, split, code_k, code_x,
    *, patches, fields, edge, size_x, size_y, chips_y, cores, new_count, pairs,
):
    rows = fields * edge
    lanes = edge * edge
    half = lanes // 2
    index_y = place[0]
    core = place[1]
    index_x = place[3]
    chip_y = place[4]
    size_z = chips_y * cores

    def prepare(o, carry):
        high, low = halves(own[o])
        split[o, 0:rows] = high
        split[o, rows:2 * rows] = low
        high, low = halves(peer[o])
        split[patches + o, 0:rows] = high
        split[patches + o, rows:2 * rows] = low
        return carry

    lax.fori_loop(0, patches, prepare, 0)

    out_a[...] = jnp.zeros_like(out_a)
    out_b[...] = jnp.zeros_like(out_b)
    cell = iota((lanes, lanes), 0)
    code_k[...] = (cell // edge) * 4096 + cell % edge
    row = iota((rows, 2 * rows), 0)
    col = iota((rows, 2 * rows), 1) % rows
    code_x[...] = (col // edge - row // edge) * 4096 + col % edge

    def enlist(p, found, meta, base):
        dest = meta[5, p]
        mine = dest % cores == core

        @pl.when(mine)
        def _():
            table[0, found] = base + meta[0, p]
            iz = dest % size_z
            ix = dest // size_z
            slot = meta[1, p]
            owner = (ix * size_y + index_y) * size_z + iz
            table[1, found] = ratio[owner * new_count + slot]
            table[2, found] = meta[2, p]
            table[3, found] = meta[3, p] * 4096 + meta[4, p]
            table[4, found] = (ix * chips_y + iz // cores) * new_count + slot
            step_y = (iz // cores - chip_y) & (chips_y - 1)
            step_x = (ix - index_x) & (size_x - 1)
            table[5, found] = (step_y * size_x + step_x) * new_count + slot

        return found + mine.astype(I32)

    found = lax.fori_loop(0, pairs, functools.partial(enlist, meta=meta_own, base=0), jnp.int32(0))
    found = lax.fori_loop(0, pairs, functools.partial(enlist, meta=meta_peer, base=patches), found)

    for extra in range(UNROLL - 1):
        table[0, found + extra] = 0
        table[1, found + extra] = 1
        table[2, found + extra] = 0
        table[3, found + extra] = 0
        table[4, found + extra] = 0
        table[5, found + extra] = 0

    lane_k = iota((1, lanes), 1)
    lane_code = (lane_k // edge) * 4096 + lane_k % edge
    row_x = iota((rows, 1), 0) % edge

    def remap(step, carry):
        results = []
        for u in range(UNROLL):
            p = step * UNROLL + u
            live = (p < found).astype(F32)
            r = table[1, p]
            inverse = jnp.where(r == 2, 0.5, 1.0).astype(F32)
            spread = code_x[...] - (row_x * r + table[2, p])
            weight_x = jnp.where((spread & ~(r - 1)) == 0, inverse, 0.0).astype(BF16)
            section = jnp.dot(weight_x, split[table[0, p]], preferred_element_type=F32)
            spread = code_k[...] - (lane_code * r + table[3, p])
            weight_k = jnp.where((spread & ~((r - 1) * 4097)) == 0, inverse * inverse, 0.0).astype(BF16)
            high, low = halves(section)
            stacked = jnp.concatenate([high, low], axis=0)
            product = jnp.dot(stacked, weight_k, preferred_element_type=F32)
            part = (product[:rows] + product[rows:]) * live
            results.append((p, part))
        for p, part in results:
            to_a = table[4, p]
            to_b = table[5, p]
            out_a[to_a] = out_a[to_a] + part[:, :half]
            out_b[to_b] = out_b[to_b] + part[:, half:]
        return carry

    steps = (found + UNROLL - 1) // UNROLL
    lax.fori_loop(0, steps, remap, 0)
    chunk = size_x * new_count
    for k, out in enumerate((out_b0, out_b1, out_b2, out_b3)):
        out[...] = out_b[k * chunk:(k + 1) * chunk]


def fold_kernel(a, out):
    total = a[0]
    for s in range(1, a.shape[0]):
        total = total + a[s]
    out[...] = total


def cross_kernel(b0, b1, b2, b3, *outs):
    count = outs[0].shape[0]
    for k, out in enumerate(outs):
        at = slice(k * count, (k + 1) * count)
        out[...] = (b0[at] + b1[at]) + (b2[at] + b3[at])


def gather_kernel(a, b0, b1, b2, b3, new_data, faces, *, count, fields, edge):
    rows = fields * edge
    lanes = edge * edge
    sources = a.shape[0]
    total_a = a[0]
    total_b = (b0[...] + b1[...]) + (b2[...] + b3[...])
    for s in range(1, sources):
        total_a = total_a + a[s]
    whole = jnp.concatenate([total_a, total_b], axis=1)
    new_data[...] = whole
    high, low = halves(whole)
    stacked = jnp.concatenate([high, low], axis=0)
    source = iota((lanes, lanes), 0)
    target = iota((lanes, lanes), 1) % edge
    here = (iota((edge, lanes), 1) // edge) == iota((edge, lanes), 0)
    picks = (
        source == target,
        source == target + (lanes - edge),
        source == target * edge,
        source == target * edge + (edge - 1),
    )
    for q in range(count):
        for f in range(fields):
            start = q * rows + f * edge
            faces[q, 0, f:f + 1, :] = whole[start:start + 1]
            faces[q, 1, f:f + 1, :] = whole[start + edge - 1:start + edge]
    for e, pick in enumerate(picks):
        weight = jnp.where(pick, 1.0, 0.0).astype(BF16)
        product = jnp.dot(stacked, weight, preferred_element_type=F32)
        layer = product[:count * rows] + product[count * rows:]
        for q in range(count):
            for f in range(fields):
                start = q * rows + f * edge
                line = jnp.sum(jnp.where(here, layer[start:start + edge], 0.0), axis=0, keepdims=True)
                faces[q, 2 + e, f:f + 1, :] = line


def jump_kernel(place, side, patch, own, before, after, jump, *, count, fields, devices):
    linear = place[2]
    for q in range(count):
        for e in range(6):
            u = side[q, e]
            n = patch[q, e]
            at = linear + u - 1
            present = (u < 3) & (at >= 0) & (at < devices)
            other = e ^ 1
            ghost = jnp.where(
                u == 0, before[n, other], jnp.where(u == 1, own[n, other], after[n, other])
            )
            line = jnp.where(present, ghost - own[q, e], 0.0)
            for f in range(fields):
                jump[q, f, e:e + 1, :] = line[f:f + 1]


def body(
    old_data, pair_old, pair_slot, pair_shift, pair_dest, new_ratio, neighbor_side, neighbor_patch
):
    patches, fields, edge, lanes = old_data.shape
    pairs = pair_old.shape[0]
    count = neighbor_side.shape[0]
    rows = fields * edge
    half = lanes // 2
    size_x = lax.axis_size("gx")
    size_y = lax.axis_size("gy")
    chips_y = lax.axis_size("gz_0")
    cores = lax.axis_size("gz_1")
    devices = size_x * size_y * chips_y * cores
    index_y = lax.axis_index("gy")
    core = lax.axis_index("gz_1")
    index_x = lax.axis_index("gx")
    chip_y = lax.axis_index("gz_0")
    linear = ((index_x * size_y + index_y) * chips_y + chip_y) * cores + core
    place = jnp.stack([index_y, core, linear, index_x, chip_y]).astype(I32)
    meta = jnp.concatenate(
        [pair_old[None], pair_slot[None], pair_shift.T, pair_dest.T], axis=0
    )
    own = old_data.reshape(patches, rows, lanes)
    swap = [(i, cores - 1 - i) for i in range(cores)]
    peer_meta = lax.ppermute(meta, "gz_1", swap)
    peer = lax.ppermute(own, "gz_1", swap)
    owners = size_x * chips_y * count
    chunk = owners // chips_y
    smem = pl.BlockSpec(memory_space=SMEM)
    vmem = pl.BlockSpec(memory_space=VMEM)
    params = pltpu.CompilerParams(vmem_limit_bytes=24 * 1024 * 1024)
    mass = pl.pallas_call(
        functools.partial(
            mass_kernel, patches=patches, fields=fields, edge=edge, size_y=size_y,
            size_z=chips_y * cores, new_count=count, pairs=pairs,
        ),
        out_shape=VMEM((size_x * chips_y, 8, half), F32),
        in_specs=[smem, smem, smem, vmem],
        out_specs=vmem,
        scratch_shapes=[pltpu.VMEM((patches, edge, lanes), F32)],
        compiler_params=params,
        name="mass",
    )(place, meta, new_ratio, own)
    plane = lax.all_to_all(mass, PLANE, 0, 0, tiled=True)
    out_a, *out_b = pl.pallas_call(
        functools.partial(
            partials_kernel, patches=patches, fields=fields, edge=edge, size_x=size_x,
            size_y=size_y, chips_y=chips_y, cores=cores, new_count=count, pairs=pairs,
        ),
        out_shape=(VMEM((owners, rows, half), F32),)
        + (VMEM((chunk, rows, half), F32),) * chips_y,
        in_specs=[smem, smem, smem, smem, vmem, vmem],
        out_specs=(vmem,) * (1 + chips_y),
        scratch_shapes=[
            pltpu.VMEM((owners, rows, half), F32),
            pltpu.SMEM((6, 2 * pairs + UNROLL), I32),
            pltpu.VMEM((2 * patches, 2 * rows, lanes), BF16),
            pltpu.VMEM((lanes, lanes), I32),
            pltpu.VMEM((rows, 2 * rows), I32),
        ],
        compiler_params=params,
        name="partials",
    )(place, meta, peer_meta, new_ratio, own, fast(peer))

    first_a = lax.all_to_all(out_a, "gx", 0, 0, tiled=True)
    for k in (1, 3, 2):
        out_b[k] = rotated(out_b[k], "gz_0", k)
    total = jnp.sum(plane, axis=0)
    total = crossed(total, "gz_1", 1)
    distance = 1
    while distance < size_y:
        total = crossed(total, "gy", distance)
        distance = distance * 2
    mid_a = pl.pallas_call(
        fold_kernel,
        out_shape=VMEM((chips_y * count, rows, half), F32),
        in_specs=[vmem],
        out_specs=vmem,
        compiler_params=params,
        name="fold",
    )(fast(first_a.reshape(size_x, chips_y * count, rows, half)))
    last_a = lax.all_to_all(mid_a, "gz_0", 0, 0, tiled=True)
    mid_b = list(pl.pallas_call(
        cross_kernel,
        out_shape=(VMEM((count, rows, half), F32),) * size_x,
        in_specs=[vmem] * chips_y,
        out_specs=(vmem,) * size_x,
        compiler_params=params,
        name="cross",
    )(*[fast(b) for b in out_b]))
    for k in (1, 3, 2):
        mid_b[k] = rotated(mid_b[k], "gx", k)

    new_data, faces = pl.pallas_call(
        functools.partial(gather_kernel, count=count, fields=fields, edge=edge),
        out_shape=(
            jax.ShapeDtypeStruct((count * rows, lanes), F32),
            VMEM((count, 6, fields, lanes), F32),
        ),
        in_specs=[vmem] * (1 + size_x),
        out_specs=(vmem, vmem),
        compiler_params=params,
        name="gather",
    )(
        fast(last_a.reshape(chips_y, count * rows, half)),
        *[fast(b.reshape(count * rows, half)) for b in mid_b],
    )
    before = shifted(faces, ALL_AXES, 1)
    after = shifted(faces, ALL_AXES, -1)
    interface_jump = pl.pallas_call(
        functools.partial(jump_kernel, count=count, fields=fields, devices=devices),
        out_shape=jax.ShapeDtypeStruct((count, fields, 6, lanes), F32),
        in_specs=[smem, smem, smem, vmem, vmem, vmem],
        out_specs=vmem,
        name="jump",
    )(place, neighbor_side, neighbor_patch, fast(faces), fast(before), fast(after))
    total_cells = patches * devices * edge * lanes
    mass_totals = total[:fields, :2].T / total_cells
    return (new_data.reshape(count, fields, edge, lanes), interface_jump, mass_totals)


def solution(mesh):
    torus = Mesh(
        mesh.devices.reshape(mesh.shape["gx"], mesh.shape["gy"], 4, 2), ("gx", "gy", "gz_0", "gz_1")
    )
    return jax.shard_map(
        body,
        mesh=torus,
        in_specs=(
            P(ALL_AXES, None, None, None),
            P(ALL_AXES),
            P(ALL_AXES),
            P(ALL_AXES, None),
            P(ALL_AXES, None),
            P(),
            P(ALL_AXES, None),
            P(ALL_AXES, None),
        ),
        out_specs=(P(ALL_AXES, None, None, None), P(ALL_AXES, None, None, None), P()),
        check_vma=False,
    )
```

```python
import functools

import jax
import jax.numpy as jnp
from jax import lax
from jax.experimental import pallas as pl
from jax.experimental.pallas import tpu as pltpu
from jax.sharding import Mesh
from jax.sharding import PartitionSpec as P


ALL_AXES = ("gx", "gy", "gz_0", "gz_1")
PLANE = ("gx", "gz_0")
UNROLL = 4
BF16 = jnp.bfloat16
F32 = jnp.float32
I32 = jnp.int32
VMEM = pltpu.VMEM
SMEM = pltpu.SMEM


def shifted(block, axis, distance):
    devices = range(lax.axis_size(axis))
    route = [(i - distance, i) for i in devices if i - distance in devices]
    return lax.ppermute(block, axis, route)


def crossed(block, axis, distance):
    return block + lax.ppermute(block, axis, [(i, i ^ distance) for i in range(lax.axis_size(axis))])


def fast(block):
    return pltpu.with_memory_space_constraint(block, VMEM)


def mixed_groups(size_x, size_y, chips_y, cores):
    def device(x, z, y, c):
        return ((x * size_y + z) * chips_y + y) * cores + c

    along_x, along_y = [], []
    for c in range(cores):
        lines_x = [[device(x, z, y, c) for x in range(size_x)] for z in range(size_y) for y in range(chips_y)]
        lines_y = [[device(x, z, y, c) for y in range(chips_y)] for z in range(size_y) for x in range(size_x)]
        along_x += lines_x if c == 0 else lines_y
        along_y += lines_y if c == 0 else lines_x
    return along_x, along_y


def halves(block):
    high = block.astype(BF16)
    low = (block - high.astype(F32)).astype(BF16)
    return high, low


def iota(shape, dim):
    return lax.broadcasted_iota(I32, shape, dim)


def mass_kernel(place, meta, ratio, own, out, counts, *, patches, fields, edge, size_y, size_z, new_count, pairs):
    lanes = edge * edge
    half = lanes // 2
    index_y = place[0]
    counts[...] = jnp.zeros_like(counts)
    at_x = iota((edge, lanes), 0)
    at_y = iota((edge, lanes), 1) // edge
    at_z = iota((edge, lanes), 1) % edge

    def count(p, carry):
        dest = meta[5, p]
        owner = ((dest // size_z) * size_y + index_y) * size_z + dest % size_z
        reach = edge * ratio[owner * new_count + meta[1, p]]
        hit = jnp.full((edge, lanes), True)
        for a, at in enumerate((at_x, at_y, at_z)):
            distance = at - meta[2 + a, p]
            hit = hit & (distance >= 0) & (distance < reach)
        o = meta[0, p]
        counts[o] = counts[o] + jnp.where(hit, 1.0, 0.0)
        return carry

    lax.fori_loop(0, pairs, count, 0)

    def add(o, sums):
        weight = counts[o]
        olds, news = sums
        old_list, new_list = [], []
        for f in range(fields):
            block = own[o, f * edge:(f + 1) * edge]
            scaled = block * weight
            old_list.append(olds[f] + (block[:, :half] + block[:, half:]))
            new_list.append(news[f] + (scaled[:, :half] + scaled[:, half:]))
        return tuple(old_list), tuple(new_list)

    zero = tuple(jnp.zeros((edge, half), F32) for _ in range(fields))
    olds, news = lax.fori_loop(0, patches, add, (zero, zero))
    lane = iota((1, half), 1)
    lines = []
    for f in range(fields):
        old_f = jnp.sum(olds[f], keepdims=True)
        new_f = jnp.sum(news[f], keepdims=True)
        lines.append(jnp.where(lane == 0, old_f, jnp.where(lane == 1, new_f, 0.0)))
    lines.append(jnp.zeros((8 - fields, half), F32))
    packed = jnp.concatenate(lines, axis=0)
    out[...] = jnp.broadcast_to(packed[None], out.shape)


def partials_kernel(
    place, meta_own, meta_peer, ratio, own, peer,
    out, table, split, code_k, code_x,
    *, patches, fields, edge, size_x, size_y, chips_y, cores, new_count, pairs,
):
    rows = fields * edge
    lanes = edge * edge
    index_y = place[0]
    core = place[1]
    size_z = chips_y * cores

    def prepare(o, carry):
        high, low = halves(own[o])
        split[o, 0:rows] = high
        split[o, rows:2 * rows] = low
        high, low = halves(peer[o])
        split[patches + o, 0:rows] = high
        split[patches + o, rows:2 * rows] = low
        return carry

    lax.fori_loop(0, patches, prepare, 0)

    out[...] = jnp.zeros_like(out)
    cell = iota((lanes, lanes), 0)
    code_k[...] = (cell // edge) * 4096 + cell % edge
    row = iota((rows, 2 * rows), 0)
    col = iota((rows, 2 * rows), 1) % rows
    code_x[...] = (col // edge - row // edge) * 4096 + col % edge

    def enlist(p, found, meta, base):
        dest = meta[5, p]
        mine = dest % cores == core

        @pl.when(mine)
        def _():
            table[0, found] = base + meta[0, p]
            iz = dest % size_z
            ix = dest // size_z
            slot = meta[1, p]
            owner = (ix * size_y + index_y) * size_z + iz
            table[1, found] = ratio[owner * new_count + slot]
            table[2, found] = meta[2, p]
            table[3, found] = meta[3, p] * 4096 + meta[4, p]
            chip_y = iz // cores
            chip = jnp.where(core == 0, ix * chips_y + chip_y, chip_y * size_x + ix)
            table[4, found] = chip * new_count + slot

        return found + mine.astype(I32)

    found = lax.fori_loop(0, pairs, functools.partial(enlist, meta=meta_own, base=0), jnp.int32(0))
    found = lax.fori_loop(0, pairs, functools.partial(enlist, meta=meta_peer, base=patches), found)

    for extra in range(UNROLL - 1):
        table[0, found + extra] = 0
        table[1, found + extra] = 1
        table[2, found + extra] = 0
        table[3, found + extra] = 0
        table[4, found + extra] = 0

    lane_k = iota((1, lanes), 1)
    lane_code = (lane_k // edge) * 4096 + lane_k % edge
    row_x = iota((rows, 1), 0) % edge

    def remap(step, carry):
        results = []
        for u in range(UNROLL):
            p = step * UNROLL + u
            live = (p < found).astype(F32)
            r = table[1, p]
            inverse = jnp.where(r == 2, 0.5, 1.0).astype(F32)
            spread = code_x[...] - (row_x * r + table[2, p])
            weight_x = jnp.where((spread & ~(r - 1)) == 0, inverse, 0.0).astype(BF16)
            section = jnp.dot(weight_x, split[table[0, p]], preferred_element_type=F32)
            spread = code_k[...] - (lane_code * r + table[3, p])
            weight_k = jnp.where((spread & ~((r - 1) * 4097)) == 0, inverse * inverse, 0.0).astype(BF16)
            high, low = halves(section)
            stacked = jnp.concatenate([high, low], axis=0)
            product = jnp.dot(stacked, weight_k, preferred_element_type=F32)
            part = (product[:rows] + product[rows:]) * live
            results.append((p, part))
        for p, part in results:
            to = table[4, p]
            out[to] = out[to] + part
        return carry

    steps = (found + UNROLL - 1) // UNROLL
    lax.fori_loop(0, steps, remap, 0)


def fold_kernel(a, out):
    total = a[0]
    for s in range(1, a.shape[0]):
        total = total + a[s]
    out[...] = total


def gather_kernel(a, new_data, faces, *, count, fields, edge):
    rows = fields * edge
    lanes = edge * edge
    whole = a[0]
    for s in range(1, a.shape[0]):
        whole = whole + a[s]
    new_data[...] = whole
    high, low = halves(whole)
    stacked = jnp.concatenate([high, low], axis=0)
    source = iota((lanes, lanes), 0)
    target = iota((lanes, lanes), 1) % edge
    here = (iota((edge, lanes), 1) // edge) == iota((edge, lanes), 0)
    picks = (
        source == target,
        source == target + (lanes - edge),
        source == target * edge,
        source == target * edge + (edge - 1),
    )
    for q in range(count):
        for f in range(fields):
            start = q * rows + f * edge
            faces[q, 0, f:f + 1, :] = whole[start:start + 1]
            faces[q, 1, f:f + 1, :] = whole[start + edge - 1:start + edge]
    for e, pick in enumerate(picks):
        weight = jnp.where(pick, 1.0, 0.0).astype(BF16)
        product = jnp.dot(stacked, weight, preferred_element_type=F32)
        layer = product[:count * rows] + product[count * rows:]
        for q in range(count):
            for f in range(fields):
                start = q * rows + f * edge
                line = jnp.sum(jnp.where(here, layer[start:start + edge], 0.0), axis=0, keepdims=True)
                faces[q, 2 + e, f:f + 1, :] = line


def jump_kernel(place, side, patch, own, before, after, jump, *, count, fields, devices):
    linear = place[2]
    for q in range(count):
        for e in range(6):
            u = side[q, e]
            n = patch[q, e]
            at = linear + u - 1
            present = (u < 3) & (at >= 0) & (at < devices)
            other = e ^ 1
            ghost = jnp.where(
                u == 0, before[n, other], jnp.where(u == 1, own[n, other], after[n, other])
            )
            line = jnp.where(present, ghost - own[q, e], 0.0)
            for f in range(fields):
                jump[q, f, e:e + 1, :] = line[f:f + 1]


def body(
    old_data, pair_old, pair_slot, pair_shift, pair_dest, new_ratio, neighbor_side, neighbor_patch
):
    patches, fields, edge, lanes = old_data.shape
    pairs = pair_old.shape[0]
    count = neighbor_side.shape[0]
    rows = fields * edge
    half = lanes // 2
    size_x = lax.axis_size("gx")
    size_y = lax.axis_size("gy")
    chips_y = lax.axis_size("gz_0")
    cores = lax.axis_size("gz_1")
    devices = size_x * size_y * chips_y * cores
    index_y = lax.axis_index("gy")
    core = lax.axis_index("gz_1")
    index_x = lax.axis_index("gx")
    chip_y = lax.axis_index("gz_0")
    linear = ((index_x * size_y + index_y) * chips_y + chip_y) * cores + core
    place = jnp.stack([index_y, core, linear, index_x, chip_y]).astype(I32)
    meta = jnp.concatenate(
        [pair_old[None], pair_slot[None], pair_shift.T, pair_dest.T], axis=0
    )
    own = old_data.reshape(patches, rows, lanes)
    swap = [(i, cores - 1 - i) for i in range(cores)]
    peer_meta = lax.ppermute(meta, "gz_1", swap)
    peer = lax.ppermute(own, "gz_1", swap)
    owners = size_x * chips_y * count
    smem = pl.BlockSpec(memory_space=SMEM)
    vmem = pl.BlockSpec(memory_space=VMEM)
    params = pltpu.CompilerParams(vmem_limit_bytes=24 * 1024 * 1024)
    mass = pl.pallas_call(
        functools.partial(
            mass_kernel, patches=patches, fields=fields, edge=edge, size_y=size_y,
            size_z=chips_y * cores, new_count=count, pairs=pairs,
        ),
        out_shape=VMEM((size_x * chips_y, 8, half), F32),
        in_specs=[smem, smem, smem, vmem],
        out_specs=vmem,
        scratch_shapes=[pltpu.VMEM((patches, edge, lanes), F32)],
        compiler_params=params,
        name="mass",
    )(place, meta, new_ratio, own)
    plane = lax.all_to_all(mass, PLANE, 0, 0, tiled=True)
    partials = pl.pallas_call(
        functools.partial(
            partials_kernel, patches=patches, fields=fields, edge=edge, size_x=size_x,
            size_y=size_y, chips_y=chips_y, cores=cores, new_count=count, pairs=pairs,
        ),
        out_shape=jax.ShapeDtypeStruct((owners, rows, lanes), F32),
        in_specs=[smem, smem, smem, smem, vmem, vmem],
        out_specs=vmem,
        scratch_shapes=[
            pltpu.SMEM((5, 2 * pairs + UNROLL), I32),
            pltpu.VMEM((2 * patches, 2 * rows, lanes), BF16),
            pltpu.VMEM((lanes, lanes), I32),
            pltpu.VMEM((rows, 2 * rows), I32),
        ],
        compiler_params=params,
        name="partials",
    )(place, meta, peer_meta, new_ratio, own, fast(peer))

    first_groups, last_groups = mixed_groups(size_x, size_y, chips_y, cores)
    first = lax.all_to_all(partials, ALL_AXES, 0, 0, tiled=True, axis_index_groups=first_groups)
    total = jnp.sum(plane, axis=0)
    total = crossed(total, "gz_1", 1)
    distance = 1
    while distance < size_y:
        total = crossed(total, "gy", distance)
        distance = distance * 2
    folded = pl.pallas_call(
        fold_kernel,
        out_shape=VMEM((owners // size_x, rows, lanes), F32),
        in_specs=[vmem],
        out_specs=vmem,
        compiler_params=params,
        name="fold",
    )(fast(first.reshape(size_x, owners // size_x, rows, lanes)))
    last = lax.all_to_all(folded, ALL_AXES, 0, 0, tiled=True, axis_index_groups=last_groups)
    new_data, faces = pl.pallas_call(
        functools.partial(gather_kernel, count=count, fields=fields, edge=edge),
        out_shape=(
            jax.ShapeDtypeStruct((count * rows, lanes), F32),
            VMEM((count, 6, fields, lanes), F32),
        ),
        in_specs=[vmem],
        out_specs=(vmem, vmem),
        compiler_params=params,
        name="gather",
    )(fast(last.reshape(chips_y, count * rows, lanes)))
    before = shifted(faces, ALL_AXES, 1)
    after = shifted(faces, ALL_AXES, -1)
    interface_jump = pl.pallas_call(
        functools.partial(jump_kernel, count=count, fields=fields, devices=devices),
        out_shape=jax.ShapeDtypeStruct((count, fields, 6, lanes), F32),
        in_specs=[smem, smem, smem, vmem, vmem, vmem],
        out_specs=vmem,
        name="jump",
    )(place, neighbor_side, neighbor_patch, fast(faces), fast(before), fast(after))
    total_cells = patches * devices * edge * lanes
    mass_totals = total[:fields, :2].T / total_cells
    return (new_data.reshape(count, fields, edge, lanes), interface_jump, mass_totals)


def solution(mesh):
    torus = Mesh(
        mesh.devices.reshape(mesh.shape["gx"], mesh.shape["gy"], 4, 2), ("gx", "gy", "gz_0", "gz_1")
    )
    return jax.shard_map(
        body,
        mesh=torus,
        in_specs=(
            P(ALL_AXES, None, None, None),
            P(ALL_AXES),
            P(ALL_AXES),
            P(ALL_AXES, None),
            P(ALL_AXES, None),
            P(),
            P(ALL_AXES, None),
            P(ALL_AXES, None),
        ),
        out_specs=(P(ALL_AXES, None, None, None), P(ALL_AXES, None, None, None), P()),
        check_vma=False,
    )
```

```python
import functools

import jax
import jax.numpy as jnp
from jax import lax
from jax.experimental import pallas as pl
from jax.experimental.pallas import tpu as pltpu
from jax.sharding import Mesh
from jax.sharding import PartitionSpec as P


ALL_AXES = ("gx", "gy", "gz_0", "gz_1")
UNROLL = 4
BF16 = jnp.bfloat16
F32 = jnp.float32
I32 = jnp.int32
VMEM = pltpu.VMEM
SMEM = pltpu.SMEM
HBM = pltpu.HBM
DMA = pltpu.SemaphoreType.DMA


def shifted(block, axis, distance):
    devices = range(lax.axis_size(axis))
    route = [(i - distance, i) for i in devices if i - distance in devices]
    return lax.ppermute(block, axis, route)


def fast(block):
    return pltpu.with_memory_space_constraint(block, VMEM)


def mixed_groups(size_x, size_y, chips_y, cores):
    def device(x, z, y, c):
        return ((x * size_y + z) * chips_y + y) * cores + c

    along_x, along_y = [], []
    for c in range(cores):
        lines_x = [[device(x, z, y, c) for x in range(size_x)] for z in range(size_y) for y in range(chips_y)]
        lines_y = [[device(x, z, y, c) for y in range(chips_y)] for z in range(size_y) for x in range(size_x)]
        along_x += lines_x if c == 0 else lines_y
        along_y += lines_y if c == 0 else lines_x
    return along_x, along_y


def mixed_steps(size_x, size_y, chips_y, cores):
    shape = (size_x, size_y, chips_y, cores)
    spots = [
        (x, z, y, c) for x in range(size_x) for z in range(size_y) for y in range(chips_y) for c in range(cores)
    ]

    def number(spot):
        at = 0
        for size, i in zip(shape, spot):
            at = at * size + i
        return at

    def step(across, distance):
        def other(spot):
            axis = (2 if spot[3] == 0 else 0) if across else (0 if spot[3] == 0 else 2)
            return tuple(i ^ distance if n == axis else i for n, i in enumerate(spot))

        return [(number(spot), number(other(spot))) for spot in spots]

    steps = [step(across, distance) for across in (True, False) for distance in (1, 2)]
    steps.append([(number(spot), number((*spot[:3], spot[3] ^ 1))) for spot in spots])
    return steps


def slow(block):
    return pltpu.with_memory_space_constraint(block, HBM)


def halves(block):
    high = block.astype(BF16)
    low = (block - high.astype(F32)).astype(BF16)
    return high, low


def iota(shape, dim):
    return lax.broadcasted_iota(I32, shape, dim)


def mass_kernel(place, meta, ratio_in, own_in, out, ratio, own, counts, sems, *, patches, fields, edge, size_y, size_z, new_count, pairs):
    lanes = edge * edge
    half = lanes // 2
    index_y = place[0]
    ratio_copy = pltpu.make_async_copy(ratio_in, ratio, sems.at[0])
    own_copy = pltpu.make_async_copy(own_in, own, sems.at[1])
    ratio_copy.start()
    own_copy.start()
    counts[...] = jnp.zeros_like(counts)
    at_x = iota((edge, lanes), 0)
    at_y = iota((edge, lanes), 1) // edge
    at_z = iota((edge, lanes), 1) % edge

    def count(p, carry):
        dest = meta[5, p]
        owner = ((dest // size_z) * size_y + index_y) * size_z + dest % size_z
        reach = edge * ratio[owner * new_count + meta[1, p]]
        hit = jnp.full((edge, lanes), True)
        for a, at in enumerate((at_x, at_y, at_z)):
            distance = at - meta[2 + a, p]
            hit = hit & (distance >= 0) & (distance < reach)
        o = meta[0, p]
        counts[o] = counts[o] + jnp.where(hit, 1.0, 0.0)
        return carry

    ratio_copy.wait()
    lax.fori_loop(0, pairs, count, 0)
    own_copy.wait()

    def add(o, sums):
        weight = counts[o]
        olds, news = sums
        old_list, new_list = [], []
        for f in range(fields):
            block = own[o, f * edge:(f + 1) * edge]
            scaled = block * weight
            old_list.append(olds[f] + (block[:, :half] + block[:, half:]))
            new_list.append(news[f] + (scaled[:, :half] + scaled[:, half:]))
        return tuple(old_list), tuple(new_list)

    zero = tuple(jnp.zeros((edge, half), F32) for _ in range(fields))
    olds, news = lax.fori_loop(0, patches, add, (zero, zero))
    lane = iota((1, half), 1)
    lines = []
    for f in range(fields):
        old_f = jnp.sum(olds[f], keepdims=True)
        new_f = jnp.sum(news[f], keepdims=True)
        lines.append(jnp.where(lane == 0, old_f, jnp.where(lane == 1, new_f, 0.0)))
    lines.append(jnp.zeros((8 - fields, half), F32))
    packed = jnp.concatenate(lines, axis=0)
    out[...] = jnp.broadcast_to(packed[None], out.shape)


def partials_kernel(
    place, meta_own, meta_peer, ratio_in, own_in, peer,
    out, ratio, own, table, split, code_k, code_x, sems,
    *, patches, fields, edge, size_x, size_y, chips_y, cores, new_count, pairs,
):
    rows = fields * edge
    lanes = edge * edge
    index_y = place[0]
    core = place[1]
    size_z = chips_y * cores
    ratio_copy = pltpu.make_async_copy(ratio_in, ratio, sems.at[0])
    own_copy = pltpu.make_async_copy(own_in, own, sems.at[1])
    ratio_copy.start()
    own_copy.start()

    def prepare(o, carry):
        high, low = halves(own[o])
        split[o, 0:rows] = high
        split[o, rows:2 * rows] = low
        high, low = halves(peer[o])
        split[patches + o, 0:rows] = high
        split[patches + o, rows:2 * rows] = low
        return carry

    out[...] = jnp.zeros_like(out)
    cell = iota((lanes, lanes), 0)
    code_k[...] = (cell // edge) * 4096 + cell % edge
    row = iota((rows, 2 * rows), 0)
    col = iota((rows, 2 * rows), 1) % rows
    code_x[...] = (col // edge - row // edge) * 4096 + col % edge

    def enlist(p, found, meta, base):
        dest = meta[5, p]
        mine = dest % cores == core

        @pl.when(mine)
        def _():
            table[0, found] = base + meta[0, p]
            iz = dest % size_z
            ix = dest // size_z
            slot = meta[1, p]
            owner = (ix * size_y + index_y) * size_z + iz
            table[1, found] = ratio[owner * new_count + slot]
            table[2, found] = meta[2, p]
            table[3, found] = meta[3, p] * 4096 + meta[4, p]
            chip_y = iz // cores
            chip = jnp.where(core == 0, ix * chips_y + chip_y, chip_y * size_x + ix)
            table[4, found] = chip * new_count + slot

        return found + mine.astype(I32)

    ratio_copy.wait()
    found = lax.fori_loop(0, pairs, functools.partial(enlist, meta=meta_own, base=0), jnp.int32(0))
    found = lax.fori_loop(0, pairs, functools.partial(enlist, meta=meta_peer, base=patches), found)

    for extra in range(UNROLL - 1):
        table[0, found + extra] = 0
        table[1, found + extra] = 1
        table[2, found + extra] = 0
        table[3, found + extra] = 0
        table[4, found + extra] = 0

    own_copy.wait()
    lax.fori_loop(0, patches, prepare, 0)

    lane_k = iota((1, lanes), 1)
    lane_code = (lane_k // edge) * 4096 + lane_k % edge
    row_x = iota((rows, 1), 0) % edge

    def remap(step, carry):
        results = []
        for u in range(UNROLL):
            p = step * UNROLL + u
            live = (p < found).astype(F32)
            r = table[1, p]
            inverse = jnp.where(r == 2, 0.5, 1.0).astype(F32)
            spread = code_x[...] - (row_x * r + table[2, p])
            weight_x = jnp.where((spread & ~(r - 1)) == 0, inverse, 0.0).astype(BF16)
            section = jnp.dot(weight_x, split[table[0, p]], preferred_element_type=F32)
            spread = code_k[...] - (lane_code * r + table[3, p])
            weight_k = jnp.where((spread & ~((r - 1) * 4097)) == 0, inverse * inverse, 0.0).astype(BF16)
            high, low = halves(section)
            stacked = jnp.concatenate([high, low], axis=0)
            product = jnp.dot(stacked, weight_k, preferred_element_type=F32)
            part = (product[:rows] + product[rows:]) * live
            results.append((p, part))
        for p, part in results:
            to = table[4, p]
            out[to] = out[to] + part
        return carry

    steps = (found + UNROLL - 1) // UNROLL
    lax.fori_loop(0, steps, remap, 0)


def fold_kernel(a, out):
    size = out.shape[0]
    sources = a.shape[0] // size

    def add(i, carry):
        total = a[i]
        for s in range(1, sources):
            total = total + a[s * size + i]
        out[i] = total
        return carry

    lax.fori_loop(0, size, add, 0)


def gather_kernel(a, new_data, faces, *, count, fields, edge):
    rows = fields * edge
    lanes = edge * edge
    sources = a.shape[0] // count
    sums = []
    for q in range(count):
        total = a[q]
        for s in range(1, sources):
            total = total + a[s * count + q]
        sums.append(total)
    whole = jnp.concatenate(sums, axis=0)
    new_data[...] = whole
    high, low = halves(whole)
    stacked = jnp.concatenate([high, low], axis=0)
    source = iota((lanes, lanes), 0)
    target = iota((lanes, lanes), 1) % edge
    here = (iota((edge, lanes), 1) // edge) == iota((edge, lanes), 0)
    picks = (
        source == target,
        source == target + (lanes - edge),
        source == target * edge,
        source == target * edge + (edge - 1),
    )
    for q in range(count):
        for f in range(fields):
            start = q * rows + f * edge
            faces[q, 0, f:f + 1, :] = whole[start:start + 1]
            faces[q, 1, f:f + 1, :] = whole[start + edge - 1:start + edge]
    for e, pick in enumerate(picks):
        weight = jnp.where(pick, 1.0, 0.0).astype(BF16)
        product = jnp.dot(stacked, weight, preferred_element_type=F32)
        layer = product[:count * rows] + product[count * rows:]
        for q in range(count):
            for f in range(fields):
                start = q * rows + f * edge
                line = jnp.sum(jnp.where(here, layer[start:start + edge], 0.0), axis=0, keepdims=True)
                faces[q, 2 + e, f:f + 1, :] = line


def jump_kernel(place, side, patch, own, before, after, jump, *, count, fields, devices):
    linear = place[2]
    for q in range(count):
        for e in range(6):
            u = side[q, e]
            n = patch[q, e]
            at = linear + u - 1
            present = (u < 3) & (at >= 0) & (at < devices)
            other = e ^ 1
            ghost = jnp.where(
                u == 0, before[n, other], jnp.where(u == 1, own[n, other], after[n, other])
            )
            line = jnp.where(present, ghost - own[q, e], 0.0)
            for f in range(fields):
                jump[q, f, e:e + 1, :] = line[f:f + 1]


def body(
    old_data, pair_old, pair_slot, pair_shift, pair_dest, new_ratio, neighbor_side, neighbor_patch
):
    patches, fields, edge, lanes = old_data.shape
    pairs = pair_old.shape[0]
    count = neighbor_side.shape[0]
    rows = fields * edge
    half = lanes // 2
    size_x = lax.axis_size("gx")
    size_y = lax.axis_size("gy")
    chips_y = lax.axis_size("gz_0")
    cores = lax.axis_size("gz_1")
    devices = size_x * size_y * chips_y * cores
    index_y = lax.axis_index("gy")
    core = lax.axis_index("gz_1")
    index_x = lax.axis_index("gx")
    chip_y = lax.axis_index("gz_0")
    linear = ((index_x * size_y + index_y) * chips_y + chip_y) * cores + core
    place = jnp.stack([index_y, core, linear, index_x, chip_y]).astype(I32)
    meta = jnp.concatenate(
        [pair_old[None], pair_slot[None], pair_shift.T, pair_dest.T], axis=0
    )
    own = old_data.reshape(patches, rows, lanes)
    swap = [(i, cores - 1 - i) for i in range(cores)]
    peer_meta = lax.ppermute(meta, "gz_1", swap)
    peer = lax.ppermute(own, "gz_1", swap)
    owners = size_x * chips_y * count
    smem = pl.BlockSpec(memory_space=SMEM)
    vmem = pl.BlockSpec(memory_space=VMEM)
    hbm = pl.BlockSpec(memory_space=HBM)
    params = pltpu.CompilerParams(vmem_limit_bytes=24 * 1024 * 1024)
    mass = pl.pallas_call(
        functools.partial(
            mass_kernel, patches=patches, fields=fields, edge=edge, size_y=size_y,
            size_z=chips_y * cores, new_count=count, pairs=pairs,
        ),
        out_shape=jax.ShapeDtypeStruct((size_y, 8, half), F32),
        in_specs=[smem, smem, hbm, hbm],
        out_specs=vmem,
        scratch_shapes=[
            pltpu.SMEM(new_ratio.shape, I32),
            pltpu.VMEM((patches, rows, lanes), F32),
            pltpu.VMEM((patches, edge, lanes), F32),
            DMA((2,)),
        ],
        compiler_params=params,
        name="mass",
    )(place, meta, slow(new_ratio), slow(own))
    column = lax.all_to_all(mass, "gy", 0, 0, tiled=True)
    partials = pl.pallas_call(
        functools.partial(
            partials_kernel, patches=patches, fields=fields, edge=edge, size_x=size_x,
            size_y=size_y, chips_y=chips_y, cores=cores, new_count=count, pairs=pairs,
        ),
        out_shape=HBM((owners, rows, lanes), F32),
        in_specs=[smem, smem, smem, hbm, hbm, vmem],
        out_specs=vmem,
        scratch_shapes=[
            pltpu.SMEM(new_ratio.shape, I32),
            pltpu.VMEM((patches, rows, lanes), F32),
            pltpu.SMEM((5, 2 * pairs + UNROLL), I32),
            pltpu.VMEM((2 * patches, 2 * rows, lanes), BF16),
            pltpu.VMEM((lanes, lanes), I32),
            pltpu.VMEM((rows, 2 * rows), I32),
            DMA((2,)),
        ],
        compiler_params=params,
        name="partials",
    )(place, meta, peer_meta, slow(new_ratio), slow(own), fast(peer))

    first_groups, last_groups = mixed_groups(size_x, size_y, chips_y, cores)
    first = lax.all_to_all(partials, ALL_AXES, 0, 0, tiled=True, axis_index_groups=first_groups)
    total = jnp.sum(column, axis=0)
    for pairs_of in mixed_steps(size_x, size_y, chips_y, cores):
        total = total + lax.ppermute(total, ALL_AXES, pairs_of)
    folded = pl.pallas_call(
        fold_kernel,
        out_shape=VMEM((owners // size_x, rows, lanes), F32),
        in_specs=[vmem],
        out_specs=vmem,
        compiler_params=params,
        name="fold",
    )(fast(first))
    last = lax.all_to_all(folded, ALL_AXES, 0, 0, tiled=True, axis_index_groups=last_groups)
    new_data, faces = pl.pallas_call(
        functools.partial(gather_kernel, count=count, fields=fields, edge=edge),
        out_shape=(
            jax.ShapeDtypeStruct((count * rows, lanes), F32),
            VMEM((count, 6, fields, lanes), F32),
        ),
        in_specs=[vmem],
        out_specs=(vmem, vmem),
        compiler_params=params,
        name="gather",
    )(fast(last))
    before = shifted(faces, ALL_AXES, 1)
    after = shifted(faces, ALL_AXES, -1)
    interface_jump = pl.pallas_call(
        functools.partial(jump_kernel, count=count, fields=fields, devices=devices),
        out_shape=jax.ShapeDtypeStruct((count, fields, 6, lanes), F32),
        in_specs=[smem, smem, smem, vmem, vmem, vmem],
        out_specs=vmem,
        name="jump",
    )(place, neighbor_side, neighbor_patch, fast(faces), fast(before), fast(after))
    total_cells = patches * devices * edge * lanes
    mass_totals = total[:fields, :2].T / total_cells
    return (new_data.reshape(count, fields, edge, lanes), interface_jump, mass_totals)


def solution(mesh):
    torus = Mesh(
        mesh.devices.reshape(mesh.shape["gx"], mesh.shape["gy"], 4, 2), ("gx", "gy", "gz_0", "gz_1")
    )
    return jax.shard_map(
        body,
        mesh=torus,
        in_specs=(
            P(ALL_AXES, None, None, None),
            P(ALL_AXES),
            P(ALL_AXES),
            P(ALL_AXES, None),
            P(ALL_AXES, None),
            P(),
            P(ALL_AXES, None),
            P(ALL_AXES, None),
        ),
        out_specs=(P(ALL_AXES, None, None, None), P(ALL_AXES, None, None, None), P()),
        check_vma=False,
    )
```

```python
import functools

import jax
import jax.numpy as jnp
from jax import lax
from jax.experimental import pallas as pl
from jax.experimental.pallas import tpu as pltpu
from jax.sharding import Mesh
from jax.sharding import PartitionSpec as P


ALL_AXES = ("gx", "gy", "gz_0", "gz_1")
UNROLL = 4
BF16 = jnp.bfloat16
F32 = jnp.float32
I32 = jnp.int32
VMEM = pltpu.VMEM
SMEM = pltpu.SMEM
HBM = pltpu.HBM
DMA = pltpu.SemaphoreType.DMA


def shifted(block, axis, distance):
    devices = range(lax.axis_size(axis))
    route = [(i - distance, i) for i in devices if i - distance in devices]
    return lax.ppermute(block, axis, route)


def fast(block):
    return pltpu.with_memory_space_constraint(block, VMEM)


def mixed_groups(size_x, size_y, chips_y, cores):
    def device(x, z, y, c):
        return ((x * size_y + z) * chips_y + y) * cores + c

    along_x, along_y = [], []
    for c in range(cores):
        lines_x = [[device(x, z, y, c) for x in range(size_x)] for z in range(size_y) for y in range(chips_y)]
        lines_y = [[device(x, z, y, c) for y in range(chips_y)] for z in range(size_y) for x in range(size_x)]
        along_x += lines_x if c == 0 else lines_y
        along_y += lines_y if c == 0 else lines_x
    return along_x, along_y


def slow(block):
    return pltpu.with_memory_space_constraint(block, HBM)


def halves(block):
    high = block.astype(BF16)
    low = (block - high.astype(F32)).astype(BF16)
    return high, low


def over(value, size):
    return value >> (size.bit_length() - 1)


def within(value, size):
    return value & (size - 1)


def iota(shape, dim):
    return lax.broadcasted_iota(I32, shape, dim)


def mass_kernel(place, meta, ratio_in, own_in, out, ratio, own, counts, sems, *, patches, fields, edge, size_y, size_z, new_count, pairs):
    lanes = edge * edge
    half = lanes // 2
    index_y = place[0]
    ratio_copy = pltpu.make_async_copy(ratio_in, ratio, sems.at[0])
    own_copy = pltpu.make_async_copy(own_in, own, sems.at[1])
    ratio_copy.start()
    own_copy.start()
    counts[...] = jnp.zeros_like(counts)
    at_x = iota((edge, lanes), 0)
    at_y = over(iota((edge, lanes), 1), edge)
    at_z = within(iota((edge, lanes), 1), edge)

    def count(p, carry):
        dest = meta[5, p]
        owner = (over(dest, size_z) * size_y + index_y) * size_z + within(dest, size_z)
        reach = edge * ratio[owner * new_count + meta[1, p]]
        hit = jnp.full((edge, lanes), True)
        for a, at in enumerate((at_x, at_y, at_z)):
            distance = at - meta[2 + a, p]
            hit = hit & (distance >= 0) & (distance < reach)
        o = meta[0, p]
        counts[o] = counts[o] + jnp.where(hit, 1.0, 0.0)
        return carry

    ratio_copy.wait()
    lax.fori_loop(0, pairs, count, 0)
    own_copy.wait()

    def add(o, sums):
        weight = counts[o]
        olds, news = sums
        old_list, new_list = [], []
        for f in range(fields):
            block = own[o, f * edge:(f + 1) * edge]
            scaled = block * weight
            old_list.append(olds[f] + (block[:, :half] + block[:, half:]))
            new_list.append(news[f] + (scaled[:, :half] + scaled[:, half:]))
        return tuple(old_list), tuple(new_list)

    zero = tuple(jnp.zeros((edge, half), F32) for _ in range(fields))
    olds, news = lax.fori_loop(0, patches, add, (zero, zero))
    lane = iota((1, half), 1)
    lines = []
    for f in range(fields):
        old_f = jnp.sum(olds[f], keepdims=True)
        new_f = jnp.sum(news[f], keepdims=True)
        lines.append(jnp.where(lane == 0, old_f, jnp.where(lane == 1, new_f, 0.0)))
    lines.append(jnp.zeros((8 - fields, half), F32))
    packed = jnp.concatenate(lines, axis=0)
    out[...] = jnp.broadcast_to(packed[None], out.shape)


def partials_kernel(
    place, meta_own, meta_peer, ratio_in, own_in, peer,
    out, ratio, own, table, split, code_k, code_x, sems,
    *, patches, fields, edge, size_x, size_y, chips_y, cores, new_count, pairs,
):
    rows = fields * edge
    lanes = edge * edge
    index_y = place[0]
    core = place[1]
    size_z = chips_y * cores
    for size in (edge, size_z, cores):
        assert size & (size - 1) == 0
    ratio_copy = pltpu.make_async_copy(ratio_in, ratio, sems.at[0])
    own_copy = pltpu.make_async_copy(own_in, own, sems.at[1])
    ratio_copy.start()
    own_copy.start()

    def prepare(o, carry):
        high, low = halves(own[o])
        split[o, 0:rows] = high
        split[o, rows:2 * rows] = low
        high, low = halves(peer[o])
        split[patches + o, 0:rows] = high
        split[patches + o, rows:2 * rows] = low
        return carry

    out[...] = jnp.zeros_like(out)
    cell = iota((lanes, lanes), 0)
    code_k[...] = over(cell, edge) * 4096 + within(cell, edge)
    row = iota((rows, 2 * rows), 0)
    col = iota((rows, 2 * rows), 1) % rows
    code_x[...] = (over(col, edge) - over(row, edge)) * 4096 + within(col, edge)

    def enlist(p, found, meta, base):
        dest = meta[5, p]
        mine = within(dest, cores) == core

        @pl.when(mine)
        def _():
            table[0, found] = base + meta[0, p]
            iz = within(dest, size_z)
            ix = over(dest, size_z)
            slot = meta[1, p]
            owner = (ix * size_y + index_y) * size_z + iz
            table[1, found] = ratio[owner * new_count + slot]
            table[2, found] = meta[2, p]
            table[3, found] = meta[3, p] * 4096 + meta[4, p]
            chip_y = over(iz, cores)
            chip = jnp.where(core == 0, ix * chips_y + chip_y, chip_y * size_x + ix)
            table[4, found] = chip * new_count + slot

        return found + mine.astype(I32)

    ratio_copy.wait()
    found = lax.fori_loop(0, pairs, functools.partial(enlist, meta=meta_own, base=0), jnp.int32(0))
    found = lax.fori_loop(0, pairs, functools.partial(enlist, meta=meta_peer, base=patches), found)

    for extra in range(UNROLL - 1):
        table[0, found + extra] = 0
        table[1, found + extra] = 1
        table[2, found + extra] = 0
        table[3, found + extra] = 0
        table[4, found + extra] = 0

    own_copy.wait()
    lax.fori_loop(0, patches, prepare, 0)

    lane_k = iota((1, lanes), 1)
    lane_code = over(lane_k, edge) * 4096 + within(lane_k, edge)
    row_x = within(iota((rows, 1), 0), edge)

    def remap(step, carry):
        results = []
        for u in range(UNROLL):
            p = step * UNROLL + u
            live = (p < found).astype(F32)
            r = table[1, p]
            inverse = jnp.where(r == 2, 0.5, 1.0).astype(F32)
            spread = code_x[...] - (row_x * r + table[2, p])
            weight_x = jnp.where((spread & ~(r - 1)) == 0, inverse, 0.0).astype(BF16)
            section = jnp.dot(weight_x, split[table[0, p]], preferred_element_type=F32)
            spread = code_k[...] - (lane_code * r + table[3, p])
            weight_k = jnp.where((spread & ~((r - 1) * 4097)) == 0, inverse * inverse, 0.0).astype(BF16)
            high, low = halves(section)
            stacked = jnp.concatenate([high, low], axis=0)
            product = jnp.dot(stacked, weight_k, preferred_element_type=F32)
            part = (product[:rows] + product[rows:]) * live
            results.append((p, part))
        for p, part in results:
            to = table[4, p]
            out[to] = out[to] + part
        return carry

    steps = (found + UNROLL - 1) // UNROLL
    lax.fori_loop(0, steps, remap, 0)


def fold_kernel(a, out):
    total = a[0]
    for s in range(1, a.shape[0]):
        total = total + a[s]
    out[...] = total


def gather_kernel(a, new_data, faces, *, count, fields, edge):
    rows = fields * edge
    lanes = edge * edge
    sources = a.shape[0] // count
    sums = []
    for q in range(count):
        total = a[q]
        for s in range(1, sources):
            total = total + a[s * count + q]
        sums.append(total)
    whole = jnp.concatenate(sums, axis=0)
    new_data[...] = whole
    high, low = halves(whole)
    stacked = jnp.concatenate([high, low], axis=0)
    source = iota((lanes, lanes), 0)
    target = within(iota((lanes, lanes), 1), edge)
    here = over(iota((edge, lanes), 1), edge) == iota((edge, lanes), 0)
    picks = (
        source == target,
        source == target + (lanes - edge),
        source == target * edge,
        source == target * edge + (edge - 1),
    )
    for q in range(count):
        for f in range(fields):
            start = q * rows + f * edge
            faces[q, 0, f:f + 1, :] = whole[start:start + 1]
            faces[q, 1, f:f + 1, :] = whole[start + edge - 1:start + edge]
    for e, pick in enumerate(picks):
        weight = jnp.where(pick, 1.0, 0.0).astype(BF16)
        product = jnp.dot(stacked, weight, preferred_element_type=F32)
        layer = product[:count * rows] + product[count * rows:]
        for q in range(count):
            for f in range(fields):
                start = q * rows + f * edge
                line = jnp.sum(jnp.where(here, layer[start:start + edge], 0.0), axis=0, keepdims=True)
                faces[q, 2 + e, f:f + 1, :] = line


def jump_kernel(place, side, patch, own, before, after, jump, *, count, fields, devices):
    linear = place[2]
    for q in range(count):
        for e in range(6):
            u = side[q, e]
            n = patch[q, e]
            at = linear + u - 1
            present = (u < 3) & (at >= 0) & (at < devices)
            other = e ^ 1
            ghost = jnp.where(
                u == 0, before[n, other], jnp.where(u == 1, own[n, other], after[n, other])
            )
            line = jnp.where(present, ghost - own[q, e], 0.0)
            for f in range(fields):
                jump[q, f, e:e + 1, :] = line[f:f + 1]


def body(
    old_data, pair_old, pair_slot, pair_shift, pair_dest, new_ratio, neighbor_side, neighbor_patch
):
    patches, fields, edge, lanes = old_data.shape
    pairs = pair_old.shape[0]
    count = neighbor_side.shape[0]
    rows = fields * edge
    half = lanes // 2
    size_x = lax.axis_size("gx")
    size_y = lax.axis_size("gy")
    chips_y = lax.axis_size("gz_0")
    cores = lax.axis_size("gz_1")
    devices = size_x * size_y * chips_y * cores
    index_y = lax.axis_index("gy")
    core = lax.axis_index("gz_1")
    index_x = lax.axis_index("gx")
    chip_y = lax.axis_index("gz_0")
    linear = ((index_x * size_y + index_y) * chips_y + chip_y) * cores + core
    place = jnp.stack([index_y, core, linear, index_x, chip_y]).astype(I32)
    meta = jnp.concatenate(
        [pair_old[None], pair_slot[None], pair_shift.T, pair_dest.T], axis=0
    )
    own = old_data.reshape(patches, rows, lanes)
    swap = [(i, cores - 1 - i) for i in range(cores)]
    peer_meta = lax.ppermute(meta, "gz_1", swap)
    peer = lax.ppermute(own, "gz_1", swap)
    owners = size_x * chips_y * count
    smem = pl.BlockSpec(memory_space=SMEM)
    vmem = pl.BlockSpec(memory_space=VMEM)
    hbm = pl.BlockSpec(memory_space=HBM)
    params = pltpu.CompilerParams(vmem_limit_bytes=24 * 1024 * 1024)
    mass = pl.pallas_call(
        functools.partial(
            mass_kernel, patches=patches, fields=fields, edge=edge, size_y=size_y,
            size_z=chips_y * cores, new_count=count, pairs=pairs,
        ),
        out_shape=jax.ShapeDtypeStruct((size_x * chips_y, 8, half), F32),
        in_specs=[smem, smem, hbm, hbm],
        out_specs=vmem,
        scratch_shapes=[
            pltpu.SMEM(new_ratio.shape, I32),
            pltpu.VMEM((patches, rows, lanes), F32),
            pltpu.VMEM((patches, edge, lanes), F32),
            DMA((2,)),
        ],
        compiler_params=params,
        name="mass",
    )(place, meta, slow(new_ratio), slow(own))
    plane = lax.all_to_all(mass, ("gx", "gz_0"), 0, 0, tiled=True)
    partials = pl.pallas_call(
        functools.partial(
            partials_kernel, patches=patches, fields=fields, edge=edge, size_x=size_x,
            size_y=size_y, chips_y=chips_y, cores=cores, new_count=count, pairs=pairs,
        ),
        out_shape=HBM((owners, rows, lanes), F32),
        in_specs=[smem, smem, smem, hbm, hbm, vmem],
        out_specs=vmem,
        scratch_shapes=[
            pltpu.SMEM(new_ratio.shape, I32),
            pltpu.VMEM((patches, rows, lanes), F32),
            pltpu.SMEM((5, 2 * pairs + UNROLL), I32),
            pltpu.VMEM((2 * patches, 2 * rows, lanes), BF16),
            pltpu.VMEM((lanes, lanes), I32),
            pltpu.VMEM((rows, 2 * rows), I32),
            DMA((2,)),
        ],
        compiler_params=params,
        name="partials",
    )(place, meta, peer_meta, slow(new_ratio), slow(own), fast(peer))

    first_groups, last_groups = mixed_groups(size_x, size_y, chips_y, cores)
    first = lax.all_to_all(partials, ALL_AXES, 0, 0, tiled=True, axis_index_groups=first_groups)
    total = jnp.sum(plane, axis=0)
    total = lax.psum(total, "gy")
    total = total + lax.ppermute(total, "gz_1", swap)
    kept = owners // size_x
    folded = pl.pallas_call(
        fold_kernel,
        out_shape=jax.ShapeDtypeStruct((kept, rows, lanes), F32),
        grid=(kept // count,),
        in_specs=[pl.BlockSpec((size_x, count, rows, lanes), lambda i: (0, i, 0, 0))],
        out_specs=pl.BlockSpec((count, rows, lanes), lambda i: (i, 0, 0)),
        compiler_params=params,
        name="fold",
    )(first.reshape(size_x, kept, rows, lanes))
    last = lax.all_to_all(folded, ALL_AXES, 0, 0, tiled=True, axis_index_groups=last_groups)
    new_data, faces = pl.pallas_call(
        functools.partial(gather_kernel, count=count, fields=fields, edge=edge),
        out_shape=(
            jax.ShapeDtypeStruct((count * rows, lanes), F32),
            VMEM((count, 6, fields, lanes), F32),
        ),
        in_specs=[vmem],
        out_specs=(vmem, vmem),
        compiler_params=params,
        name="gather",
    )(fast(last))
    before = shifted(faces, ALL_AXES, 1)
    after = shifted(faces, ALL_AXES, -1)
    interface_jump = pl.pallas_call(
        functools.partial(jump_kernel, count=count, fields=fields, devices=devices),
        out_shape=jax.ShapeDtypeStruct((count, fields, 6, lanes), F32),
        in_specs=[smem, smem, smem, vmem, vmem, vmem],
        out_specs=vmem,
        name="jump",
    )(place, neighbor_side, neighbor_patch, fast(faces), fast(before), fast(after))
    total_cells = patches * devices * edge * lanes
    mass_totals = total[:fields, :2].T / total_cells
    return (new_data.reshape(count, fields, edge, lanes), interface_jump, mass_totals)


def solution(mesh):
    torus = Mesh(
        mesh.devices.reshape(mesh.shape["gx"], mesh.shape["gy"], 4, 2), ("gx", "gy", "gz_0", "gz_1")
    )
    return jax.shard_map(
        body,
        mesh=torus,
        in_specs=(
            P(ALL_AXES, None, None, None),
            P(ALL_AXES),
            P(ALL_AXES),
            P(ALL_AXES, None),
            P(ALL_AXES, None),
            P(),
            P(ALL_AXES, None),
            P(ALL_AXES, None),
        ),
        out_specs=(P(ALL_AXES, None, None, None), P(ALL_AXES, None, None, None), P()),
        check_vma=False,
    )
```

```python
import functools

import jax
import jax.numpy as jnp
from jax import lax
from jax.experimental import pallas as pl
from jax.experimental.pallas import tpu as pltpu
from jax.sharding import Mesh
from jax.sharding import PartitionSpec as P


ALL_AXES = ("gx", "gy", "gz_0", "gz_1")
PLANE = ("gx", "gz_0", "gz_1")
UNROLL = 4
BF16 = jnp.bfloat16
F32 = jnp.float32
I32 = jnp.int32
VMEM = pltpu.VMEM
SMEM = pltpu.SMEM
HBM = pltpu.HBM
DMA = pltpu.SemaphoreType.DMA


def shifted(block, axis, distance):
    devices = range(lax.axis_size(axis))
    route = [(i - distance, i) for i in devices if i - distance in devices]
    return lax.ppermute(block, axis, route)


def fast(block):
    return pltpu.with_memory_space_constraint(block, VMEM)


def mixed_groups(size_x, size_y, chips_y, cores):
    def device(x, z, y, c):
        return ((x * size_y + z) * chips_y + y) * cores + c

    along_x, along_y = [], []
    for c in range(cores):
        lines_x = [[device(x, z, y, c) for x in range(size_x)] for z in range(size_y) for y in range(chips_y)]
        lines_y = [[device(x, z, y, c) for y in range(chips_y)] for z in range(size_y) for x in range(size_x)]
        along_x += lines_x if c == 0 else lines_y
        along_y += lines_y if c == 0 else lines_x
    return along_x, along_y


def slow(block):
    return pltpu.with_memory_space_constraint(block, HBM)


def halves(block):
    high = block.astype(BF16)
    low = (block - high.astype(F32)).astype(BF16)
    return high, low


def over(value, size):
    return value >> (size.bit_length() - 1)


def within(value, size):
    return value & (size - 1)


def iota(shape, dim):
    return lax.broadcasted_iota(I32, shape, dim)


def mass_kernel(place, meta, ratio_in, own_in, out, ratio, own, counts, sems, *, patches, fields, edge, size_y, size_z, new_count, pairs):
    lanes = edge * edge
    half = lanes // 2
    index_y = place[0]
    ratio_copy = pltpu.make_async_copy(ratio_in, ratio, sems.at[0])
    own_copy = pltpu.make_async_copy(own_in, own, sems.at[1])
    ratio_copy.start()
    own_copy.start()
    counts[...] = jnp.zeros_like(counts)
    at_x = iota((edge, lanes), 0)
    at_y = over(iota((edge, lanes), 1), edge)
    at_z = within(iota((edge, lanes), 1), edge)

    def count(p, carry):
        dest = meta[5, p]
        owner = (over(dest, size_z) * size_y + index_y) * size_z + within(dest, size_z)
        reach = edge * ratio[owner * new_count + meta[1, p]]
        hit = jnp.full((edge, lanes), True)
        for a, at in enumerate((at_x, at_y, at_z)):
            distance = at - meta[2 + a, p]
            hit = hit & (distance >= 0) & (distance < reach)
        o = meta[0, p]
        counts[o] = counts[o] + jnp.where(hit, 1.0, 0.0)
        return carry

    ratio_copy.wait()
    lax.fori_loop(0, pairs, count, 0)
    own_copy.wait()

    def add(o, sums):
        weight = counts[o]
        olds, news = sums
        old_list, new_list = [], []
        for f in range(fields):
            block = own[o, f * edge:(f + 1) * edge]
            scaled = block * weight
            old_list.append(olds[f] + (block[:, :half] + block[:, half:]))
            new_list.append(news[f] + (scaled[:, :half] + scaled[:, half:]))
        return tuple(old_list), tuple(new_list)

    zero = tuple(jnp.zeros((edge, half), F32) for _ in range(fields))
    olds, news = lax.fori_loop(0, patches, add, (zero, zero))
    lane = iota((1, half), 1)
    lines = []
    for f in range(fields):
        old_f = jnp.sum(olds[f], keepdims=True)
        new_f = jnp.sum(news[f], keepdims=True)
        lines.append(jnp.where(lane == 0, old_f, jnp.where(lane == 1, new_f, 0.0)))
    lines.append(jnp.zeros((8 - fields, half), F32))
    packed = jnp.concatenate(lines, axis=0)
    out[...] = jnp.broadcast_to(packed[None], out.shape)


def partials_kernel(
    place, meta_own, meta_peer, ratio_in, own_in, peer,
    out, ratio, own, table, split, code_k, code_x, sems,
    *, patches, fields, edge, size_x, size_y, chips_y, cores, new_count, pairs,
):
    rows = fields * edge
    lanes = edge * edge
    index_y = place[0]
    core = place[1]
    size_z = chips_y * cores
    for size in (edge, size_z, cores):
        assert size & (size - 1) == 0
    ratio_copy = pltpu.make_async_copy(ratio_in, ratio, sems.at[0])
    own_copy = pltpu.make_async_copy(own_in, own, sems.at[1])
    ratio_copy.start()
    own_copy.start()

    def prepare(o, carry):
        high, low = halves(own[o])
        split[o, 0:rows] = high
        split[o, rows:2 * rows] = low
        high, low = halves(peer[o])
        split[patches + o, 0:rows] = high
        split[patches + o, rows:2 * rows] = low
        return carry

    out[...] = jnp.zeros_like(out)
    cell = iota((lanes, lanes), 0)
    code_k[...] = over(cell, edge) * 4096 + within(cell, edge)
    row = iota((rows, 2 * rows), 0)
    col = iota((rows, 2 * rows), 1) % rows
    code_x[...] = (over(col, edge) - over(row, edge)) * 4096 + within(col, edge)

    def enlist(p, found, meta, base):
        dest = meta[5, p]
        mine = within(dest, cores) == core

        @pl.when(mine)
        def _():
            table[0, found] = base + meta[0, p]
            iz = within(dest, size_z)
            ix = over(dest, size_z)
            slot = meta[1, p]
            owner = (ix * size_y + index_y) * size_z + iz
            table[1, found] = ratio[owner * new_count + slot]
            table[2, found] = meta[2, p]
            table[3, found] = meta[3, p] * 4096 + meta[4, p]
            chip_y = over(iz, cores)
            chip = jnp.where(core == 0, ix * chips_y + chip_y, chip_y * size_x + ix)
            table[4, found] = chip * new_count + slot

        return found + mine.astype(I32)

    ratio_copy.wait()
    found = lax.fori_loop(0, pairs, functools.partial(enlist, meta=meta_own, base=0), jnp.int32(0))
    found = lax.fori_loop(0, pairs, functools.partial(enlist, meta=meta_peer, base=patches), found)

    for extra in range(UNROLL - 1):
        table[0, found + extra] = 0
        table[1, found + extra] = 1
        table[2, found + extra] = 0
        table[3, found + extra] = 0
        table[4, found + extra] = 0

    own_copy.wait()
    lax.fori_loop(0, patches, prepare, 0)

    lane_k = iota((1, lanes), 1)
    lane_code = over(lane_k, edge) * 4096 + within(lane_k, edge)
    row_x = within(iota((rows, 1), 0), edge)

    def remap(step, carry):
        results = []
        for u in range(UNROLL):
            p = step * UNROLL + u
            live = (p < found).astype(F32)
            r = table[1, p]
            inverse = jnp.where(r == 2, 0.5, 1.0).astype(F32)
            spread = code_x[...] - (row_x * r + table[2, p])
            weight_x = jnp.where((spread & ~(r - 1)) == 0, inverse, 0.0).astype(BF16)
            section = jnp.dot(weight_x, split[table[0, p]], preferred_element_type=F32)
            spread = code_k[...] - (lane_code * r + table[3, p])
            weight_k = jnp.where((spread & ~((r - 1) * 4097)) == 0, inverse * inverse, 0.0).astype(BF16)
            high, low = halves(section)
            stacked = jnp.concatenate([high, low], axis=0)
            product = jnp.dot(stacked, weight_k, preferred_element_type=F32)
            part = (product[:rows] + product[rows:]) * live
            results.append((p, part))
        for p, part in results:
            to = table[4, p]
            out[to] = out[to] + part
        return carry

    steps = (found + UNROLL - 1) // UNROLL
    lax.fori_loop(0, steps, remap, 0)


def fold_kernel(a, out, parts, sums, in_sems, out_sems, *, sources, chunk):
    kept = out.shape[0]
    chunks = kept // chunk
    copies = [
        [
            pltpu.make_async_copy(
                a.at[pl.ds(s * kept + j * chunk, chunk)], parts.at[pl.ds(s * kept + j * chunk, chunk)], in_sems.at[j, s]
            )
            for s in range(sources)
        ]
        for j in range(chunks)
    ]
    for row in copies:
        for copy in row:
            copy.start()
    outs = []
    for j in range(chunks):
        for copy in copies[j]:
            copy.wait()
        at = j * chunk
        total = parts[at:at + chunk]
        for s in range(1, sources):
            total = total + parts[s * kept + at:s * kept + at + chunk]
        sums[at:at + chunk] = total
        outs.append(pltpu.make_async_copy(sums.at[pl.ds(at, chunk)], out.at[pl.ds(at, chunk)], out_sems.at[j]))
        outs[-1].start()
    for copy in outs:
        copy.wait()


def gather_kernel(a, new_data, faces, *, count, fields, edge):
    rows = fields * edge
    lanes = edge * edge
    sources = a.shape[0] // count
    sums = []
    for q in range(count):
        total = a[q]
        for s in range(1, sources):
            total = total + a[s * count + q]
        sums.append(total)
    whole = jnp.concatenate(sums, axis=0)
    new_data[...] = whole
    high, low = halves(whole)
    stacked = jnp.concatenate([high, low], axis=0)
    source = iota((lanes, lanes), 0)
    target = within(iota((lanes, lanes), 1), edge)
    here = over(iota((edge, lanes), 1), edge) == iota((edge, lanes), 0)
    picks = (
        source == target,
        source == target + (lanes - edge),
        source == target * edge,
        source == target * edge + (edge - 1),
    )
    for q in range(count):
        for f in range(fields):
            start = q * rows + f * edge
            faces[q, 0, f:f + 1, :] = whole[start:start + 1]
            faces[q, 1, f:f + 1, :] = whole[start + edge - 1:start + edge]
    for e, pick in enumerate(picks):
        weight = jnp.where(pick, 1.0, 0.0).astype(BF16)
        product = jnp.dot(stacked, weight, preferred_element_type=F32)
        layer = product[:count * rows] + product[count * rows:]
        for q in range(count):
            for f in range(fields):
                start = q * rows + f * edge
                line = jnp.sum(jnp.where(here, layer[start:start + edge], 0.0), axis=0, keepdims=True)
                faces[q, 2 + e, f:f + 1, :] = line


def jump_kernel(place, side, patch, own, before, after, jump, *, count, fields, devices):
    linear = place[2]
    for q in range(count):
        for e in range(6):
            u = side[q, e]
            n = patch[q, e]
            at = linear + u - 1
            present = (u < 3) & (at >= 0) & (at < devices)
            other = e ^ 1
            ghost = jnp.where(
                u == 0, before[n, other], jnp.where(u == 1, own[n, other], after[n, other])
            )
            line = jnp.where(present, ghost - own[q, e], 0.0)
            for f in range(fields):
                jump[q, f, e:e + 1, :] = line[f:f + 1]


def body(
    old_data, pair_old, pair_slot, pair_shift, pair_dest, new_ratio, neighbor_side, neighbor_patch
):
    patches, fields, edge, lanes = old_data.shape
    pairs = pair_old.shape[0]
    count = neighbor_side.shape[0]
    rows = fields * edge
    half = lanes // 2
    size_x = lax.axis_size("gx")
    size_y = lax.axis_size("gy")
    chips_y = lax.axis_size("gz_0")
    cores = lax.axis_size("gz_1")
    devices = size_x * size_y * chips_y * cores
    index_y = lax.axis_index("gy")
    core = lax.axis_index("gz_1")
    index_x = lax.axis_index("gx")
    chip_y = lax.axis_index("gz_0")
    linear = ((index_x * size_y + index_y) * chips_y + chip_y) * cores + core
    place = jnp.stack([index_y, core, linear, index_x, chip_y]).astype(I32)
    meta = jnp.concatenate(
        [pair_old[None], pair_slot[None], pair_shift.T, pair_dest.T], axis=0
    )
    own = old_data.reshape(patches, rows, lanes)
    swap = [(i, cores - 1 - i) for i in range(cores)]
    peer_meta = lax.ppermute(meta, "gz_1", swap)
    peer = lax.ppermute(own, "gz_1", swap)
    owners = size_x * chips_y * count
    smem = pl.BlockSpec(memory_space=SMEM)
    vmem = pl.BlockSpec(memory_space=VMEM)
    hbm = pl.BlockSpec(memory_space=HBM)
    params = pltpu.CompilerParams(vmem_limit_bytes=24 * 1024 * 1024)
    mass = pl.pallas_call(
        functools.partial(
            mass_kernel, patches=patches, fields=fields, edge=edge, size_y=size_y,
            size_z=chips_y * cores, new_count=count, pairs=pairs,
        ),
        out_shape=jax.ShapeDtypeStruct((size_x * chips_y * cores, 8, half), F32),
        in_specs=[smem, smem, hbm, hbm],
        out_specs=vmem,
        scratch_shapes=[
            pltpu.SMEM(new_ratio.shape, I32),
            pltpu.VMEM((patches, rows, lanes), F32),
            pltpu.VMEM((patches, edge, lanes), F32),
            DMA((2,)),
        ],
        compiler_params=params,
        name="mass",
    )(place, meta, slow(new_ratio), slow(own))
    plane = lax.all_to_all(mass, PLANE, 0, 0, tiled=True)
    partials = pl.pallas_call(
        functools.partial(
            partials_kernel, patches=patches, fields=fields, edge=edge, size_x=size_x,
            size_y=size_y, chips_y=chips_y, cores=cores, new_count=count, pairs=pairs,
        ),
        out_shape=HBM((owners, rows, lanes), F32),
        in_specs=[smem, smem, smem, hbm, hbm, vmem],
        out_specs=vmem,
        scratch_shapes=[
            pltpu.SMEM(new_ratio.shape, I32),
            pltpu.VMEM((patches, rows, lanes), F32),
            pltpu.SMEM((5, 2 * pairs + UNROLL), I32),
            pltpu.VMEM((2 * patches, 2 * rows, lanes), BF16),
            pltpu.VMEM((lanes, lanes), I32),
            pltpu.VMEM((rows, 2 * rows), I32),
            DMA((2,)),
        ],
        compiler_params=params,
        name="partials",
    )(place, meta, peer_meta, slow(new_ratio), slow(own), fast(peer))

    first_groups, last_groups = mixed_groups(size_x, size_y, chips_y, cores)
    first = lax.all_to_all(partials, ALL_AXES, 0, 0, tiled=True, axis_index_groups=first_groups)
    total = jnp.sum(plane, axis=0)

    def crossed(value, distance):
        return value + lax.ppermute(value, "gy", [(i, i ^ distance) for i in range(size_y)])

    total = crossed(total, 8)
    total = crossed(total, 4)
    total = crossed(total, 2)
    total = crossed(total, 1)
    kept = owners // size_x
    folded = pl.pallas_call(
        functools.partial(fold_kernel, sources=size_x, chunk=count),
        out_shape=HBM((kept, rows, lanes), F32),
        in_specs=[hbm],
        out_specs=hbm,
        scratch_shapes=[
            pltpu.VMEM((owners, rows, lanes), F32),
            pltpu.VMEM((kept, rows, lanes), F32),
            DMA((kept // count, size_x)),
            DMA((kept // count,)),
        ],
        compiler_params=params,
        name="fold",
    )(slow(first))
    last = lax.all_to_all(folded, ALL_AXES, 0, 0, tiled=True, axis_index_groups=last_groups)
    new_data, faces = pl.pallas_call(
        functools.partial(gather_kernel, count=count, fields=fields, edge=edge),
        out_shape=(
            jax.ShapeDtypeStruct((count * rows, lanes), F32),
            VMEM((count, 6, fields, lanes), F32),
        ),
        in_specs=[vmem],
        out_specs=(vmem, vmem),
        compiler_params=params,
        name="gather",
    )(fast(last))
    before = shifted(faces, ALL_AXES, 1)
    after = shifted(faces, ALL_AXES, -1)
    interface_jump = pl.pallas_call(
        functools.partial(jump_kernel, count=count, fields=fields, devices=devices),
        out_shape=jax.ShapeDtypeStruct((count, fields, 6, lanes), F32),
        in_specs=[smem, smem, smem, vmem, vmem, vmem],
        out_specs=vmem,
        name="jump",
    )(place, neighbor_side, neighbor_patch, fast(faces), fast(before), fast(after))
    total_cells = patches * devices * edge * lanes
    mass_totals = total[:fields, :2].T / total_cells
    return (new_data.reshape(count, fields, edge, lanes), interface_jump, mass_totals)


def solution(mesh):
    torus = Mesh(
        mesh.devices.reshape(mesh.shape["gx"], mesh.shape["gy"], 4, 2), ("gx", "gy", "gz_0", "gz_1")
    )
    return jax.shard_map(
        body,
        mesh=torus,
        in_specs=(
            P(ALL_AXES, None, None, None),
            P(ALL_AXES),
            P(ALL_AXES),
            P(ALL_AXES, None),
            P(ALL_AXES, None),
            P(),
            P(ALL_AXES, None),
            P(ALL_AXES, None),
        ),
        out_specs=(P(ALL_AXES, None, None, None), P(ALL_AXES, None, None, None), P()),
        check_vma=False,
    )
```

```python
import functools

import jax
import jax.numpy as jnp
from jax import lax
from jax.experimental import pallas as pl
from jax.experimental.pallas import tpu as pltpu
from jax.sharding import Mesh
from jax.sharding import PartitionSpec as P


ALL_AXES = ("gx", "gy", "gz_0", "gz_1")
PLANE = ("gx", "gz_0", "gz_1")
UNROLL = 4
META_ROWS = 40
BF16 = jnp.bfloat16
F32 = jnp.float32
I32 = jnp.int32
VMEM = pltpu.VMEM
SMEM = pltpu.SMEM
HBM = pltpu.HBM
DMA = pltpu.SemaphoreType.DMA


def swapped(block, first):
    devices = lax.axis_size(ALL_AXES)
    pairs = [(i, i + 1) for i in range(first, devices - 1, 2)]
    return lax.ppermute(block, ALL_AXES, pairs + [(j, i) for i, j in pairs])


def fast(block):
    return pltpu.with_memory_space_constraint(block, VMEM)


def mixed_groups(size_x, size_y, chips_y, cores):
    def device(x, z, y, c):
        return ((x * size_y + z) * chips_y + y) * cores + c

    along_x, along_y = [], []
    for c in range(cores):
        lines_x = [[device(x, z, y, c) for x in range(size_x)] for z in range(size_y) for y in range(chips_y)]
        lines_y = [[device(x, z, y, c) for y in range(chips_y)] for z in range(size_y) for x in range(size_x)]
        along_x += lines_x if c == 0 else lines_y
        along_y += lines_y if c == 0 else lines_x
    return along_x, along_y


def slow(block):
    return pltpu.with_memory_space_constraint(block, HBM)


def halves(block):
    high = block.astype(BF16)
    low = (block - high.astype(F32)).astype(BF16)
    return high, low


def over(value, size):
    return value >> (size.bit_length() - 1)


def within(value, size):
    return value & (size - 1)


def iota(shape, dim):
    return lax.broadcasted_iota(I32, shape, dim)


def head_kernel(
    place, pair_old, pair_slot, pair_shift, pair_dest, old_row, slot_row, shift_col, dest_col, ratio_in, own_in,
    out, packed, ratio, counts, sems,
    *, patches, fields, edge, size_y, size_z, new_count, pairs,
):
    lanes = edge * edge
    half = lanes // 2
    index_y = place[0]
    ratio_copy = pltpu.make_async_copy(ratio_in, ratio, sems.at[0])
    rows = fields * edge
    cells = patches * rows
    own_copy = pltpu.make_async_copy(own_in, packed.at[pl.ds(0, cells)], sems.at[1])
    ratio_copy.start()
    own_copy.start()
    lane = iota((pairs, lanes), 1)
    shift = shift_col[...].astype(F32)
    table = jnp.where(lane == 3, dest_col[...].astype(F32), 0.0)
    for a in range(3):
        table = jnp.where(lane == a, shift[:, a:a + 1], table)
    packed[cells:cells + pairs] = table
    packed[cells + pairs:] = jnp.zeros((META_ROWS - pairs, lanes), F32)
    packed[cells + pairs:cells + pairs + 1, 0:pairs] = old_row[...].astype(F32)
    packed[cells + pairs + 1:cells + pairs + 2, 0:pairs] = slot_row[...].astype(F32)
    counts[...] = jnp.zeros_like(counts)
    at_x = iota((edge, lanes), 0)
    at_y = over(iota((edge, lanes), 1), edge)
    at_z = within(iota((edge, lanes), 1), edge)

    def count(p, carry):
        dest = pair_dest[p, 0]
        owner = (over(dest, size_z) * size_y + index_y) * size_z + within(dest, size_z)
        reach = edge * ratio[owner * new_count + pair_slot[p]]
        hit = jnp.full((edge, lanes), True)
        for a, at in enumerate((at_x, at_y, at_z)):
            distance = at - pair_shift[p, a]
            hit = hit & (distance >= 0) & (distance < reach)
        o = pair_old[p]
        counts[o] = counts[o] + jnp.where(hit, 1.0, 0.0)
        return carry

    ratio_copy.wait()
    lax.fori_loop(0, pairs, count, 0)
    own_copy.wait()

    def add(o, sums):
        weight = counts[o]
        olds, news = sums
        old_list, new_list = [], []
        for f in range(fields):
            block = packed[pl.ds(o * rows + f * edge, edge)]
            scaled = block * weight
            old_list.append(olds[f] + (block[:, :half] + block[:, half:]))
            new_list.append(news[f] + (scaled[:, :half] + scaled[:, half:]))
        return tuple(old_list), tuple(new_list)

    zero = tuple(jnp.zeros((edge, half), F32) for _ in range(fields))
    olds, news = lax.fori_loop(0, patches, add, (zero, zero))
    lane = iota((1, half), 1)
    lines = []
    for f in range(fields):
        old_f = jnp.sum(olds[f], keepdims=True)
        new_f = jnp.sum(news[f], keepdims=True)
        lines.append(jnp.where(lane == 0, old_f, jnp.where(lane == 1, new_f, 0.0)))
    lines.append(jnp.zeros((8 - fields, half), F32))
    packed = jnp.concatenate(lines, axis=0)
    out[...] = jnp.broadcast_to(packed[None], out.shape)


def partials_kernel(
    place, pair_old, pair_slot, pair_shift, pair_dest, ratio_in, own_in, peer,
    out, ratio, own, meta_v, meta, table, split, code_k, code_x, sems,
    *, patches, fields, edge, size_x, size_y, chips_y, cores, new_count, pairs,
):
    rows = fields * edge
    lanes = edge * edge
    index_y = place[0]
    core = place[1]
    size_z = chips_y * cores
    for size in (edge, size_z, cores):
        assert size & (size - 1) == 0
    ratio_copy = pltpu.make_async_copy(ratio_in, ratio, sems.at[0])
    own_copy = pltpu.make_async_copy(own_in, own, sems.at[1])
    ratio_copy.start()
    own_copy.start()
    cells = patches * rows
    meta_v[...] = peer[cells:cells + META_ROWS, 0:meta_v.shape[1]].astype(I32)
    meta_copy = pltpu.make_async_copy(meta_v, meta, sems.at[2])
    meta_copy.start()

    def prepare(o, carry):
        high, low = halves(own[o])
        split[o, 0:rows] = high
        split[o, rows:2 * rows] = low
        high, low = halves(peer[pl.ds(o * rows, rows)])
        split[patches + o, 0:rows] = high
        split[patches + o, rows:2 * rows] = low
        return carry

    out[...] = jnp.zeros_like(out)
    cell = iota((lanes, lanes), 0)
    code_k[...] = over(cell, edge) * 4096 + within(cell, edge)
    row = iota((rows, 2 * rows), 0)
    col = iota((rows, 2 * rows), 1) % rows
    code_x[...] = (over(col, edge) - over(row, edge)) * 4096 + within(col, edge)

    def enlist(found, base, old, slot, shift, dest):
        mine = within(dest, cores) == core

        @pl.when(mine)
        def _():
            table[0, found] = base + old
            iz = within(dest, size_z)
            ix = over(dest, size_z)
            owner = (ix * size_y + index_y) * size_z + iz
            table[1, found] = ratio[owner * new_count + slot]
            table[2, found] = shift[0]
            table[3, found] = shift[1] * 4096 + shift[2]
            chip_y = over(iz, cores)
            chip = jnp.where(core == 0, ix * chips_y + chip_y, chip_y * size_x + ix)
            table[4, found] = chip * new_count + slot

        return found + mine.astype(I32)

    def enlist_own(p, found):
        shift = [pair_shift[p, a] for a in range(3)]
        return enlist(found, 0, pair_old[p], pair_slot[p], shift, pair_dest[p, 0])

    def enlist_peer(p, found):
        shift = [meta[p, a] for a in range(3)]
        return enlist(found, patches, meta[pairs, p], meta[pairs + 1, p], shift, meta[p, 3])

    ratio_copy.wait()
    found = lax.fori_loop(0, pairs, enlist_own, jnp.int32(0))
    meta_copy.wait()
    found = lax.fori_loop(0, pairs, enlist_peer, found)

    for extra in range(UNROLL - 1):
        table[0, found + extra] = 0
        table[1, found + extra] = 1
        table[2, found + extra] = 0
        table[3, found + extra] = 0
        table[4, found + extra] = 0

    own_copy.wait()
    lax.fori_loop(0, patches, prepare, 0)

    lane_k = iota((1, lanes), 1)
    lane_code = over(lane_k, edge) * 4096 + within(lane_k, edge)
    row_x = within(iota((rows, 1), 0), edge)

    def remap(step, carry):
        results = []
        for u in range(UNROLL):
            p = step * UNROLL + u
            live = (p < found).astype(F32)
            r = table[1, p]
            inverse = jnp.where(r == 2, 0.5, 1.0).astype(F32)
            spread = code_x[...] - (row_x * r + table[2, p])
            weight_x = jnp.where((spread & ~(r - 1)) == 0, inverse, 0.0).astype(BF16)
            section = jnp.dot(weight_x, split[table[0, p]], preferred_element_type=F32)
            spread = code_k[...] - (lane_code * r + table[3, p])
            weight_k = jnp.where((spread & ~((r - 1) * 4097)) == 0, inverse * inverse, 0.0).astype(BF16)
            high, low = halves(section)
            stacked = jnp.concatenate([high, low], axis=0)
            product = jnp.dot(stacked, weight_k, preferred_element_type=F32)
            part = (product[:rows] + product[rows:]) * live
            results.append((p, part))
        for p, part in results:
            to = table[4, p]
            out[to] = out[to] + part
        return carry

    steps = (found + UNROLL - 1) // UNROLL
    lax.fori_loop(0, steps, remap, 0)


def fold_kernel(a, out, parts, sums, in_sems, out_sems, *, sources, chunk):
    kept = out.shape[0]
    chunks = kept // chunk
    copies = [
        [
            pltpu.make_async_copy(
                a.at[pl.ds(s * kept + j * chunk, chunk)], parts.at[pl.ds(s * kept + j * chunk, chunk)], in_sems.at[j, s]
            )
            for s in range(sources)
        ]
        for j in range(chunks)
    ]
    for row in copies:
        for copy in row:
            copy.start()
    outs = []
    for j in range(chunks):
        for copy in copies[j]:
            copy.wait()
        at = j * chunk
        total = parts[at:at + chunk]
        for s in range(1, sources):
            total = total + parts[s * kept + at:s * kept + at + chunk]
        sums[at:at + chunk] = total
        outs.append(pltpu.make_async_copy(sums.at[pl.ds(at, chunk)], out.at[pl.ds(at, chunk)], out_sems.at[j]))
        outs[-1].start()
    for copy in outs:
        copy.wait()


def gather_kernel(a, new_data, faces, *, count, fields, edge):
    rows = fields * edge
    lanes = edge * edge
    sources = a.shape[0] // count
    sums = []
    for q in range(count):
        total = a[q]
        for s in range(1, sources):
            total = total + a[s * count + q]
        sums.append(total)
    whole = jnp.concatenate(sums, axis=0)
    new_data[...] = whole
    high, low = halves(whole)
    stacked = jnp.concatenate([high, low], axis=0)
    source = iota((lanes, lanes), 0)
    target = within(iota((lanes, lanes), 1), edge)
    here = over(iota((edge, lanes), 1), edge) == iota((edge, lanes), 0)
    picks = (
        source == target,
        source == target + (lanes - edge),
        source == target * edge,
        source == target * edge + (edge - 1),
    )
    for q in range(count):
        for f in range(fields):
            start = q * rows + f * edge
            faces[q, 0, f:f + 1, :] = whole[start:start + 1]
            faces[q, 1, f:f + 1, :] = whole[start + edge - 1:start + edge]
    for e, pick in enumerate(picks):
        weight = jnp.where(pick, 1.0, 0.0).astype(BF16)
        product = jnp.dot(stacked, weight, preferred_element_type=F32)
        layer = product[:count * rows] + product[count * rows:]
        for q in range(count):
            for f in range(fields):
                start = q * rows + f * edge
                line = jnp.sum(jnp.where(here, layer[start:start + edge], 0.0), axis=0, keepdims=True)
                faces[q, 2 + e, f:f + 1, :] = line


def jump_kernel(place, side, patch, own, near, cross, jump, *, count, fields, devices):
    linear = place[2]
    even = within(linear, 2) == 0
    for q in range(count):
        for e in range(6):
            u = side[q, e]
            n = patch[q, e]
            at = linear + u - 1
            present = (u < 3) & (at >= 0) & (at < devices)
            other = e ^ 1
            inside = (u == 2) == even
            ghost = jnp.where(
                u == 1, own[n, other], jnp.where(inside, near[n, other], cross[n, other])
            )
            line = jnp.where(present, ghost - own[q, e], 0.0)
            for f in range(fields):
                jump[q, f, e:e + 1, :] = line[f:f + 1]


def body(
    old_data, pair_old, pair_slot, pair_shift, pair_dest, new_ratio, neighbor_side, neighbor_patch
):
    patches, fields, edge, lanes = old_data.shape
    pairs = pair_old.shape[0]
    count = neighbor_side.shape[0]
    rows = fields * edge
    half = lanes // 2
    size_x = lax.axis_size("gx")
    size_y = lax.axis_size("gy")
    chips_y = lax.axis_size("gz_0")
    cores = lax.axis_size("gz_1")
    devices = size_x * size_y * chips_y * cores
    index_y = lax.axis_index("gy")
    core = lax.axis_index("gz_1")
    index_x = lax.axis_index("gx")
    chip_y = lax.axis_index("gz_0")
    linear = ((index_x * size_y + index_y) * chips_y + chip_y) * cores + core
    place = jnp.stack([index_y, core, linear, index_x, chip_y]).astype(I32)
    own = old_data.reshape(patches, rows, lanes)
    swap = [(i, cores - 1 - i) for i in range(cores)]
    owners = size_x * chips_y * count
    smem = pl.BlockSpec(memory_space=SMEM)
    vmem = pl.BlockSpec(memory_space=VMEM)
    hbm = pl.BlockSpec(memory_space=HBM)
    params = pltpu.CompilerParams(vmem_limit_bytes=24 * 1024 * 1024)
    mass, packed = pl.pallas_call(
        functools.partial(
            head_kernel, patches=patches, fields=fields, edge=edge, size_y=size_y,
            size_z=chips_y * cores, new_count=count, pairs=pairs,
        ),
        out_shape=(
            jax.ShapeDtypeStruct((size_x * chips_y * cores, 8, half), F32),
            VMEM((patches * rows + META_ROWS, lanes), F32),
        ),
        in_specs=[smem] * 5 + [vmem] * 4 + [hbm, hbm],
        out_specs=(vmem, vmem),
        scratch_shapes=[
            pltpu.SMEM(new_ratio.shape, I32),
            pltpu.VMEM((patches, edge, lanes), F32),
            DMA((2,)),
        ],
        compiler_params=params,
        name="head",
    )(
        place, pair_old, pair_slot, pair_shift, pair_dest,
        pair_old.reshape(1, pairs), pair_slot.reshape(1, pairs), pair_shift, pair_dest,
        slow(new_ratio), slow(old_data.reshape(patches * rows, lanes)),
    )
    peer = lax.ppermute(packed, "gz_1", swap)
    plane = lax.all_to_all(mass, PLANE, 0, 0, tiled=True)
    partials = pl.pallas_call(
        functools.partial(
            partials_kernel, patches=patches, fields=fields, edge=edge, size_x=size_x,
            size_y=size_y, chips_y=chips_y, cores=cores, new_count=count, pairs=pairs,
        ),
        out_shape=HBM((owners, rows, lanes), F32),
        in_specs=[smem] * 5 + [hbm, hbm, vmem],
        out_specs=vmem,
        scratch_shapes=[
            pltpu.SMEM(new_ratio.shape, I32),
            pltpu.VMEM((patches, rows, lanes), F32),
            pltpu.VMEM((META_ROWS, half), I32),
            pltpu.SMEM((META_ROWS, half), I32),
            pltpu.SMEM((5, 2 * pairs + UNROLL), I32),
            pltpu.VMEM((2 * patches, 2 * rows, lanes), BF16),
            pltpu.VMEM((lanes, lanes), I32),
            pltpu.VMEM((rows, 2 * rows), I32),
            DMA((3,)),
        ],
        compiler_params=params,
        name="partials",
    )(place, pair_old, pair_slot, pair_shift, pair_dest, slow(new_ratio), slow(own), fast(peer))

    first_groups, last_groups = mixed_groups(size_x, size_y, chips_y, cores)
    first = lax.all_to_all(partials, ALL_AXES, 0, 0, tiled=True, axis_index_groups=first_groups)
    total = jnp.sum(plane, axis=0)

    def crossed(value, distance):
        return value + lax.ppermute(value, "gy", [(i, i ^ distance) for i in range(size_y)])

    total = crossed(total, 8)
    total = crossed(total, 4)
    total = crossed(total, 2)
    total = crossed(total, 1)
    kept = owners // size_x
    folded = pl.pallas_call(
        functools.partial(fold_kernel, sources=size_x, chunk=count),
        out_shape=HBM((kept, rows, lanes), F32),
        in_specs=[hbm],
        out_specs=hbm,
        scratch_shapes=[
            pltpu.VMEM((owners, rows, lanes), F32),
            pltpu.VMEM((kept, rows, lanes), F32),
            DMA((kept // count, size_x)),
            DMA((kept // count,)),
        ],
        compiler_params=params,
        name="fold",
    )(slow(first))
    last = lax.all_to_all(folded, ALL_AXES, 0, 0, tiled=True, axis_index_groups=last_groups)
    new_data, faces = pl.pallas_call(
        functools.partial(gather_kernel, count=count, fields=fields, edge=edge),
        out_shape=(
            jax.ShapeDtypeStruct((count * rows, lanes), F32),
            VMEM((count, 6, fields, lanes), F32),
        ),
        in_specs=[vmem],
        out_specs=(vmem, vmem),
        compiler_params=params,
        name="gather",
    )(fast(last))
    cross = swapped(faces, 1)
    near = swapped(faces, 0)
    interface_jump = pl.pallas_call(
        functools.partial(jump_kernel, count=count, fields=fields, devices=devices),
        out_shape=jax.ShapeDtypeStruct((count, fields, 6, lanes), F32),
        in_specs=[smem, smem, smem, vmem, vmem, vmem],
        out_specs=vmem,
        name="jump",
    )(place, neighbor_side, neighbor_patch, fast(faces), fast(near), fast(cross))
    total_cells = patches * devices * edge * lanes
    mass_totals = total[:fields, :2].T / total_cells
    return (new_data.reshape(count, fields, edge, lanes), interface_jump, mass_totals)


def solution(mesh):
    torus = Mesh(
        mesh.devices.reshape(mesh.shape["gx"], mesh.shape["gy"], 4, 2), ("gx", "gy", "gz_0", "gz_1")
    )
    return jax.shard_map(
        body,
        mesh=torus,
        in_specs=(
            P(ALL_AXES, None, None, None),
            P(ALL_AXES),
            P(ALL_AXES),
            P(ALL_AXES, None),
            P(ALL_AXES, None),
            P(),
            P(ALL_AXES, None),
            P(ALL_AXES, None),
        ),
        out_specs=(P(ALL_AXES, None, None, None), P(ALL_AXES, None, None, None), P()),
        check_vma=False,
    )
```

```python
import functools

import jax
import jax.numpy as jnp
from jax import lax
from jax.experimental import pallas as pl
from jax.experimental.pallas import tpu as pltpu
from jax.sharding import Mesh
from jax.sharding import PartitionSpec as P


ALL_AXES = ("gx", "gy", "gz_0", "gz_1")
PLANE = ("gx", "gz_0", "gz_1")
UNROLL = 8
META_ROWS = 8
BF16 = jnp.bfloat16
F32 = jnp.float32
I32 = jnp.int32
VMEM = pltpu.VMEM
SMEM = pltpu.SMEM
HBM = pltpu.HBM
DMA = pltpu.SemaphoreType.DMA


def swapped(block, first):
    devices = lax.axis_size(ALL_AXES)
    pairs = [(i, i + 1) for i in range(first, devices - 1, 2)]
    return lax.ppermute(block, ALL_AXES, pairs + [(j, i) for i, j in pairs])


def fast(block):
    return pltpu.with_memory_space_constraint(block, VMEM)


def mixed_groups(size_x, size_y, chips_y, cores):
    def device(x, z, y, c):
        return ((x * size_y + z) * chips_y + y) * cores + c

    along_x, along_y = [], []
    for c in range(cores):
        lines_x = [[device(x, z, y, c) for x in range(size_x)] for z in range(size_y) for y in range(chips_y)]
        lines_y = [[device(x, z, y, c) for y in range(chips_y)] for z in range(size_y) for x in range(size_x)]
        along_x += lines_x if c == 0 else lines_y
        along_y += lines_y if c == 0 else lines_x
    return along_x, along_y


def slow(block):
    return pltpu.with_memory_space_constraint(block, HBM)


def halves(block):
    high = block.astype(BF16)
    low = (block - high.astype(F32)).astype(BF16)
    return high, low


def over(value, size):
    return value >> (size.bit_length() - 1)


def within(value, size):
    return value & (size - 1)


def iota(shape, dim):
    return lax.broadcasted_iota(I32, shape, dim)


def head_kernel(
    place, pair_old, pair_slot, pair_shift, pair_dest, old_row, slot_row, dest_row, shift_rows, ratio_in, own_in,
    out, packed, ratio, counts, sems,
    *, patches, fields, edge, size_y, size_z, new_count, pairs,
):
    lanes = edge * edge
    half = lanes // 2
    index_y = place[0]
    ratio_copy = pltpu.make_async_copy(ratio_in, ratio, sems.at[0])
    rows = fields * edge
    cells = patches * rows
    own_copy = pltpu.make_async_copy(own_in, packed.at[pl.ds(0, cells)], sems.at[1])
    ratio_copy.start()
    own_copy.start()
    packed[cells:] = jnp.zeros((META_ROWS, lanes), F32)
    at = cells
    for rows_in in (old_row, slot_row, dest_row, shift_rows):
        size = rows_in.shape[0]
        packed[at:at + size, 0:pairs] = rows_in[...].astype(F32)
        at += size
    counts[...] = jnp.zeros_like(counts)
    at_x = iota((edge, lanes), 0)
    at_y = over(iota((edge, lanes), 1), edge)
    at_z = within(iota((edge, lanes), 1), edge)

    def count(p, carry):
        dest = pair_dest[0, p]
        owner = (over(dest, size_z) * size_y + index_y) * size_z + within(dest, size_z)
        reach = edge * ratio[owner * new_count + pair_slot[p]]
        hit = jnp.full((edge, lanes), True)
        for a, at in enumerate((at_x, at_y, at_z)):
            distance = at - pair_shift[a, p]
            hit = hit & (distance >= 0) & (distance < reach)
        o = pair_old[p]
        counts[o] = counts[o] + jnp.where(hit, 1.0, 0.0)
        return carry

    ratio_copy.wait()
    lax.fori_loop(0, pairs, count, 0)
    own_copy.wait()

    def add(o, sums):
        weight = counts[o]
        olds, news = sums
        old_list, new_list = [], []
        for f in range(fields):
            block = packed[pl.ds(o * rows + f * edge, edge)]
            scaled = block * weight
            old_list.append(olds[f] + (block[:, :half] + block[:, half:]))
            new_list.append(news[f] + (scaled[:, :half] + scaled[:, half:]))
        return tuple(old_list), tuple(new_list)

    zero = tuple(jnp.zeros((edge, half), F32) for _ in range(fields))
    olds, news = lax.fori_loop(0, patches, add, (zero, zero))
    lane = iota((1, half), 1)
    lines = []
    for f in range(fields):
        old_f = jnp.sum(olds[f], keepdims=True)
        new_f = jnp.sum(news[f], keepdims=True)
        lines.append(jnp.where(lane == 0, old_f, jnp.where(lane == 1, new_f, 0.0)))
    lines.append(jnp.zeros((8 - fields, half), F32))
    packed = jnp.concatenate(lines, axis=0)
    out[...] = jnp.broadcast_to(packed[None], out.shape)


def partials_kernel(
    place, pair_old, pair_slot, pair_shift, pair_dest, ratio_in, own_in, peer,
    out, ratio, own, meta_v, meta, table, order, ends, sums, split, code_k, code_x, sems, out_sems,
    *, patches, fields, edge, size_y, chips_y, cores, new_count, pairs,
):
    rows = fields * edge
    lanes = edge * edge
    index_y = place[0]
    core = place[1]
    size_z = chips_y * cores
    for size in (edge, size_z, cores):
        assert size & (size - 1) == 0
    ratio_copy = pltpu.make_async_copy(ratio_in, ratio, sems.at[0])
    own_copy = pltpu.make_async_copy(own_in, own, sems.at[1])
    ratio_copy.start()
    own_copy.start()
    cells = patches * rows
    meta_v[...] = peer[cells:cells + META_ROWS, 0:meta_v.shape[1]].astype(I32)
    meta_copy = pltpu.make_async_copy(meta_v, meta, sems.at[2])
    meta_copy.start()

    def prepare(o, carry):
        high, low = halves(own[o])
        split[o, 0:rows] = high
        split[o, rows:2 * rows] = low
        high, low = halves(peer[pl.ds(o * rows, rows)])
        split[patches + o, 0:rows] = high
        split[patches + o, rows:2 * rows] = low
        return carry

    sums[...] = jnp.zeros_like(sums)
    chunks = ends.shape[0]
    chunk_size = out.shape[0] // chunks
    spare = out.shape[0]
    cell = iota((lanes, lanes), 0)
    code_k[...] = over(cell, edge) * 4096 + within(cell, edge)
    row = iota((rows, 2 * rows), 0)
    col = iota((rows, 2 * rows), 1) % rows
    code_x[...] = (over(col, edge) - over(row, edge)) * 4096 + within(col, edge)

    def enlist(found, base, old, slot, shift, dest):
        mine = within(dest, cores) == core

        @pl.when(mine)
        def _():
            table[0, found] = base + old
            iz = within(dest, size_z)
            ix = over(dest, size_z)
            owner = (ix * size_y + index_y) * size_z + iz
            table[1, found] = ratio[owner * new_count + slot]
            table[2, found] = shift[0]
            table[3, found] = shift[1] * 4096 + shift[2]
            chip_y = over(iz, cores)
            chunk = jnp.where(core == 0, ix, chip_y)
            table[4, found] = (chunk * chips_y + jnp.where(core == 0, chip_y, ix)) * new_count + slot
            rank = ends[chunk]
            table[5, found] = chunk
            table[6, found] = rank
            ends[chunk] = rank + 1

        return found + mine.astype(I32)

    def enlist_own(p, found):
        shift = [pair_shift[a, p] for a in range(3)]
        return enlist(found, 0, pair_old[p], pair_slot[p], shift, pair_dest[0, p])

    def enlist_peer(p, found):
        shift = [meta[3 + a, p] for a in range(3)]
        return enlist(found, patches, meta[0, p], meta[1, p], shift, meta[2, p])

    for k in range(chunks):
        ends[k] = 0
    ratio_copy.wait()
    found = lax.fori_loop(0, pairs, enlist_own, jnp.int32(0))
    meta_copy.wait()
    found = lax.fori_loop(0, pairs, enlist_peer, found)

    before = jnp.int32(0)
    starts = []
    for k in range(chunks):
        starts.append(before)
        before = before + ends[k]
        ends[k] = starts[k]

    def place_in_order(p, carry):
        order[ends[table[5, p]] + table[6, p]] = p
        return carry

    lax.fori_loop(0, found, place_in_order, 0)
    stops = starts[1:] + [found]
    blank = table.shape[1] - 1
    for field, value in enumerate((0, 1, 0, 0, spare)):
        table[field, blank] = value
    for extra in range(UNROLL - 1):
        order[found + extra] = blank

    def copy_out(k):
        at = pl.ds(k * chunk_size, chunk_size)
        return pltpu.make_async_copy(sums.at[at], out.at[at], out_sems.at[k])

    def send(low, high):
        for k in range(chunks):

            @pl.when((stops[k] > low) & (stops[k] <= high))
            def _():
                copy_out(k).start()

    own_copy.wait()
    lax.fori_loop(0, patches, prepare, 0)

    lane_k = iota((1, lanes), 1)
    lane_code = over(lane_k, edge) * 4096 + within(lane_k, edge)
    row_x = within(iota((rows, 1), 0), edge)

    def remap(step, carry):
        results = []
        for u in range(UNROLL):
            p = order[step * UNROLL + u]
            r = table[1, p]
            inverse = jnp.where(r == 2, 0.5, 1.0).astype(F32)
            spread = code_x[...] - (row_x * r + table[2, p])
            weight_x = jnp.where((spread & ~(r - 1)) == 0, inverse, 0.0).astype(BF16)
            section = jnp.dot(weight_x, split[table[0, p]], preferred_element_type=F32)
            spread = code_k[...] - (lane_code * r + table[3, p])
            weight_k = jnp.where((spread & ~((r - 1) * 4097)) == 0, inverse * inverse, 0.0).astype(BF16)
            high, low = halves(section)
            stacked = jnp.concatenate([high, low], axis=0)
            product = jnp.dot(stacked, weight_k, preferred_element_type=F32)
            part = product[:rows] + product[rows:]
            results.append((p, part))
        for p, part in results:
            to = table[4, p]
            sums[to] = sums[to] + part
        send(step * UNROLL, (step + 1) * UNROLL)
        return carry

    steps = (found + UNROLL - 1) // UNROLL
    send(-1, 0)
    lax.fori_loop(0, steps, remap, 0)
    for k in range(chunks):
        copy_out(k).wait()


def fold_kernel(a, out, parts, sums, in_sems, out_sems, *, sources, chunk):
    kept = out.shape[0]
    chunks = kept // chunk
    copies = [
        [
            pltpu.make_async_copy(
                a.at[pl.ds(s * kept + j * chunk, chunk)], parts.at[pl.ds(s * kept + j * chunk, chunk)], in_sems.at[j, s]
            )
            for s in range(sources)
        ]
        for j in range(chunks)
    ]
    for row in copies:
        for copy in row:
            copy.start()
    outs = []
    for j in range(chunks):
        for copy in copies[j]:
            copy.wait()
        at = j * chunk
        total = parts[at:at + chunk]
        for s in range(1, sources):
            total = total + parts[s * kept + at:s * kept + at + chunk]
        sums[at:at + chunk] = total
        outs.append(pltpu.make_async_copy(sums.at[pl.ds(at, chunk)], out.at[pl.ds(at, chunk)], out_sems.at[j]))
        outs[-1].start()
    for copy in outs:
        copy.wait()


def gather_kernel(a, new_data, faces, *, count, fields, edge):
    rows = fields * edge
    lanes = edge * edge
    sources = a.shape[0] // count
    sums = []
    for q in range(count):
        total = a[q]
        for s in range(1, sources):
            total = total + a[s * count + q]
        sums.append(total)
    whole = jnp.concatenate(sums, axis=0)
    new_data[...] = whole
    high, low = halves(whole)
    stacked = jnp.concatenate([high, low], axis=0)
    source = iota((lanes, lanes), 0)
    target = within(iota((lanes, lanes), 1), edge)
    here = over(iota((edge, lanes), 1), edge) == iota((edge, lanes), 0)
    picks = (
        source == target,
        source == target + (lanes - edge),
        source == target * edge,
        source == target * edge + (edge - 1),
    )
    for q in range(count):
        for f in range(fields):
            start = q * rows + f * edge
            faces[q, 0, f:f + 1, :] = whole[start:start + 1]
            faces[q, 1, f:f + 1, :] = whole[start + edge - 1:start + edge]
    for e, pick in enumerate(picks):
        weight = jnp.where(pick, 1.0, 0.0).astype(BF16)
        product = jnp.dot(stacked, weight, preferred_element_type=F32)
        layer = product[:count * rows] + product[count * rows:]
        for q in range(count):
            for f in range(fields):
                start = q * rows + f * edge
                line = jnp.sum(jnp.where(here, layer[start:start + edge], 0.0), axis=0, keepdims=True)
                faces[q, 2 + e, f:f + 1, :] = line


def jump_kernel(place, side, patch, own, near, cross, jump, *, count, fields, devices):
    linear = place[2]
    even = within(linear, 2) == 0
    for q in range(count):
        for e in range(6):
            u = side[q, e]
            n = patch[q, e]
            at = linear + u - 1
            present = (u < 3) & (at >= 0) & (at < devices)
            other = e ^ 1
            inside = (u == 2) == even
            ghost = jnp.where(
                u == 1, own[n, other], jnp.where(inside, near[n, other], cross[n, other])
            )
            line = jnp.where(present, ghost - own[q, e], 0.0)
            for f in range(fields):
                jump[q, f, e:e + 1, :] = line[f:f + 1]


def body(
    old_data, pair_old, pair_slot, pair_shift, pair_dest, new_ratio, neighbor_side, neighbor_patch
):
    patches, fields, edge, lanes = old_data.shape
    pairs = pair_old.shape[0]
    count = neighbor_side.shape[0]
    rows = fields * edge
    half = lanes // 2
    size_x = lax.axis_size("gx")
    size_y = lax.axis_size("gy")
    chips_y = lax.axis_size("gz_0")
    cores = lax.axis_size("gz_1")
    devices = size_x * size_y * chips_y * cores
    index_y = lax.axis_index("gy")
    core = lax.axis_index("gz_1")
    index_x = lax.axis_index("gx")
    chip_y = lax.axis_index("gz_0")
    linear = ((index_x * size_y + index_y) * chips_y + chip_y) * cores + core
    place = jnp.stack([index_y, core, linear, index_x, chip_y]).astype(I32)
    own = old_data.reshape(patches, rows, lanes)
    table = [slow(pair_old), slow(pair_slot), slow(pair_shift.T), slow(pair_dest.T)]
    swap = [(i, cores - 1 - i) for i in range(cores)]
    owners = size_x * chips_y * count
    smem = pl.BlockSpec(memory_space=SMEM)
    vmem = pl.BlockSpec(memory_space=VMEM)
    hbm = pl.BlockSpec(memory_space=HBM)
    params = pltpu.CompilerParams(vmem_limit_bytes=24 * 1024 * 1024)
    mass, packed = pl.pallas_call(
        functools.partial(
            head_kernel, patches=patches, fields=fields, edge=edge, size_y=size_y,
            size_z=chips_y * cores, new_count=count, pairs=pairs,
        ),
        out_shape=(
            jax.ShapeDtypeStruct((size_x * chips_y * cores, 8, half), F32),
            VMEM((patches * rows + META_ROWS, lanes), F32),
        ),
        in_specs=[smem] * 5 + [vmem] * 4 + [hbm, hbm],
        out_specs=(vmem, vmem),
        scratch_shapes=[
            pltpu.SMEM(new_ratio.shape, I32),
            pltpu.VMEM((patches, edge, lanes), F32),
            DMA((2,)),
        ],
        compiler_params=params,
        name="head",
    )(
        place, *table, slow(pair_old.reshape(1, pairs)), slow(pair_slot.reshape(1, pairs)), *table[:1:-1],
        slow(new_ratio), slow(old_data.reshape(patches * rows, lanes)),
    )
    peer = lax.ppermute(packed, "gz_1", swap)
    plane = lax.all_to_all(mass, PLANE, 0, 0, tiled=True)
    partials = pl.pallas_call(
        functools.partial(
            partials_kernel, patches=patches, fields=fields, edge=edge,
            size_y=size_y, chips_y=chips_y, cores=cores, new_count=count, pairs=pairs,
        ),
        out_shape=HBM((owners, rows, lanes), F32),
        in_specs=[smem] * 5 + [hbm, hbm, vmem],
        out_specs=hbm,
        scratch_shapes=[
            pltpu.SMEM(new_ratio.shape, I32),
            pltpu.VMEM((patches, rows, lanes), F32),
            pltpu.VMEM((META_ROWS, half), I32),
            pltpu.SMEM((META_ROWS, half), I32),
            pltpu.SMEM((7, 2 * pairs + 1), I32),
            pltpu.SMEM((2 * pairs + UNROLL,), I32),
            pltpu.SMEM((size_x,), I32),
            pltpu.VMEM((owners + 1, rows, lanes), F32),
            pltpu.VMEM((2 * patches, 2 * rows, lanes), BF16),
            pltpu.VMEM((lanes, lanes), I32),
            pltpu.VMEM((rows, 2 * rows), I32),
            DMA((3,)),
            DMA((size_x,)),
        ],
        compiler_params=params,
        name="partials",
    )(place, *table, slow(new_ratio), slow(own), fast(peer))

    first_groups, last_groups = mixed_groups(size_x, size_y, chips_y, cores)
    first = lax.all_to_all(partials, ALL_AXES, 0, 0, tiled=True, axis_index_groups=first_groups)
    total = jnp.sum(plane, axis=0)

    def crossed(value, distance):
        return value + lax.ppermute(value, "gy", [(i, i ^ distance) for i in range(size_y)])

    total = crossed(total, 8)
    total = crossed(total, 4)
    total = crossed(total, 2)
    total = crossed(total, 1)
    kept = owners // size_x
    folded = pl.pallas_call(
        functools.partial(fold_kernel, sources=size_x, chunk=count),
        out_shape=HBM((kept, rows, lanes), F32),
        in_specs=[hbm],
        out_specs=hbm,
        scratch_shapes=[
            pltpu.VMEM((owners, rows, lanes), F32),
            pltpu.VMEM((kept, rows, lanes), F32),
            DMA((kept // count, size_x)),
            DMA((kept // count,)),
        ],
        compiler_params=params,
        name="fold",
    )(slow(first))
    last = lax.all_to_all(folded, ALL_AXES, 0, 0, tiled=True, axis_index_groups=last_groups)
    new_data, faces = pl.pallas_call(
        functools.partial(gather_kernel, count=count, fields=fields, edge=edge),
        out_shape=(
            jax.ShapeDtypeStruct((count * rows, lanes), F32),
            VMEM((count, 6, fields, lanes), F32),
        ),
        in_specs=[vmem],
        out_specs=(vmem, vmem),
        compiler_params=params,
        name="gather",
    )(fast(last))
    cross = swapped(faces, 1)
    near = swapped(faces, 0)
    interface_jump = pl.pallas_call(
        functools.partial(jump_kernel, count=count, fields=fields, devices=devices),
        out_shape=jax.ShapeDtypeStruct((count, fields, 6, lanes), F32),
        in_specs=[smem, smem, smem, vmem, vmem, vmem],
        out_specs=vmem,
        name="jump",
    )(place, neighbor_side, neighbor_patch, fast(faces), fast(near), fast(cross))
    total_cells = patches * devices * edge * lanes
    mass_totals = total[:fields, :2].T / total_cells
    return (new_data.reshape(count, fields, edge, lanes), interface_jump, mass_totals)


def solution(mesh):
    torus = Mesh(
        mesh.devices.reshape(mesh.shape["gx"], mesh.shape["gy"], 4, 2), ("gx", "gy", "gz_0", "gz_1")
    )
    return jax.shard_map(
        body,
        mesh=torus,
        in_specs=(
            P(ALL_AXES, None, None, None),
            P(ALL_AXES),
            P(ALL_AXES),
            P(ALL_AXES, None),
            P(ALL_AXES, None),
            P(),
            P(ALL_AXES, None),
            P(ALL_AXES, None),
        ),
        out_specs=(P(ALL_AXES, None, None, None), P(ALL_AXES, None, None, None), P()),
        check_vma=False,
    )
```

```python
import functools

import jax
import jax.numpy as jnp
from jax import lax
from jax.experimental import pallas as pl
from jax.experimental.pallas import tpu as pltpu
from jax.sharding import Mesh
from jax.sharding import PartitionSpec as P


ALL_AXES = ("gx", "gy", "gz_0", "gz_1")
PLANE = ("gx", "gz_0", "gz_1")
UNROLL = 8
META_ROWS = 8
FACE_ROWS = 32
BF16 = jnp.bfloat16
F32 = jnp.float32
I32 = jnp.int32
VMEM = pltpu.VMEM
SMEM = pltpu.SMEM
HBM = pltpu.HBM
DMA = pltpu.SemaphoreType.DMA


def swapped(block, first):
    devices = lax.axis_size(ALL_AXES)
    pairs = [(i, i + 1) for i in range(first, devices - 1, 2)]
    return lax.ppermute(block, ALL_AXES, pairs + [(j, i) for i, j in pairs])


def fast(block):
    return pltpu.with_memory_space_constraint(block, VMEM)


def mixed_groups(size_x, size_y, chips_y, cores):
    def device(x, z, y, c):
        return ((x * size_y + z) * chips_y + y) * cores + c

    along_x, along_y = [], []
    for c in range(cores):
        lines_x = [[device(x, z, y, c) for x in range(size_x)] for z in range(size_y) for y in range(chips_y)]
        lines_y = [[device(x, z, y, c) for y in range(chips_y)] for z in range(size_y) for x in range(size_x)]
        along_x += lines_x if c == 0 else lines_y
        along_y += lines_y if c == 0 else lines_x
    return along_x, along_y


def slow(block):
    return pltpu.with_memory_space_constraint(block, HBM)


def halves(block):
    high = block.astype(BF16)
    low = (block - high.astype(F32)).astype(BF16)
    return high, low


def over(value, size):
    return value >> (size.bit_length() - 1)


def within(value, size):
    return value & (size - 1)


def iota(shape, dim):
    return lax.broadcasted_iota(I32, shape, dim)


def head_kernel(
    place, pair_old, pair_slot, pair_shift, pair_dest, old_row, slot_row, dest_row, shift_rows, ratio_in, own_in,
    out, packed, ratio, counts, sems,
    *, patches, fields, edge, size_y, size_z, new_count, pairs,
):
    lanes = edge * edge
    half = lanes // 2
    index_y = place[0]
    ratio_copy = pltpu.make_async_copy(ratio_in, ratio, sems.at[0])
    rows = fields * edge
    cells = patches * rows
    own_copy = pltpu.make_async_copy(own_in, packed.at[pl.ds(0, cells)], sems.at[1])
    ratio_copy.start()
    own_copy.start()
    packed[cells:] = jnp.zeros((META_ROWS, lanes), F32)
    at = cells
    for rows_in in (old_row, slot_row, dest_row, shift_rows):
        size = rows_in.shape[0]
        packed[at:at + size, 0:pairs] = rows_in[...].astype(F32)
        at += size
    counts[...] = jnp.zeros_like(counts)
    at_x = iota((edge, lanes), 0)
    at_y = over(iota((edge, lanes), 1), edge)
    at_z = within(iota((edge, lanes), 1), edge)

    def count(p, carry):
        dest = pair_dest[0, p]
        owner = (over(dest, size_z) * size_y + index_y) * size_z + within(dest, size_z)
        reach = edge * ratio[owner * new_count + pair_slot[p]]
        hit = jnp.full((edge, lanes), True)
        for a, at in enumerate((at_x, at_y, at_z)):
            distance = at - pair_shift[a, p]
            hit = hit & (distance >= 0) & (distance < reach)
        o = pair_old[p]
        counts[o] = counts[o] + jnp.where(hit, 1.0, 0.0)
        return carry

    ratio_copy.wait()
    lax.fori_loop(0, pairs, count, 0)
    own_copy.wait()

    def add(o, sums):
        weight = counts[o]
        olds, news = sums
        old_list, new_list = [], []
        for f in range(fields):
            block = packed[pl.ds(o * rows + f * edge, edge)]
            scaled = block * weight
            old_list.append(olds[f] + (block[:, :half] + block[:, half:]))
            new_list.append(news[f] + (scaled[:, :half] + scaled[:, half:]))
        return tuple(old_list), tuple(new_list)

    zero = tuple(jnp.zeros((edge, half), F32) for _ in range(fields))
    olds, news = lax.fori_loop(0, patches, add, (zero, zero))
    lane = iota((1, half), 1)
    lines = []
    for f in range(fields):
        old_f = jnp.sum(olds[f], keepdims=True)
        new_f = jnp.sum(news[f], keepdims=True)
        lines.append(jnp.where(lane == 0, old_f, jnp.where(lane == 1, new_f, 0.0)))
    lines.append(jnp.zeros((8 - fields, half), F32))
    packed = jnp.concatenate(lines, axis=0)
    out[...] = jnp.broadcast_to(packed[None], out.shape)


def partials_kernel(
    place, pair_old, pair_slot, pair_shift, pair_dest, ratio_in, own_in, peer,
    out, ratio, own, meta_v, meta, table, order, ends, sums, split, code_k, code_x, sems, out_sems,
    *, patches, fields, edge, size_y, chips_y, cores, new_count, pairs,
):
    rows = fields * edge
    lanes = edge * edge
    index_y = place[0]
    core = place[1]
    size_z = chips_y * cores
    for size in (edge, size_z, cores):
        assert size & (size - 1) == 0
    ratio_copy = pltpu.make_async_copy(ratio_in, ratio, sems.at[0])
    own_copy = pltpu.make_async_copy(own_in, own, sems.at[1])
    ratio_copy.start()
    own_copy.start()
    cells = patches * rows
    meta_v[...] = peer[cells:cells + META_ROWS, 0:meta_v.shape[1]].astype(I32)
    meta_copy = pltpu.make_async_copy(meta_v, meta, sems.at[2])
    meta_copy.start()

    def prepare(o, carry):
        high, low = halves(own[o])
        split[o, 0:rows] = high
        split[o, rows:2 * rows] = low
        high, low = halves(peer[pl.ds(o * rows, rows)])
        split[patches + o, 0:rows] = high
        split[patches + o, rows:2 * rows] = low
        return carry

    sums[...] = jnp.zeros_like(sums)
    chunks = ends.shape[0]
    chunk_size = out.shape[0] // chunks
    spare = out.shape[0]
    cell = iota((lanes, lanes), 0)
    code_k[...] = over(cell, edge) * 4096 + within(cell, edge)
    row = iota((rows, 2 * rows), 0)
    col = iota((rows, 2 * rows), 1) % rows
    code_x[...] = (over(col, edge) - over(row, edge)) * 4096 + within(col, edge)

    def enlist(found, base, old, slot, shift, dest):
        mine = jnp.where(within(dest, cores) == core, 1, 0)
        iz = within(dest, size_z)
        ix = over(dest, size_z)
        owner = (ix * size_y + index_y) * size_z + iz
        chip_y = over(iz, cores)
        chunk = jnp.where(core == 0, ix, chip_y)
        rank = ends[chunk]
        table[0, found] = base + old
        table[1, found] = ratio[owner * new_count + slot]
        table[2, found] = shift[0]
        table[3, found] = shift[1] * 4096 + shift[2]
        table[4, found] = (chunk * chips_y + jnp.where(core == 0, chip_y, ix)) * new_count + slot
        table[5, found] = chunk
        table[6, found] = rank
        ends[chunk] = rank + mine
        return found + mine

    def enlist_own(p, found):
        shift = [pair_shift[a, p] for a in range(3)]
        return enlist(found, 0, pair_old[p], pair_slot[p], shift, pair_dest[0, p])

    def enlist_peer(p, found):
        shift = [meta[3 + a, p] for a in range(3)]
        return enlist(found, patches, meta[0, p], meta[1, p], shift, meta[2, p])

    for k in range(chunks):
        ends[k] = 0
    ratio_copy.wait()
    found = lax.fori_loop(0, pairs, enlist_own, jnp.int32(0), unroll=4)
    meta_copy.wait()
    found = lax.fori_loop(0, pairs, enlist_peer, found, unroll=4)

    before = jnp.int32(0)
    starts = []
    for k in range(chunks):
        starts.append(before)
        before = before + ends[k]
        ends[k] = starts[k]

    def place_in_order(p, carry):
        order[ends[table[5, p]] + table[6, p]] = p
        return carry

    lax.fori_loop(0, found, place_in_order, 0)
    stops = starts[1:] + [found]
    blank = table.shape[1] - 1
    for field, value in enumerate((0, 1, 0, 0, spare)):
        table[field, blank] = value
    for extra in range(UNROLL - 1):
        order[found + extra] = blank

    def copy_out(k):
        at = pl.ds(k * chunk_size, chunk_size)
        return pltpu.make_async_copy(sums.at[at], out.at[at], out_sems.at[k])

    def send(low, high):
        for k in range(chunks):

            @pl.when((stops[k] > low) & (stops[k] <= high))
            def _():
                copy_out(k).start()

    own_copy.wait()
    lax.fori_loop(0, patches, prepare, 0)

    lane_k = iota((1, lanes), 1)
    lane_code = over(lane_k, edge) * 4096 + within(lane_k, edge)
    row_x = within(iota((rows, 1), 0), edge)

    def remap(step, carry):
        results = []
        for u in range(UNROLL):
            p = order[step * UNROLL + u]
            r = table[1, p]
            inverse = jnp.where(r == 2, 0.5, 1.0).astype(F32)
            spread = code_x[...] - (row_x * r + table[2, p])
            weight_x = jnp.where((spread & ~(r - 1)) == 0, inverse, 0.0).astype(BF16)
            section = jnp.dot(weight_x, split[table[0, p]], preferred_element_type=F32)
            spread = code_k[...] - (lane_code * r + table[3, p])
            weight_k = jnp.where((spread & ~((r - 1) * 4097)) == 0, inverse * inverse, 0.0).astype(BF16)
            high, low = halves(section)
            stacked = jnp.concatenate([high, low], axis=0)
            product = jnp.dot(stacked, weight_k, preferred_element_type=F32)
            part = product[:rows] + product[rows:]
            results.append((p, part))
        for p, part in results:
            to = table[4, p]
            sums[to] = sums[to] + part
        send(step * UNROLL, (step + 1) * UNROLL)
        return carry

    steps = (found + UNROLL - 1) // UNROLL
    send(-1, 0)
    lax.fori_loop(0, steps, remap, 0)
    for k in range(chunks):
        copy_out(k).wait()


def fold_kernel(a, out, parts, sums, in_sems, out_sems, *, sources, chunk):
    kept = out.shape[0]
    chunks = kept // chunk
    copies = [
        [
            pltpu.make_async_copy(
                a.at[pl.ds(s * kept + j * chunk, chunk)], parts.at[pl.ds(s * kept + j * chunk, chunk)], in_sems.at[j, s]
            )
            for s in range(sources)
        ]
        for j in range(chunks)
    ]
    for row in copies:
        for copy in row:
            copy.start()
    outs = []
    for j in range(chunks):
        for copy in copies[j]:
            copy.wait()
        at = j * chunk
        total = parts[at:at + chunk]
        for s in range(1, sources):
            total = total + parts[s * kept + at:s * kept + at + chunk]
        sums[at:at + chunk] = total
        outs.append(pltpu.make_async_copy(sums.at[pl.ds(at, chunk)], out.at[pl.ds(at, chunk)], out_sems.at[j]))
        outs[-1].start()
    for copy in outs:
        copy.wait()


def gather_kernel(a, new_data, faces, *, count, fields, edge):
    rows = fields * edge
    lanes = edge * edge
    sources = a.shape[0] // count
    sums = []
    for q in range(count):
        total = a[q]
        for s in range(1, sources):
            total = total + a[s * count + q]
        sums.append(total)
    whole = jnp.concatenate(sums, axis=0)
    new_data[...] = whole
    high, low = halves(whole)
    stacked = jnp.concatenate([high, low], axis=0)
    source = iota((lanes, lanes), 0)
    target = within(iota((lanes, lanes), 1), edge)
    here = over(iota((edge, lanes), 1), edge) == iota((edge, lanes), 0)
    picks = (
        source == target,
        source == target + (lanes - edge),
        source == target * edge,
        source == target * edge + (edge - 1),
    )
    for q in range(count):
        faces[q, 6 * fields:, :] = jnp.zeros((FACE_ROWS - 6 * fields, lanes), F32)
        for f in range(fields):
            start = q * rows + f * edge
            faces[q, f:f + 1, :] = whole[start:start + 1]
            faces[q, fields + f:fields + f + 1, :] = whole[start + edge - 1:start + edge]
    for e, pick in enumerate(picks):
        weight = jnp.where(pick, 1.0, 0.0).astype(BF16)
        product = jnp.dot(stacked, weight, preferred_element_type=F32)
        layer = product[:count * rows] + product[count * rows:]
        for q in range(count):
            for f in range(fields):
                start = q * rows + f * edge
                line = jnp.sum(jnp.where(here, layer[start:start + edge], 0.0), axis=0, keepdims=True)
                at = (2 + e) * fields + f
                faces[q, at:at + 1, :] = line


def jump_kernel(place, side, patch, own, near, cross, jump, *, count, fields, devices):
    linear = place[2]
    even = within(linear, 2) == 0
    for q in range(count):
        for e in range(6):
            u = side[q, e]
            n = patch[q, e]
            at = linear + u - 1
            present = (u < 3) & (at >= 0) & (at < devices)
            other = pl.ds((e ^ 1) * fields, fields)
            inside = (u == 2) == even
            ghost = jnp.where(
                u == 1, own[n, other], jnp.where(inside, near[n, other], cross[n, other])
            )
            line = jnp.where(present, ghost - own[q, pl.ds(e * fields, fields)], 0.0)
            for f in range(fields):
                jump[q, f, e:e + 1, :] = line[f:f + 1]


def body(
    old_data, pair_old, pair_slot, pair_shift, pair_dest, new_ratio, neighbor_side, neighbor_patch
):
    patches, fields, edge, lanes = old_data.shape
    pairs = pair_old.shape[0]
    count = neighbor_side.shape[0]
    rows = fields * edge
    half = lanes // 2
    size_x = lax.axis_size("gx")
    size_y = lax.axis_size("gy")
    chips_y = lax.axis_size("gz_0")
    cores = lax.axis_size("gz_1")
    devices = size_x * size_y * chips_y * cores
    index_y = lax.axis_index("gy")
    core = lax.axis_index("gz_1")
    index_x = lax.axis_index("gx")
    chip_y = lax.axis_index("gz_0")
    linear = ((index_x * size_y + index_y) * chips_y + chip_y) * cores + core
    place = jnp.stack([index_y, core, linear, index_x, chip_y]).astype(I32)
    own = old_data.reshape(patches, rows, lanes)
    table = [slow(pair_old), slow(pair_slot), slow(pair_shift.T), slow(pair_dest.T)]
    swap = [(i, cores - 1 - i) for i in range(cores)]
    owners = size_x * chips_y * count
    smem = pl.BlockSpec(memory_space=SMEM)
    vmem = pl.BlockSpec(memory_space=VMEM)
    hbm = pl.BlockSpec(memory_space=HBM)
    params = pltpu.CompilerParams(vmem_limit_bytes=24 * 1024 * 1024)
    mass, packed = pl.pallas_call(
        functools.partial(
            head_kernel, patches=patches, fields=fields, edge=edge, size_y=size_y,
            size_z=chips_y * cores, new_count=count, pairs=pairs,
        ),
        out_shape=(
            jax.ShapeDtypeStruct((size_x * chips_y * cores, 8, half), F32),
            VMEM((patches * rows + META_ROWS, lanes), F32),
        ),
        in_specs=[smem] * 5 + [vmem] * 4 + [hbm, hbm],
        out_specs=(vmem, vmem),
        scratch_shapes=[
            pltpu.SMEM(new_ratio.shape, I32),
            pltpu.VMEM((patches, edge, lanes), F32),
            DMA((2,)),
        ],
        compiler_params=params,
        name="head",
    )(
        place, *table, slow(pair_old.reshape(1, pairs)), slow(pair_slot.reshape(1, pairs)), *table[:1:-1],
        slow(new_ratio), slow(old_data.reshape(patches * rows, lanes)),
    )
    peer = lax.ppermute(packed, "gz_1", swap)
    plane = lax.all_to_all(mass, PLANE, 0, 0, tiled=True)
    partials = pl.pallas_call(
        functools.partial(
            partials_kernel, patches=patches, fields=fields, edge=edge,
            size_y=size_y, chips_y=chips_y, cores=cores, new_count=count, pairs=pairs,
        ),
        out_shape=HBM((owners, rows, lanes), F32),
        in_specs=[smem] * 5 + [hbm, hbm, vmem],
        out_specs=hbm,
        scratch_shapes=[
            pltpu.SMEM(new_ratio.shape, I32),
            pltpu.VMEM((patches, rows, lanes), F32),
            pltpu.VMEM((META_ROWS, half), I32),
            pltpu.SMEM((META_ROWS, half), I32),
            pltpu.SMEM((7, 2 * pairs + 1), I32),
            pltpu.SMEM((2 * pairs + UNROLL,), I32),
            pltpu.SMEM((size_x,), I32),
            pltpu.VMEM((owners + 1, rows, lanes), F32),
            pltpu.VMEM((2 * patches, 2 * rows, lanes), BF16),
            pltpu.VMEM((lanes, lanes), I32),
            pltpu.VMEM((rows, 2 * rows), I32),
            DMA((3,)),
            DMA((size_x,)),
        ],
        compiler_params=params,
        name="partials",
    )(place, *table, slow(new_ratio), slow(own), fast(peer))

    first_groups, last_groups = mixed_groups(size_x, size_y, chips_y, cores)
    first = lax.all_to_all(partials, ALL_AXES, 0, 0, tiled=True, axis_index_groups=first_groups)
    total = jnp.sum(plane, axis=0)

    def crossed(value, distance):
        return value + lax.ppermute(value, "gy", [(i, i ^ distance) for i in range(size_y)])

    total = crossed(total, 8)
    total = crossed(total, 4)
    total = crossed(total, 2)
    total = crossed(total, 1)
    kept = owners // size_x
    folded = pl.pallas_call(
        functools.partial(fold_kernel, sources=size_x, chunk=count),
        out_shape=HBM((kept, rows, lanes), F32),
        in_specs=[hbm],
        out_specs=hbm,
        scratch_shapes=[
            pltpu.VMEM((owners, rows, lanes), F32),
            pltpu.VMEM((kept, rows, lanes), F32),
            DMA((kept // count, size_x)),
            DMA((kept // count,)),
        ],
        compiler_params=params,
        name="fold",
    )(slow(first))
    last = lax.all_to_all(folded, ALL_AXES, 0, 0, tiled=True, axis_index_groups=last_groups)
    new_data, faces = pl.pallas_call(
        functools.partial(gather_kernel, count=count, fields=fields, edge=edge),
        out_shape=(
            jax.ShapeDtypeStruct((count * rows, lanes), F32),
            VMEM((count, FACE_ROWS, lanes), F32),
        ),
        in_specs=[vmem],
        out_specs=(vmem, vmem),
        compiler_params=params,
        name="gather",
    )(fast(last))
    cross = swapped(faces, 1)
    near = swapped(faces, 0)
    interface_jump = pl.pallas_call(
        functools.partial(jump_kernel, count=count, fields=fields, devices=devices),
        out_shape=jax.ShapeDtypeStruct((count, fields, 6, lanes), F32),
        in_specs=[smem, smem, smem, vmem, vmem, vmem],
        out_specs=vmem,
        compiler_params=params,
        name="jump",
    )(place, neighbor_side, neighbor_patch, fast(faces), fast(near), fast(cross))
    total_cells = patches * devices * edge * lanes
    mass_totals = total[:fields, :2].T / total_cells
    return (new_data.reshape(count, fields, edge, lanes), interface_jump, mass_totals)


def solution(mesh):
    torus = Mesh(
        mesh.devices.reshape(mesh.shape["gx"], mesh.shape["gy"], 4, 2), ("gx", "gy", "gz_0", "gz_1")
    )
    return jax.shard_map(
        body,
        mesh=torus,
        in_specs=(
            P(ALL_AXES, None, None, None),
            P(ALL_AXES),
            P(ALL_AXES),
            P(ALL_AXES, None),
            P(ALL_AXES, None),
            P(),
            P(ALL_AXES, None),
            P(ALL_AXES, None),
        ),
        out_specs=(P(ALL_AXES, None, None, None), P(ALL_AXES, None, None, None), P()),
        check_vma=False,
    )
```

```python
import functools

import jax
import jax.numpy as jnp
from jax import lax
from jax.experimental import pallas as pl
from jax.experimental.pallas import tpu as pltpu
from jax.sharding import Mesh
from jax.sharding import PartitionSpec as P


ALL_AXES = ("gx", "gy", "gz_0", "gz_1")
PLANE = ("gx", "gz_0", "gz_1")
UNROLL = 8
META_ROWS = 8
FACE_ROWS = 32
BF16 = jnp.bfloat16
F32 = jnp.float32
I32 = jnp.int32
VMEM = pltpu.VMEM
SMEM = pltpu.SMEM
HBM = pltpu.HBM
DMA = pltpu.SemaphoreType.DMA


def swapped(block, first):
    devices = lax.axis_size(ALL_AXES)
    pairs = [(i, i + 1) for i in range(first, devices - 1, 2)]
    return lax.ppermute(block, ALL_AXES, pairs + [(j, i) for i, j in pairs])


def fast(block):
    return pltpu.with_memory_space_constraint(block, VMEM)


def mixed_groups(size_x, size_y, chips_y, cores):
    def device(x, z, y, c):
        return ((x * size_y + z) * chips_y + y) * cores + c

    along_x, along_y = [], []
    for c in range(cores):
        lines_x = [[device(x, z, y, c) for x in range(size_x)] for z in range(size_y) for y in range(chips_y)]
        lines_y = [[device(x, z, y, c) for y in range(chips_y)] for z in range(size_y) for x in range(size_x)]
        along_x += lines_x if c == 0 else lines_y
        along_y += lines_y if c == 0 else lines_x
    return along_x, along_y


def slow(block):
    return pltpu.with_memory_space_constraint(block, HBM)


def halves(block):
    high = block.astype(BF16)
    low = (block - high.astype(F32)).astype(BF16)
    return high, low


def over(value, size):
    return value >> (size.bit_length() - 1)


def within(value, size):
    return value & (size - 1)


def iota(shape, dim):
    return lax.broadcasted_iota(I32, shape, dim)


def head_kernel(
    place, pair_old, pair_slot, pair_shift, pair_dest, old_row, slot_row, dest_row, shift_rows, ratio_in, own_in,
    out, packed, ratio, counts, sems,
    *, patches, fields, edge, size_y, size_z, new_count, pairs,
):
    lanes = edge * edge
    half = lanes // 2
    index_y = place[0]
    ratio_copy = pltpu.make_async_copy(ratio_in, ratio, sems.at[0])
    rows = fields * edge
    cells = patches * rows
    own_copy = pltpu.make_async_copy(own_in, packed.at[pl.ds(0, cells)], sems.at[1])
    ratio_copy.start()
    own_copy.start()
    packed[cells:] = jnp.zeros((META_ROWS, lanes), F32)
    at = cells
    for rows_in in (old_row, slot_row, dest_row, shift_rows):
        size = rows_in.shape[0]
        packed[at:at + size, 0:pairs] = rows_in[...].astype(F32)
        at += size
    counts[...] = jnp.zeros_like(counts)
    at_x = iota((edge, lanes), 0)
    at_y = over(iota((edge, lanes), 1), edge)
    at_z = within(iota((edge, lanes), 1), edge)

    def count(p, carry):
        dest = pair_dest[0, p]
        owner = (over(dest, size_z) * size_y + index_y) * size_z + within(dest, size_z)
        reach = edge * ratio[owner * new_count + pair_slot[p]]
        hit = jnp.full((edge, lanes), True)
        for a, at in enumerate((at_x, at_y, at_z)):
            distance = at - pair_shift[a, p]
            hit = hit & (distance >= 0) & (distance < reach)
        o = pair_old[p]
        counts[o] = counts[o] + jnp.where(hit, 1.0, 0.0)
        return carry

    ratio_copy.wait()
    lax.fori_loop(0, pairs, count, 0, unroll=4)
    own_copy.wait()

    def add(o, sums):
        weight = counts[o]
        olds, news = sums
        old_list, new_list = [], []
        for f in range(fields):
            block = packed[pl.ds(o * rows + f * edge, edge)]
            scaled = block * weight
            old_list.append(olds[f] + (block[:, :half] + block[:, half:]))
            new_list.append(news[f] + (scaled[:, :half] + scaled[:, half:]))
        return tuple(old_list), tuple(new_list)

    zero = tuple(jnp.zeros((edge, half), F32) for _ in range(fields))
    olds, news = lax.fori_loop(0, patches, add, (zero, zero), unroll=2)
    lane = iota((8, half), 1)
    blank = [jnp.zeros((8 - fields, half), F32)]
    old_rows = jnp.concatenate([jnp.sum(block, axis=0, keepdims=True) for block in olds] + blank, axis=0)
    new_rows = jnp.concatenate([jnp.sum(block, axis=0, keepdims=True) for block in news] + blank, axis=0)
    old_mass = jnp.sum(old_rows, axis=1, keepdims=True)
    new_mass = jnp.sum(new_rows, axis=1, keepdims=True)
    both = jnp.where(lane == 0, old_mass, jnp.where(lane == 1, new_mass, 0.0))
    out[...] = jnp.broadcast_to(both[None], out.shape)


def partials_kernel(
    place, pair_old, pair_slot, pair_shift, pair_dest, ratio_in, own_in, peer,
    out, ratio, own, meta_v, meta, table, order, ends, sums, split, code_x, sems, out_sems,
    *, patches, fields, edge, size_y, chips_y, cores, new_count, pairs,
):
    rows = fields * edge
    lanes = edge * edge
    index_y = place[0]
    core = place[1]
    size_z = chips_y * cores
    for size in (edge, size_z, cores):
        assert size & (size - 1) == 0
    ratio_copy = pltpu.make_async_copy(ratio_in, ratio, sems.at[0])
    own_copy = pltpu.make_async_copy(own_in, own, sems.at[1])
    ratio_copy.start()
    own_copy.start()
    cells = patches * rows
    meta_v[...] = peer[cells:cells + META_ROWS, 0:meta_v.shape[1]].astype(I32)
    meta_copy = pltpu.make_async_copy(meta_v, meta, sems.at[2])
    meta_copy.start()

    def prepare(o, carry):
        high, low = halves(own[o])
        split[o, 0:rows] = high
        split[o, rows:2 * rows] = low
        high, low = halves(peer[pl.ds(o * rows, rows)])
        split[patches + o, 0:rows] = high
        split[patches + o, rows:2 * rows] = low
        return carry

    sums[...] = jnp.zeros_like(sums)
    chunks = ends.shape[0]
    chunk_size = out.shape[0] // chunks
    spare = out.shape[0]
    row = iota((rows, 2 * rows), 0)
    col = iota((rows, 2 * rows), 1) % rows
    code_x[...] = (over(col, edge) - over(row, edge)) * 4096 + within(col, edge)

    def enlist(found, base, old, slot, shift, dest):
        mine = jnp.where(within(dest, cores) == core, 1, 0)
        iz = within(dest, size_z)
        ix = over(dest, size_z)
        owner = (ix * size_y + index_y) * size_z + iz
        chip_y = over(iz, cores)
        chunk = jnp.where(core == 0, ix, chip_y)
        rank = ends[chunk]
        table[0, found] = base + old
        table[1, found] = ratio[owner * new_count + slot]
        table[2, found] = shift[0]
        table[3, found] = shift[1]
        table[7, found] = shift[2]
        table[4, found] = (chunk * chips_y + jnp.where(core == 0, chip_y, ix)) * new_count + slot
        table[5, found] = chunk
        table[6, found] = rank
        ends[chunk] = rank + mine
        return found + mine

    def enlist_own(p, found):
        shift = [pair_shift[a, p] for a in range(3)]
        return enlist(found, 0, pair_old[p], pair_slot[p], shift, pair_dest[0, p])

    def enlist_peer(p, found):
        shift = [meta[3 + a, p] for a in range(3)]
        return enlist(found, patches, meta[0, p], meta[1, p], shift, meta[2, p])

    for k in range(chunks):
        ends[k] = 0
    ratio_copy.wait()
    found = lax.fori_loop(0, pairs, enlist_own, jnp.int32(0), unroll=4)
    meta_copy.wait()
    found = lax.fori_loop(0, pairs, enlist_peer, found, unroll=4)

    before = jnp.int32(0)
    starts = []
    for k in range(chunks):
        starts.append(before)
        before = before + ends[k]
        ends[k] = starts[k]

    def place_in_order(p, carry):
        order[ends[table[5, p]] + table[6, p]] = p
        return carry

    lax.fori_loop(0, found, place_in_order, 0)
    stops = starts[1:] + [found]
    blank = table.shape[1] - 1
    for field, value in enumerate((0, 1, 0, 0, spare, 0, 0, 0)):
        table[field, blank] = value
    for extra in range(UNROLL - 1):
        order[found + extra] = blank

    def copy_out(k):
        at = pl.ds(k * chunk_size, chunk_size)
        return pltpu.make_async_copy(sums.at[at], out.at[at], out_sems.at[k])

    def send(low, high):
        for k in range(chunks):

            @pl.when((stops[k] > low) & (stops[k] <= high))
            def _():
                copy_out(k).start()

    own_copy.wait()
    lax.fori_loop(0, patches, prepare, 0)

    lane_k = iota((1, lanes), 1)
    lane_y = over(lane_k, edge)
    lane_z = within(lane_k, edge)
    near_row = iota((edge, lanes), 0)
    row_x = within(iota((rows, 1), 0), edge)

    def remap(step, carry):
        results = []
        for u in range(UNROLL):
            p = order[step * UNROLL + u]
            r = table[1, p]
            inverse = jnp.where(r == 2, 0.5, 1.0).astype(F32)
            spread = code_x[...] - (row_x * r + table[2, p])
            weight_x = jnp.where((spread & ~(r - 1)) == 0, inverse, 0.0).astype(BF16)
            section = jnp.dot(weight_x, split[table[0, p]], preferred_element_type=F32)
            spread = near_row - (lane_y * r + table[3, p])
            weight_y = jnp.where((spread & ~(r - 1)) == 0, inverse, 0.0)
            spread = near_row - (lane_z * r + table[7, p])
            weight_z = jnp.where((spread & ~(r - 1)) == 0, inverse, 0.0)
            weight_k = jnp.concatenate(
                [(weight_y[n:n + 1] * weight_z).astype(BF16) for n in range(edge)], axis=0
            )
            high, low = halves(section)
            stacked = jnp.concatenate([high, low], axis=0)
            product = jnp.dot(stacked, weight_k, preferred_element_type=F32)
            part = product[:rows] + product[rows:]
            results.append((p, part))
        for p, part in results:
            to = table[4, p]
            sums[to] = sums[to] + part
        send(step * UNROLL, (step + 1) * UNROLL)
        return carry

    steps = (found + UNROLL - 1) // UNROLL
    send(-1, 0)
    lax.fori_loop(0, steps, remap, 0)
    for k in range(chunks):
        copy_out(k).wait()


def fold_kernel(a, out, parts, sums, in_sems, out_sems, *, sources, chunk):
    kept = out.shape[0]
    chunks = kept // chunk
    copies = [
        [
            pltpu.make_async_copy(
                a.at[pl.ds(s * kept + j * chunk, chunk)], parts.at[pl.ds(s * kept + j * chunk, chunk)], in_sems.at[j, s]
            )
            for s in range(sources)
        ]
        for j in range(chunks)
    ]
    for row in copies:
        for copy in row:
            copy.start()
    outs = []
    for j in range(chunks):
        for copy in copies[j]:
            copy.wait()
        at = j * chunk
        total = parts[at:at + chunk]
        for s in range(1, sources):
            total = total + parts[s * kept + at:s * kept + at + chunk]
        sums[at:at + chunk] = total
        outs.append(pltpu.make_async_copy(sums.at[pl.ds(at, chunk)], out.at[pl.ds(at, chunk)], out_sems.at[j]))
        outs[-1].start()
    for copy in outs:
        copy.wait()


def gather_kernel(a, new_data, faces, *, count, fields, edge):
    rows = fields * edge
    lanes = edge * edge
    sources = a.shape[0] // count
    sums = []
    for q in range(count):
        total = a[q]
        for s in range(1, sources):
            total = total + a[s * count + q]
        sums.append(total)
    whole = jnp.concatenate(sums, axis=0)
    new_data[...] = whole
    high, low = halves(whole)
    stacked = jnp.concatenate([high, low], axis=0)
    source = iota((lanes, lanes), 0)
    target = within(iota((lanes, lanes), 1), edge)
    here = over(iota((edge, lanes), 1), edge) == iota((edge, lanes), 0)
    picks = (
        source == target,
        source == target + (lanes - edge),
        source == target * edge,
        source == target * edge + (edge - 1),
    )
    for q in range(count):
        faces[q, 6 * fields:, :] = jnp.zeros((FACE_ROWS - 6 * fields, lanes), F32)
        for f in range(fields):
            start = q * rows + f * edge
            faces[q, f:f + 1, :] = whole[start:start + 1]
            faces[q, fields + f:fields + f + 1, :] = whole[start + edge - 1:start + edge]
    for e, pick in enumerate(picks):
        weight = jnp.where(pick, 1.0, 0.0).astype(BF16)
        product = jnp.dot(stacked, weight, preferred_element_type=F32)
        layer = product[:count * rows] + product[count * rows:]
        for q in range(count):
            for f in range(fields):
                start = q * rows + f * edge
                line = jnp.sum(jnp.where(here, layer[start:start + edge], 0.0), axis=0, keepdims=True)
                at = (2 + e) * fields + f
                faces[q, at:at + 1, :] = line


def jump_kernel(place, side, patch, own, near, cross, jump, *, count, fields, devices):
    linear = place[2]
    even = within(linear, 2) == 0
    for q in range(count):
        for e in range(6):
            u = side[q, e]
            n = patch[q, e]
            at = linear + u - 1
            present = (u < 3) & (at >= 0) & (at < devices)
            other = pl.ds((e ^ 1) * fields, fields)
            inside = (u == 2) == even
            ghost = jnp.where(
                u == 1, own[n, other], jnp.where(inside, near[n, other], cross[n, other])
            )
            line = jnp.where(present, ghost - own[q, pl.ds(e * fields, fields)], 0.0)
            for f in range(fields):
                jump[q, f, e:e + 1, :] = line[f:f + 1]


def body(
    old_data, pair_old, pair_slot, pair_shift, pair_dest, new_ratio, neighbor_side, neighbor_patch
):
    patches, fields, edge, lanes = old_data.shape
    pairs = pair_old.shape[0]
    count = neighbor_side.shape[0]
    rows = fields * edge
    half = lanes // 2
    size_x = lax.axis_size("gx")
    size_y = lax.axis_size("gy")
    chips_y = lax.axis_size("gz_0")
    cores = lax.axis_size("gz_1")
    devices = size_x * size_y * chips_y * cores
    index_y = lax.axis_index("gy")
    core = lax.axis_index("gz_1")
    index_x = lax.axis_index("gx")
    chip_y = lax.axis_index("gz_0")
    linear = ((index_x * size_y + index_y) * chips_y + chip_y) * cores + core
    place = jnp.stack([index_y, core, linear, index_x, chip_y]).astype(I32)
    own = old_data.reshape(patches, rows, lanes)
    table = [slow(pair_old), slow(pair_slot), slow(pair_shift.T), slow(pair_dest.T)]
    swap = [(i, cores - 1 - i) for i in range(cores)]
    owners = size_x * chips_y * count
    smem = pl.BlockSpec(memory_space=SMEM)
    vmem = pl.BlockSpec(memory_space=VMEM)
    hbm = pl.BlockSpec(memory_space=HBM)
    params = pltpu.CompilerParams(vmem_limit_bytes=24 * 1024 * 1024)
    mass, packed = pl.pallas_call(
        functools.partial(
            head_kernel, patches=patches, fields=fields, edge=edge, size_y=size_y,
            size_z=chips_y * cores, new_count=count, pairs=pairs,
        ),
        out_shape=(
            jax.ShapeDtypeStruct((size_x * chips_y * cores, 8, half), F32),
            VMEM((patches * rows + META_ROWS, lanes), F32),
        ),
        in_specs=[smem] * 5 + [vmem] * 4 + [hbm, hbm],
        out_specs=(vmem, vmem),
        scratch_shapes=[
            pltpu.SMEM(new_ratio.shape, I32),
            pltpu.VMEM((patches, edge, lanes), F32),
            DMA((2,)),
        ],
        compiler_params=params,
        name="head",
    )(
        place, *table, slow(pair_old.reshape(1, pairs)), slow(pair_slot.reshape(1, pairs)), *table[:1:-1],
        slow(new_ratio), slow(old_data.reshape(patches * rows, lanes)),
    )
    peer = lax.ppermute(packed, "gz_1", swap)
    plane = lax.all_to_all(mass, PLANE, 0, 0, tiled=True)
    partials = pl.pallas_call(
        functools.partial(
            partials_kernel, patches=patches, fields=fields, edge=edge,
            size_y=size_y, chips_y=chips_y, cores=cores, new_count=count, pairs=pairs,
        ),
        out_shape=HBM((owners, rows, lanes), F32),
        in_specs=[smem] * 5 + [hbm, hbm, vmem],
        out_specs=hbm,
        scratch_shapes=[
            pltpu.SMEM(new_ratio.shape, I32),
            pltpu.VMEM((patches, rows, lanes), F32),
            pltpu.VMEM((META_ROWS, half), I32),
            pltpu.SMEM((META_ROWS, half), I32),
            pltpu.SMEM((8, 2 * pairs + 1), I32),
            pltpu.SMEM((2 * pairs + UNROLL,), I32),
            pltpu.SMEM((size_x,), I32),
            pltpu.VMEM((owners + 1, rows, lanes), F32),
            pltpu.VMEM((2 * patches, 2 * rows, lanes), BF16),
            pltpu.VMEM((rows, 2 * rows), I32),
            DMA((3,)),
            DMA((size_x,)),
        ],
        compiler_params=params,
        name="partials",
    )(place, *table, slow(new_ratio), slow(own), fast(peer))

    first_groups, last_groups = mixed_groups(size_x, size_y, chips_y, cores)
    first = lax.all_to_all(partials, ALL_AXES, 0, 0, tiled=True, axis_index_groups=first_groups)
    total = jnp.sum(plane, axis=0)

    def crossed(value, distance):
        return value + lax.ppermute(value, "gy", [(i, i ^ distance) for i in range(size_y)])

    total = crossed(total, 8)
    total = crossed(total, 4)
    total = crossed(total, 2)
    total = crossed(total, 1)
    kept = owners // size_x
    folded = pl.pallas_call(
        functools.partial(fold_kernel, sources=size_x, chunk=count),
        out_shape=HBM((kept, rows, lanes), F32),
        in_specs=[hbm],
        out_specs=hbm,
        scratch_shapes=[
            pltpu.VMEM((owners, rows, lanes), F32),
            pltpu.VMEM((kept, rows, lanes), F32),
            DMA((kept // count, size_x)),
            DMA((kept // count,)),
        ],
        compiler_params=params,
        name="fold",
    )(slow(first))
    last = lax.all_to_all(folded, ALL_AXES, 0, 0, tiled=True, axis_index_groups=last_groups)
    new_data, faces = pl.pallas_call(
        functools.partial(gather_kernel, count=count, fields=fields, edge=edge),
        out_shape=(
            jax.ShapeDtypeStruct((count * rows, lanes), F32),
            VMEM((count, FACE_ROWS, lanes), F32),
        ),
        in_specs=[vmem],
        out_specs=(vmem, vmem),
        compiler_params=params,
        name="gather",
    )(fast(last))
    cross = swapped(faces, 1)
    near = swapped(faces, 0)
    interface_jump = pl.pallas_call(
        functools.partial(jump_kernel, count=count, fields=fields, devices=devices),
        out_shape=jax.ShapeDtypeStruct((count, fields, 6, lanes), F32),
        in_specs=[smem, smem, smem, vmem, vmem, vmem],
        out_specs=vmem,
        compiler_params=params,
        name="jump",
    )(place, neighbor_side, neighbor_patch, fast(faces), fast(near), fast(cross))
    total_cells = patches * devices * edge * lanes
    mass_totals = total[:fields, :2].T / total_cells
    return (new_data.reshape(count, fields, edge, lanes), interface_jump, mass_totals)


def solution(mesh):
    torus = Mesh(
        mesh.devices.reshape(mesh.shape["gx"], mesh.shape["gy"], 4, 2), ("gx", "gy", "gz_0", "gz_1")
    )
    return jax.shard_map(
        body,
        mesh=torus,
        in_specs=(
            P(ALL_AXES, None, None, None),
            P(ALL_AXES),
            P(ALL_AXES),
            P(ALL_AXES, None),
            P(ALL_AXES, None),
            P(),
            P(ALL_AXES, None),
            P(ALL_AXES, None),
        ),
        out_specs=(P(ALL_AXES, None, None, None), P(ALL_AXES, None, None, None), P()),
        check_vma=False,
    )
```

```python
import functools

import jax
import jax.numpy as jnp
from jax import lax
from jax.experimental import pallas as pl
from jax.experimental.pallas import tpu as pltpu
from jax.sharding import Mesh
from jax.sharding import PartitionSpec as P


ALL_AXES = ("gx", "gy", "gz_0", "gz_1")
PLANE = ("gx", "gz_0", "gz_1")
UNROLL = 8
META_ROWS = 8
FACE_ROWS = 32
BF16 = jnp.bfloat16
F32 = jnp.float32
I32 = jnp.int32
VMEM = pltpu.VMEM
SMEM = pltpu.SMEM
HBM = pltpu.HBM
DMA = pltpu.SemaphoreType.DMA


def swapped(block, first):
    devices = lax.axis_size(ALL_AXES)
    pairs = [(i, i + 1) for i in range(first, devices - 1, 2)]
    return lax.ppermute(block, ALL_AXES, pairs + [(j, i) for i, j in pairs])


def fast(block):
    return pltpu.with_memory_space_constraint(block, VMEM)


def mixed_groups(size_x, size_y, chips_y, cores):
    def device(x, z, y, c):
        return ((x * size_y + z) * chips_y + y) * cores + c

    along_x, along_y = [], []
    for c in range(cores):
        lines_x = [[device(x, z, y, c) for x in range(size_x)] for z in range(size_y) for y in range(chips_y)]
        lines_y = [[device(x, z, y, c) for y in range(chips_y)] for z in range(size_y) for x in range(size_x)]
        along_x += lines_x if c == 0 else lines_y
        along_y += lines_y if c == 0 else lines_x
    return along_x, along_y


def slow(block):
    return pltpu.with_memory_space_constraint(block, HBM)


def halves(block):
    high = block.astype(BF16)
    low = (block - high.astype(F32)).astype(BF16)
    return high, low


def over(value, size):
    return value >> (size.bit_length() - 1)


def within(value, size):
    return value & (size - 1)


def iota(shape, dim):
    return lax.broadcasted_iota(I32, shape, dim)


def head_kernel(
    place, pair_old, pair_slot, pair_shift, pair_dest, old_row, slot_row, dest_row, shift_rows, ratio_in, own_in,
    out, packed, ratio, counts, sems,
    *, patches, fields, edge, size_y, size_z, new_count, pairs,
):
    lanes = edge * edge
    half = lanes // 2
    index_y = place[0]
    ratio_copy = pltpu.make_async_copy(ratio_in, ratio, sems.at[0])
    rows = fields * edge
    cells = patches * rows
    own_copy = pltpu.make_async_copy(own_in, packed.at[pl.ds(0, cells)], sems.at[1])
    ratio_copy.start()
    own_copy.start()
    packed[cells:] = jnp.zeros((META_ROWS, lanes), F32)
    at = cells
    for rows_in in (old_row, slot_row, dest_row, shift_rows):
        size = rows_in.shape[0]
        packed[at:at + size, 0:pairs] = rows_in[...].astype(F32)
        at += size
    counts[...] = jnp.zeros_like(counts)
    at_x = iota((edge, lanes), 0)
    at_y = over(iota((edge, lanes), 1), edge)
    at_z = within(iota((edge, lanes), 1), edge)

    def count(p, carry):
        dest = pair_dest[0, p]
        owner = (over(dest, size_z) * size_y + index_y) * size_z + within(dest, size_z)
        reach = edge * ratio[owner * new_count + pair_slot[p]]
        hit = jnp.full((edge, lanes), True)
        for a, at in enumerate((at_x, at_y, at_z)):
            distance = at - pair_shift[a, p]
            hit = hit & (distance >= 0) & (distance < reach)
        o = pair_old[p]
        counts[o] = counts[o] + jnp.where(hit, 1.0, 0.0)
        return carry

    ratio_copy.wait()
    lax.fori_loop(0, pairs, count, 0, unroll=4)
    own_copy.wait()

    def add(o, sums):
        weight = counts[o]
        olds, news = sums
        old_list, new_list = [], []
        for f in range(fields):
            block = packed[pl.ds(o * rows + f * edge, edge)]
            scaled = block * weight
            old_list.append(olds[f] + (block[:, :half] + block[:, half:]))
            new_list.append(news[f] + (scaled[:, :half] + scaled[:, half:]))
        return tuple(old_list), tuple(new_list)

    zero = tuple(jnp.zeros((edge, half), F32) for _ in range(fields))
    olds, news = lax.fori_loop(0, patches, add, (zero, zero), unroll=2)
    lane = iota((8, half), 1)
    blank = [jnp.zeros((8 - fields, half), F32)]
    old_rows = jnp.concatenate([jnp.sum(block, axis=0, keepdims=True) for block in olds] + blank, axis=0)
    new_rows = jnp.concatenate([jnp.sum(block, axis=0, keepdims=True) for block in news] + blank, axis=0)
    old_mass = jnp.sum(old_rows, axis=1, keepdims=True)
    new_mass = jnp.sum(new_rows, axis=1, keepdims=True)
    both = jnp.where(lane == 0, old_mass, jnp.where(lane == 1, new_mass, 0.0))
    out[...] = jnp.broadcast_to(both[None], out.shape)


def partials_kernel(
    place, pair_old, pair_slot, pair_shift, pair_dest, ratio_in, own_in, peer,
    out, ratio, own, meta_v, meta, table, order, ends, sums, split, code_x, sems, out_sems,
    *, patches, fields, edge, size_y, chips_y, cores, new_count, pairs,
):
    rows = fields * edge
    lanes = edge * edge
    index_y = place[0]
    core = place[1]
    size_z = chips_y * cores
    for size in (edge, size_z, cores):
        assert size & (size - 1) == 0
    ratio_copy = pltpu.make_async_copy(ratio_in, ratio, sems.at[0])
    own_copy = pltpu.make_async_copy(own_in, own, sems.at[1])
    ratio_copy.start()
    own_copy.start()
    cells = patches * rows
    meta_v[...] = peer[cells:cells + META_ROWS, 0:meta_v.shape[1]].astype(I32)
    meta_copy = pltpu.make_async_copy(meta_v, meta, sems.at[2])
    meta_copy.start()

    def prepare(o, carry):
        high, low = halves(own[o])
        split[o, 0:rows] = high
        split[o, rows:2 * rows] = low
        high, low = halves(peer[pl.ds(o * rows, rows)])
        split[patches + o, 0:rows] = high
        split[patches + o, rows:2 * rows] = low
        return carry

    sums[...] = jnp.zeros_like(sums)
    chunks = ends.shape[0]
    chunk_size = out.shape[0] // chunks
    spare = out.shape[0]
    row = iota((rows, 2 * rows), 0)
    col = iota((rows, 2 * rows), 1) % rows
    code_x[...] = (over(col, edge) - over(row, edge)) * 4096 + within(col, edge)

    def enlist(found, base, old, slot, shift, dest):
        mine = jnp.where(within(dest, cores) == core, 1, 0)
        iz = within(dest, size_z)
        ix = over(dest, size_z)
        owner = (ix * size_y + index_y) * size_z + iz
        chip_y = over(iz, cores)
        chunk = jnp.where(core == 0, ix, chip_y)
        rank = ends[chunk]
        table[0, found] = base + old
        table[1, found] = ratio[owner * new_count + slot]
        table[2, found] = shift[0]
        table[3, found] = shift[1]
        table[7, found] = shift[2]
        table[4, found] = (chunk * chips_y + jnp.where(core == 0, chip_y, ix)) * new_count + slot
        table[5, found] = chunk
        table[6, found] = rank
        ends[chunk] = rank + mine
        return found + mine

    def enlist_own(p, found):
        shift = [pair_shift[a, p] for a in range(3)]
        return enlist(found, 0, pair_old[p], pair_slot[p], shift, pair_dest[0, p])

    def enlist_peer(p, found):
        shift = [meta[3 + a, p] for a in range(3)]
        return enlist(found, patches, meta[0, p], meta[1, p], shift, meta[2, p])

    for k in range(chunks):
        ends[k] = 0
    ratio_copy.wait()
    found = lax.fori_loop(0, pairs, enlist_own, jnp.int32(0), unroll=4)
    meta_copy.wait()
    found = lax.fori_loop(0, pairs, enlist_peer, found, unroll=4)

    before = jnp.int32(0)
    starts = []
    for k in range(chunks):
        starts.append(before)
        before = before + ends[k]
        ends[k] = starts[k]

    def place_in_order(p, carry):
        order[ends[table[5, p]] + table[6, p]] = p
        return carry

    lax.fori_loop(0, found, place_in_order, 0)
    stops = starts[1:] + [found]
    blank = table.shape[1] - 1
    for field, value in enumerate((0, 1, 0, 0, spare, 0, 0, 0)):
        table[field, blank] = value
    for extra in range(UNROLL - 1):
        order[found + extra] = blank

    def copy_out(k):
        at = pl.ds(k * chunk_size, chunk_size)
        return pltpu.make_async_copy(sums.at[at], out.at[at], out_sems.at[k])

    def send(low, high):
        for k in range(chunks):

            @pl.when((stops[k] > low) & (stops[k] <= high))
            def _():
                copy_out(k).start()

    own_copy.wait()
    lax.fori_loop(0, patches, prepare, 0)

    lane_k = iota((1, lanes), 1)
    lane_y = over(lane_k, edge)
    lane_z = within(lane_k, edge)
    near_row = iota((edge, lanes), 0)
    row_x = within(iota((rows, 1), 0), edge)

    def remap(step, carry):
        results = []
        for u in range(UNROLL):
            p = order[step * UNROLL + u]
            r = table[1, p]
            inverse = jnp.where(r == 2, 0.5, 1.0).astype(F32)
            spread = code_x[...] - (row_x * r + table[2, p])
            weight_x = jnp.where((spread & ~(r - 1)) == 0, inverse, 0.0).astype(BF16)
            section = jnp.dot(weight_x, split[table[0, p]], preferred_element_type=F32)
            spread = near_row - (lane_y * r + table[3, p])
            weight_y = jnp.where((spread & ~(r - 1)) == 0, inverse, 0.0)
            spread = near_row - (lane_z * r + table[7, p])
            weight_z = jnp.where((spread & ~(r - 1)) == 0, inverse, 0.0)
            weight_k = jnp.concatenate(
                [(weight_y[n:n + 1] * weight_z).astype(BF16) for n in range(edge)], axis=0
            )
            high, low = halves(section)
            stacked = jnp.concatenate([high, low], axis=0)
            product = jnp.dot(stacked, weight_k, preferred_element_type=F32)
            part = product[:rows] + product[rows:]
            results.append((p, part))
        for p, part in results:
            to = table[4, p]
            sums[to] = sums[to] + part
        send(step * UNROLL, (step + 1) * UNROLL)
        return carry

    steps = (found + UNROLL - 1) // UNROLL
    send(-1, 0)
    lax.fori_loop(0, steps, remap, 0)
    for k in range(chunks):
        copy_out(k).wait()


def fold_kernel(a, out, parts, sums, in_sems, out_sems, *, sources, chunk):
    kept = out.shape[0]
    chunks = kept // chunk
    copies = [
        [
            pltpu.make_async_copy(
                a.at[pl.ds(s * kept + j * chunk, chunk)], parts.at[pl.ds(s * kept + j * chunk, chunk)], in_sems.at[j, s]
            )
            for s in range(sources)
        ]
        for j in range(chunks)
    ]
    for row in copies:
        for copy in row:
            copy.start()
    outs = []
    for j in range(chunks):
        for copy in copies[j]:
            copy.wait()
        at = j * chunk
        total = parts[at:at + chunk]
        for s in range(1, sources):
            total = total + parts[s * kept + at:s * kept + at + chunk]
        sums[at:at + chunk] = total
        outs.append(pltpu.make_async_copy(sums.at[pl.ds(at, chunk)], out.at[pl.ds(at, chunk)], out_sems.at[j]))
        outs[-1].start()
    for copy in outs:
        copy.wait()


def gather_kernel(a, summed, new_data, faces, mass, *, count, fields, edge, cells):
    rows = fields * edge
    lanes = edge * edge
    sources = a.shape[0] // count
    sums = []
    for q in range(count):
        total = a[q]
        for s in range(1, sources):
            total = total + a[s * count + q]
        sums.append(total)
    whole = jnp.concatenate(sums, axis=0)
    corner = summed[...]
    on_diagonal = iota(corner.shape, 0) == iota(corner.shape, 1)
    for k in range(mass.shape[0]):
        line = jnp.sum(jnp.where(on_diagonal, corner[:, k:k + 1], 0.0), axis=0, keepdims=True)
        mass[k:k + 1, :] = line[:, :fields] / cells
    new_data[...] = whole
    high, low = halves(whole)
    stacked = jnp.concatenate([high, low], axis=0)
    source = iota((lanes, lanes), 0)
    target = within(iota((lanes, lanes), 1), edge)
    here = over(iota((edge, lanes), 1), edge) == iota((edge, lanes), 0)
    picks = (
        source == target,
        source == target + (lanes - edge),
        source == target * edge,
        source == target * edge + (edge - 1),
    )
    for q in range(count):
        faces[q, 6 * fields:, :] = jnp.zeros((FACE_ROWS - 6 * fields, lanes), F32)
        for f in range(fields):
            start = q * rows + f * edge
            faces[q, f:f + 1, :] = whole[start:start + 1]
            faces[q, fields + f:fields + f + 1, :] = whole[start + edge - 1:start + edge]
    for e, pick in enumerate(picks):
        weight = jnp.where(pick, 1.0, 0.0).astype(BF16)
        product = jnp.dot(stacked, weight, preferred_element_type=F32)
        layer = product[:count * rows] + product[count * rows:]
        for q in range(count):
            for f in range(fields):
                start = q * rows + f * edge
                line = jnp.sum(jnp.where(here, layer[start:start + edge], 0.0), axis=0, keepdims=True)
                at = (2 + e) * fields + f
                faces[q, at:at + 1, :] = line


def jump_kernel(place, side, patch, own, near, cross, jump, *, count, fields, devices):
    linear = place[2]
    even = within(linear, 2) == 0
    for q in range(count):
        for e in range(6):
            u = side[q, e]
            n = patch[q, e]
            at = linear + u - 1
            present = (u < 3) & (at >= 0) & (at < devices)
            other = pl.ds((e ^ 1) * fields, fields)
            inside = (u == 2) == even
            ghost = jnp.where(
                u == 1, own[n, other], jnp.where(inside, near[n, other], cross[n, other])
            )
            line = jnp.where(present, ghost - own[q, pl.ds(e * fields, fields)], 0.0)
            for f in range(fields):
                jump[q, f, e:e + 1, :] = line[f:f + 1]


def body(
    old_data, pair_old, pair_slot, pair_shift, pair_dest, new_ratio, neighbor_side, neighbor_patch
):
    patches, fields, edge, lanes = old_data.shape
    pairs = pair_old.shape[0]
    count = neighbor_side.shape[0]
    rows = fields * edge
    half = lanes // 2
    size_x = lax.axis_size("gx")
    size_y = lax.axis_size("gy")
    chips_y = lax.axis_size("gz_0")
    cores = lax.axis_size("gz_1")
    devices = size_x * size_y * chips_y * cores
    index_y = lax.axis_index("gy")
    core = lax.axis_index("gz_1")
    index_x = lax.axis_index("gx")
    chip_y = lax.axis_index("gz_0")
    linear = ((index_x * size_y + index_y) * chips_y + chip_y) * cores + core
    place = jnp.stack([index_y, core, linear, index_x, chip_y]).astype(I32)
    own = old_data.reshape(patches, rows, lanes)
    table = [slow(pair_old), slow(pair_slot), slow(pair_shift.T), slow(pair_dest.T)]
    swap = [(i, cores - 1 - i) for i in range(cores)]
    owners = size_x * chips_y * count
    smem = pl.BlockSpec(memory_space=SMEM)
    vmem = pl.BlockSpec(memory_space=VMEM)
    hbm = pl.BlockSpec(memory_space=HBM)
    params = pltpu.CompilerParams(vmem_limit_bytes=24 * 1024 * 1024)
    mass, packed = pl.pallas_call(
        functools.partial(
            head_kernel, patches=patches, fields=fields, edge=edge, size_y=size_y,
            size_z=chips_y * cores, new_count=count, pairs=pairs,
        ),
        out_shape=(
            jax.ShapeDtypeStruct((size_x * chips_y * cores, 8, half), F32),
            VMEM((patches * rows + META_ROWS, lanes), F32),
        ),
        in_specs=[smem] * 5 + [vmem] * 4 + [hbm, hbm],
        out_specs=(vmem, vmem),
        scratch_shapes=[
            pltpu.SMEM(new_ratio.shape, I32),
            pltpu.VMEM((patches, edge, lanes), F32),
            DMA((2,)),
        ],
        compiler_params=params,
        name="head",
    )(
        place, *table, slow(pair_old.reshape(1, pairs)), slow(pair_slot.reshape(1, pairs)), *table[:1:-1],
        slow(new_ratio), slow(old_data.reshape(patches * rows, lanes)),
    )
    peer = lax.ppermute(packed, "gz_1", swap)
    plane = lax.all_to_all(mass, PLANE, 0, 0, tiled=True)
    partials = pl.pallas_call(
        functools.partial(
            partials_kernel, patches=patches, fields=fields, edge=edge,
            size_y=size_y, chips_y=chips_y, cores=cores, new_count=count, pairs=pairs,
        ),
        out_shape=HBM((owners, rows, lanes), F32),
        in_specs=[smem] * 5 + [hbm, hbm, vmem],
        out_specs=hbm,
        scratch_shapes=[
            pltpu.SMEM(new_ratio.shape, I32),
            pltpu.VMEM((patches, rows, lanes), F32),
            pltpu.VMEM((META_ROWS, half), I32),
            pltpu.SMEM((META_ROWS, half), I32),
            pltpu.SMEM((8, 2 * pairs + 1), I32),
            pltpu.SMEM((2 * pairs + UNROLL,), I32),
            pltpu.SMEM((size_x,), I32),
            pltpu.VMEM((owners + 1, rows, lanes), F32),
            pltpu.VMEM((2 * patches, 2 * rows, lanes), BF16),
            pltpu.VMEM((rows, 2 * rows), I32),
            DMA((3,)),
            DMA((size_x,)),
        ],
        compiler_params=params,
        name="partials",
    )(place, *table, slow(new_ratio), slow(own), fast(peer))

    first_groups, last_groups = mixed_groups(size_x, size_y, chips_y, cores)
    first = lax.all_to_all(partials, ALL_AXES, 0, 0, tiled=True, axis_index_groups=first_groups)
    total = jnp.sum(plane, axis=0)

    def crossed(value, distance):
        return value + lax.ppermute(value, "gy", [(i, i ^ distance) for i in range(size_y)])

    total = crossed(total, 8)
    total = crossed(total, 4)
    total = crossed(total, 2)
    total = crossed(total, 1)
    kept = owners // size_x
    folded = pl.pallas_call(
        functools.partial(fold_kernel, sources=size_x, chunk=count),
        out_shape=HBM((kept, rows, lanes), F32),
        in_specs=[hbm],
        out_specs=hbm,
        scratch_shapes=[
            pltpu.VMEM((owners, rows, lanes), F32),
            pltpu.VMEM((kept, rows, lanes), F32),
            DMA((kept // count, size_x)),
            DMA((kept // count,)),
        ],
        compiler_params=params,
        name="fold",
    )(slow(first))
    last = lax.all_to_all(folded, ALL_AXES, 0, 0, tiled=True, axis_index_groups=last_groups)
    new_data, faces, mass_totals = pl.pallas_call(
        functools.partial(gather_kernel, count=count, fields=fields, edge=edge, cells=float(patches * devices * edge * lanes)),
        out_shape=(
            jax.ShapeDtypeStruct((count * rows, lanes), F32),
            VMEM((count, FACE_ROWS, lanes), F32),
            jax.ShapeDtypeStruct((2, fields), F32),
        ),
        in_specs=[vmem, vmem],
        out_specs=(vmem, vmem, vmem),
        compiler_params=params,
        name="gather",
    )(fast(last), total)
    cross = swapped(faces, 1)
    near = swapped(faces, 0)
    interface_jump = pl.pallas_call(
        functools.partial(jump_kernel, count=count, fields=fields, devices=devices),
        out_shape=jax.ShapeDtypeStruct((count, fields, 6, lanes), F32),
        in_specs=[smem, smem, smem, vmem, vmem, vmem],
        out_specs=vmem,
        compiler_params=params,
        name="jump",
    )(place, neighbor_side, neighbor_patch, fast(faces), fast(near), fast(cross))
    return (new_data.reshape(count, fields, edge, lanes), interface_jump, mass_totals)


def solution(mesh):
    torus = Mesh(
        mesh.devices.reshape(mesh.shape["gx"], mesh.shape["gy"], 4, 2), ("gx", "gy", "gz_0", "gz_1")
    )
    return jax.shard_map(
        body,
        mesh=torus,
        in_specs=(
            P(ALL_AXES, None, None, None),
            P(ALL_AXES),
            P(ALL_AXES),
            P(ALL_AXES, None),
            P(ALL_AXES, None),
            P(),
            P(ALL_AXES, None),
            P(ALL_AXES, None),
        ),
        out_specs=(P(ALL_AXES, None, None, None), P(ALL_AXES, None, None, None), P()),
        check_vma=False,
    )
```
